32 devices in a mesh: enc: 8 (over z, x), dec: 2 (over y), grp: 2 (over core).
Axes of the slice: x: 2, y: 2, z: 4, core: 2. Of those that a mesh axis runs over, the one named last changes fastest.
Arguments:
- images: bfloat16 [32, 4, 32, 1280], P(('enc', 'dec', 'grp')), may hold values from -6 to 6
- ln_gain: float32 [1280], replicated, may hold values from 0.1 to 1.9
- ln_bias: float32 [1280], replicated, may hold values from -3 to 3
- fc1_weight: bfloat16 [5120, 1280], P('enc'), may hold values from -0.15625 to 0.15625
- fc1_bias: float32 [5120], P('enc'), may hold values from -3 to 3
- fc2_weight: bfloat16 [5120, 1280], P('enc'), may hold values from -0.078125 to 0.078125
- fc2_bias: float32 [1280], replicated, may hold values from -3 to 3
- key_weight: bfloat16 [1280, 512], replicated, may hold values from -0.15625 to 0.15625
- value_weight: bfloat16 [1280, 512], replicated, may hold values from -0.15625 to 0.15625
- text: bfloat16 [32, 128, 8192], P(('enc', 'grp')), may hold values from -6 to 6
- query_weight: bfloat16 [8192, 4096], P('enc', 'dec'), may hold values from -0.0625 to 0.0625
- tiles: int32 [8, 2, 2], replicated, may hold values from 1 to 4, as said below
- links: int32 [32, 2], P(('enc', 'grp')), may hold values from 0 to 1, as said below
- lengths: int32 [32], P(('enc', 'grp')), may hold values from 1 to 128
- state_grads: bfloat16 [32, 4, 32, 1280], P(('enc', 'dec', 'grp')), may hold values from -0.125 to 0.125
Outputs:
- context: bfloat16 [32, 128, 4096], P(('enc', 'grp'), None, 'dec')
- fc1_grad: float32 [5120, 1280], P(('enc', 'dec', 'grp'))
- fc2_grad: float32 [5120, 1280], P(('enc', 'dec', 'grp'))
The draws below stay inside these ranges and needn't reach their ends.
Inputs may be any that keep to these rules, and one draw needn't show every extreme that they name: The 8 images that share their last two indices have 20 tiles together, and one of them has 4. `links`: every text is linked to at least one image.
All inputs are finite; a program needn't handle non-finite values.
Results may differ from the reference program's by a relative error of at most 0.017.
Values may be sent and summed in bfloat16 or wider, within the bound.
A program may use at most 128 MiB of HBM per device.

```python
import jax
import jax.numpy as jnp
from jax import lax

DV = 1280
FF = 5120
DT = 8192
HEADS = 32
KV_HEADS = 4
HD = 128
TXT = 128
TILES = 4
PATCH = 32
SAMP = 2
IMAGES = 32
TEXTS = 32
N_ENC = 8
N_DEC = 2
N_GRP = 2


def draw_tiles(key, part):
    groups = N_DEC * N_GRP
    group_keys = jax.random.split(jax.random.fold_in(key, 11), groups)

    def one_group(group_key):
        first_key, second_key = jax.random.split(group_key)
        shuffled = jax.random.permutation(first_key, 3 * (N_ENC - 1))
        chosen = (shuffled < 3 * N_ENC // 2 - 3).astype(jnp.int32)
        others = jnp.sum(chosen.reshape(N_ENC - 1, 3), axis=1)
        forced = jax.random.randint(second_key, (), 0, N_ENC)
        index = jnp.arange(N_ENC)
        earlier = jnp.take(others, jnp.clip(index, 0, N_ENC - 2))
        later = jnp.take(others, jnp.clip(index - 1, 0, N_ENC - 2))
        extra = jnp.where(index < forced, earlier, jnp.where(index == forced, 3, later))
        return 1 + extra
    columns = jax.vmap(one_group)(group_keys)
    return columns.T.reshape(N_ENC, N_DEC, N_GRP).astype(jnp.int32)


def draw_links(key, part):
    first_key, second_key = jax.random.split(jax.random.fold_in(key, 23))
    coins = jax.random.randint(first_key, (TEXTS, N_DEC), 0, 5)
    chosen = jax.random.randint(second_key, (TEXTS, 1), 0, N_DEC)
    column = jnp.arange(N_DEC)[None, :]
    return jnp.where((coins < 2) | (column == chosen), 1, 0).astype(jnp.int32)


def with_ends(array, rng, least, high):
    extent = array.shape
    index_at = [jax.random.randint(jax.random.fold_in(rng, axis), (), 0, extent[axis]) for axis in range(len(extent))]
    array = array.at[tuple(index_at)].set(least)
    longest = extent.index(max(extent))
    index_at[longest] = (index_at[longest] + 1) % extent[longest]
    return array.at[tuple(index_at)].set(high)


def steps_of(rng, extent, shards, smallest, largest):
    def one(position, shards_of):
        draws = jax.random.uniform(jax.random.fold_in(jax.random.fold_in(rng, 6), position), (shards_of,), jnp.float32, smallest / len(shards), largest / len(shards))
        return jnp.repeat(jnp.exp(draws), extent[position] // shards_of).reshape((-1,) + (1,) * (len(extent) - position - 1))

    level = one(*shards[0])
    for cut in shards[1:]:
        level = level * one(*cut)
    return level


def normal_values(own_key, shape, scale, bound, cuts=(), kind=jnp.bfloat16):
    entries = scale * jax.random.normal(own_key, shape, jnp.float32)
    if cuts:
        entries = entries * steps_of(own_key, shape, cuts, -0.22, 0.18)
    return jnp.clip(entries, -bound, bound).astype(kind)


def setup_inputs(seed: int = 0) -> dict:
    streams_of = jax.random.split(jax.random.key(seed), 16)
    images = normal_values(streams_of[0], (IMAGES, TILES, PATCH, DV), 1.0, 6.0, ((0, 32),))
    ln_gain = jnp.clip(1.0 + 0.18 * jax.random.normal(streams_of[1], (DV,), jnp.float32), 0.1, 1.9)
    ln_bias = normal_values(streams_of[2], (DV,), 0.5, 3.0, (), jnp.float32)
    fc1_weight = normal_values(streams_of[3], (FF, DV), DV ** -0.5, 0.15625, ((0, 8),))
    fc1_bias = normal_values(streams_of[4], (FF,), 0.5, 3.0, ((0, 8),), jnp.float32)
    fc2_weight = normal_values(streams_of[5], (FF, DV), FF ** -0.5, 0.078125, ((0, 8),))
    fc2_bias = normal_values(streams_of[6], (DV,), 0.5, 3.0, (), jnp.float32)
    key_weight = normal_values(streams_of[7], (DV, KV_HEADS * HD), DV ** -0.5, 0.15625)
    value_weight = normal_values(streams_of[8], (DV, KV_HEADS * HD), DV ** -0.5, 0.15625)
    text = normal_values(streams_of[9], (TEXTS, TXT, DT), 1.0, 6.0, ((0, 16),))
    query_weight = normal_values(streams_of[10], (DT, HEADS * HD), DT ** -0.5, 0.0625, ((0, 8), (1, 2)))
    tiles = draw_tiles(jax.random.fold_in(streams_of[15], 71), 0)
    links = draw_links(jax.random.fold_in(streams_of[15], 71), 0)
    lengths = with_ends(jax.random.randint(streams_of[13], (TEXTS,), 1, TXT + 1), jax.random.fold_in(streams_of[13], 1), 1, TXT).astype(jnp.int32)
    state_grads = normal_values(streams_of[14], (IMAGES, TILES, PATCH, DV), 0.02, 0.125, ((0, 32),))
    return dict(images=images, ln_gain=ln_gain, ln_bias=ln_bias, fc1_weight=fc1_weight, fc1_bias=fc1_bias, fc2_weight=fc2_weight, fc2_bias=fc2_bias, key_weight=key_weight, value_weight=value_weight, text=text, query_weight=query_weight, tiles=tiles, links=links, lengths=lengths, state_grads=state_grads)


EPSILON = 1e-06

def normalize_layer(values, gain, shift):
    middle = lax.optimization_barrier(jnp.mean(values, axis=-1, keepdims=True))
    centered = values - middle
    spread = lax.optimization_barrier(jnp.mean(centered * centered, axis=-1, keepdims=True))
    return centered * lax.rsqrt(spread + EPSILON) * gain + shift

def normalize_heads(values):
    return values * lax.rsqrt(lax.optimization_barrier(jnp.mean(values * values, axis=-1, keepdims=True)) + EPSILON)

def gelu_slope(values):
    return 0.5 * (1.0 + lax.erf(values * 0.7071067811865476)) + values * jnp.exp(-0.5 * values * values) * 0.3989422804014327

def reference(images, ln_gain, ln_bias, fc1_weight, fc1_bias, fc2_weight, fc2_bias, key_weight, value_weight, text, query_weight, tiles, links, lengths, state_grads):
    img_rows = TILES * PATCH
    per_group = HEADS // KV_HEADS
    block_width = FF // N_ENC
    flat_rows = images.reshape(IMAGES * img_rows, DV)
    normed = normalize_layer(flat_rows.astype(jnp.float32), ln_gain, ln_bias).astype(jnp.bfloat16)
    pre = lax.dot_general(normed, fc1_weight, (((1,), (1,)), ((), ())), preferred_element_type=jnp.float32) + fc1_bias
    hidden = jax.nn.gelu(pre, approximate=False).astype(jnp.bfloat16)

    def add_block(block, total):
        start = (block * block_width).astype(jnp.int32)
        part = jnp.dot(lax.dynamic_slice_in_dim(hidden, start, block_width, 1), lax.dynamic_slice_in_dim(fc2_weight, start, block_width, 0), preferred_element_type=jnp.float32)
        rounded = lax.optimization_barrier(part.astype(jnp.bfloat16))
        return total + rounded.astype(jnp.float32)
    partial_sum = lax.fori_loop(0, N_ENC, add_block, jnp.zeros((IMAGES * img_rows, DV), jnp.float32))
    states = (flat_rows.astype(jnp.float32) + partial_sum + fc2_bias).astype(jnp.bfloat16)
    key_raw = jnp.dot(states, key_weight, preferred_element_type=jnp.float32).reshape(IMAGES * img_rows, KV_HEADS, HD)
    keys = normalize_heads(key_raw).astype(jnp.bfloat16)
    values = jnp.dot(states, value_weight, preferred_element_type=jnp.float32).astype(jnp.bfloat16).reshape(IMAGES * img_rows, KV_HEADS, HD)
    keys = keys.reshape(N_ENC, N_DEC, N_GRP, img_rows, KV_HEADS, HD).transpose(0, 2, 4, 1, 3, 5).reshape(N_ENC * N_GRP, KV_HEADS, N_DEC * img_rows, HD)
    values = values.reshape(N_ENC, N_DEC, N_GRP, img_rows, KV_HEADS, HD).transpose(0, 2, 4, 1, 3, 5).reshape(N_ENC * N_GRP, KV_HEADS, N_DEC * img_rows, HD)
    group_tiles = tiles.transpose(0, 2, 1)
    live_keys = (jnp.arange(TILES)[None, None, None, :] < group_tiles[..., None]).astype(jnp.int32)
    live_keys = jnp.broadcast_to(live_keys[..., None], (N_ENC, N_GRP, N_DEC, TILES, PATCH)).reshape(N_ENC * N_GRP, N_DEC, img_rows)
    query_raw = jnp.dot(text.reshape(TEXTS * TXT, DT), query_weight, preferred_element_type=jnp.float32).reshape(TEXTS, TXT, HEADS, HD)
    queries = normalize_heads(query_raw).astype(jnp.bfloat16).reshape(N_ENC * N_GRP, SAMP, TXT, KV_HEADS, per_group, HD)
    group_links = links.reshape(N_ENC * N_GRP, SAMP, N_DEC)
    group_lengths = lengths.reshape(N_ENC * N_GRP, SAMP)

    def attend(inputs):
        group_queries, group_keys, group_values, group_live, link_rows, length_rows = inputs
        allowed = (link_rows[:, :, None] * group_live[None, :, :]).reshape(SAMP, N_DEC * img_rows) > 0
        scores = jnp.einsum('sqghd,gkd->sghqk', group_queries.astype(jnp.float32), group_keys.astype(jnp.float32)) * HD ** (-0.5)
        weights = jnp.where(allowed[:, None, None, None, :], jnp.exp(scores), 0.0)
        probs = (weights / lax.optimization_barrier(jnp.sum(weights, axis=-1, keepdims=True))).astype(jnp.bfloat16)
        mixed = jnp.einsum('sghqk,gkd->sqghd', probs.astype(jnp.float32), group_values.astype(jnp.float32))
        valid = jnp.arange(TXT)[None, :] < length_rows[:, None]
        mixed = jnp.where(valid[:, :, None, None, None], mixed, 0.0)
        return mixed.reshape(SAMP, TXT, HEADS * HD).astype(jnp.bfloat16)
    context = lax.map(attend, (queries, keys, values, live_keys, group_links, group_lengths)).reshape(TEXTS, TXT, HEADS * HD)
    live_rows = jnp.arange(TILES)[None, :] < tiles.reshape(IMAGES)[:, None]
    live_rows = jnp.broadcast_to(live_rows[:, :, None], (IMAGES, TILES, PATCH)).reshape(IMAGES * img_rows, 1)
    cotangent = jnp.where(live_rows, state_grads.reshape(IMAGES * img_rows, DV), jnp.zeros((), state_grads.dtype))
    hidden_grad = lax.dot_general(cotangent, fc2_weight, (((1,), (1,)), ((), ())), preferred_element_type=jnp.float32)
    fc2_grad = lax.dot_general(hidden, cotangent, (((0,), (0,)), ((), ())), preferred_element_type=jnp.float32)
    pre_grad = (hidden_grad * gelu_slope(pre)).astype(jnp.bfloat16)
    fc1_grad = lax.dot_general(pre_grad, normed, (((0,), (0,)), ((), ())), preferred_element_type=jnp.float32)
    return (context, fc1_grad, fc2_grad)
```

```python
import functools

import jax
import jax.numpy as jnp
from jax import lax
from jax.experimental import pallas as pl
from jax.experimental.pallas import tpu as pltpu
from jax.sharding import PartitionSpec as P


HEADS = 32
KV_HEADS = 4
HD = 128


EPSILON = 1e-06


def normalize_layer(values, gain, shift):
    middle = jnp.mean(values, axis=-1, keepdims=True)
    centered = values - middle
    spread = jnp.mean(centered * centered, axis=-1, keepdims=True)
    return centered * lax.rsqrt(spread + EPSILON) * gain + shift


def normalize_heads(values):
    return values * lax.rsqrt(jnp.mean(values * values, axis=-1, keepdims=True) + EPSILON)


def gelu_slope(values):
    return (
        0.5 * (1.0 + lax.erf(values * 0.7071067811865476))
        + values * jnp.exp(-0.5 * values * values) * 0.3989422804014327
    )


def encoder_rows(rows, fc1_weight, fc1_bias, fc2_weight):
    pre = (
        lax.dot_general(
            rows, fc1_weight, (((1,), (1,)), ((), ())), preferred_element_type=jnp.float32
        )
        + fc1_bias
    )
    hidden = jax.nn.gelu(pre, approximate=False).astype(jnp.bfloat16)
    partial_sum = jnp.dot(hidden, fc2_weight, preferred_element_type=jnp.float32)
    return (pre, hidden, partial_sum)


def weight_terms(rows, pre, hidden, cotangent, fc2_weight):
    hidden_grad = lax.dot_general(
        cotangent, fc2_weight, (((1,), (1,)), ((), ())), preferred_element_type=jnp.float32
    )
    second_term = lax.dot_general(
        hidden, cotangent, (((0,), (0,)), ((), ())), preferred_element_type=jnp.float32
    )
    pre_grad = (hidden_grad * gelu_slope(pre)).astype(jnp.bfloat16)
    first_term = lax.dot_general(
        pre_grad, rows, (((0,), (0,)), ((), ())), preferred_element_type=jnp.float32
    )
    return (first_term, second_term)


def project_heads(states, key_columns, value_columns, heads):
    width = states.shape[-1]
    key_raw = jnp.einsum(
        "rd,dhe->hre",
        states,
        key_columns.reshape(width, heads, HD),
        preferred_element_type=jnp.float32,
    )
    keys = normalize_heads(key_raw).astype(jnp.bfloat16)
    values = jnp.einsum(
        "rd,dhe->hre",
        states,
        value_columns.reshape(width, heads, HD),
        preferred_element_type=jnp.float32,
    ).astype(jnp.bfloat16)
    return (keys, values)


def shifted(values, axis, step):
    size = lax.axis_size(axis)
    return lax.ppermute(values, axis, [(i, (i + step) % size) for i in range(size)])


def swapped(values):
    return lax.ppermute(values, "enc", [(i, i ^ 1) for i in range(lax.axis_size("enc"))])


def share_text(text_rows):
    enc_count = lax.axis_size("enc")
    _, depth = text_rows.shape
    side = lax.axis_index("enc") % 2
    block = depth // enc_count
    even = jnp.stack([text_rows[:, i * block : (i + 1) * block] for i in range(0, enc_count, 2)])
    odd = jnp.stack([text_rows[:, i * block : (i + 1) * block] for i in range(1, enc_count, 2)])
    own = jnp.where(side == 0, even, odd)
    away = jnp.where(side == 0, odd, even)
    arrived = swapped(away)
    pair = jnp.concatenate([arrived, own], axis=1)
    return jnp.concatenate(
        [pair] + [shifted(pair, "grp", step) for step in range(1, lax.axis_size("grp"))], axis=1
    )


def project_queries(text_blocks, weight, before):
    grp_count = lax.axis_size("grp")
    ring = lax.axis_size("enc") // 2
    enc_count = lax.axis_size("enc")
    place = lax.axis_index("enc") // 2
    total = None
    for step in range(ring):
        if step == max(0, ring - 2):
            weight, _ = lax.optimization_barrier((weight, before))
        left = lax.dynamic_index_in_dim(text_blocks, (place - step) % ring, 0, keepdims=False)
        term = jnp.dot(left, weight, preferred_element_type=jnp.float32)
        total = term if total is None else total + term
        if step < ring - 1:
            weight = lax.ppermute(
                weight, "enc", [(i, (i + 2) % enc_count) for i in range(enc_count)]
            )
    columns = total.shape[1]
    total = total.reshape(grp_count, 2, -1, columns)
    arrived = swapped(total[:, 0].astype(jnp.bfloat16))
    raw = total[:, 1] + arrived.astype(jnp.float32)
    own = normalize_heads(raw.reshape(grp_count, -1, columns // HD, HD)).astype(jnp.bfloat16)
    blocks = jnp.stack(
        [own[0]] + [shifted(own[step], "grp", -step) for step in range(1, grp_count)], axis=1
    )
    start = (grp_count - lax.axis_index("grp")) % grp_count
    blocks = lax.dynamic_slice_in_dim(
        jnp.concatenate([blocks, blocks], axis=1), start, grp_count, 1
    )
    return blocks.reshape(blocks.shape[0], grp_count * columns)


def share_keys(states, key_weight, value_weight, first_head, kv_local):
    dec_count = lax.axis_size("dec")
    rows, _ = states.shape
    if dec_count == 2 and kv_local * dec_count == KV_HEADS:
        keys, values = project_heads(states, key_weight, value_weight, KV_HEADS)
        paired = jnp.stack([keys, values])
        own = lax.dynamic_slice_in_dim(paired, first_head, kv_local, 1)
        away = lax.dynamic_slice_in_dim(paired, KV_HEADS - kv_local - first_head, kv_local, 1)
        arrived = shifted(away, "dec", 1)
        first = lax.axis_index("dec") == 0
        paired = jnp.stack(
            [jnp.where(first, own, arrived), jnp.where(first, arrived, own)], axis=1
        )
        return (paired[0], paired[1])
    key_columns = lax.dynamic_slice_in_dim(key_weight, first_head * HD, kv_local * HD, 1)
    value_columns = lax.dynamic_slice_in_dim(value_weight, first_head * HD, kv_local * HD, 1)
    piece = lax.all_gather(states, "dec", axis=0, tiled=True)
    key_part, value_part = project_heads(piece, key_columns, value_columns, kv_local)
    shape = (kv_local, dec_count, rows, HD)
    return (
        key_part.reshape(shape).transpose(1, 0, 2, 3),
        value_part.reshape(shape).transpose(1, 0, 2, 3),
    )


def share_grads(terms):
    dec_count = lax.axis_size("dec")
    grp_count = lax.axis_size("grp")
    rows = terms.shape[1] // (dec_count * grp_count)
    if dec_count == 2 and grp_count == 2:
        parts = terms.reshape(2, dec_count, grp_count, rows, -1)
        grp_place = lax.axis_index("grp")
        dec_place = lax.axis_index("dec")
        kept = lax.dynamic_index_in_dim(parts, grp_place, 2, keepdims=False)
        away = lax.dynamic_index_in_dim(parts, 1 - grp_place, 2, keepdims=False)
        kept = kept + shifted(away.astype(jnp.bfloat16), "grp", 1).astype(jnp.float32)
        away = lax.dynamic_index_in_dim(kept, 1 - dec_place, 1, keepdims=False)
        kept = lax.dynamic_index_in_dim(kept, dec_place, 1, keepdims=False)
        kept = kept + shifted(away.astype(jnp.bfloat16), "dec", 1).astype(jnp.float32)
        return (kept[0], kept[1])
    summed = lax.psum_scatter(
        terms.astype(jnp.bfloat16), ("dec", "grp"), scatter_dimension=1, tiled=True
    ).astype(jnp.float32)
    return (summed[0], summed[1])


MESH = pl.DeviceIdType.MESH


def pick(table, place):
    return sum(jnp.where(place == i, value, 0) for i, value in enumerate(table))


def step_kernel(
    line,
    rows_ref,
    bias_ref,
    up_ref,
    down_ref,
    text_ref,
    weight_ref,
    query_ref,
    states_ref,
    up_grad_ref,
    down_grad_ref,
    tb,
    wb,
    fb,
    bb,
    bias_col,
    rows,
    pre,
    hid_t,
    hid,
    pg_t,
    po,
    psend,
    precv,
    msend,
    mrecv,
    gs1,
    gr1,
    gs2,
    gr2,
    gs3,
    gr3,
    local_sem,
    t_send,
    t_recv,
    y_send,
    y_recv,
    x_send,
    x_recv,
    s_send,
    s_recv,
    a_send,
    a_recv,
    p_send,
    p_recv,
    m_send,
    m_recv,
    g_send,
    g_recv,
):
    f32 = jnp.float32
    bf16 = jnp.bfloat16
    enc = lax.axis_index("enc")
    y = lax.axis_index("dec")
    g = lax.axis_index("grp")
    z, x = enc // 2, enc % 2
    other_x = ((z * 2 + 1 - x), y, g)
    other_y = (enc, 1 - y, g)
    other_g = (enc, y, 1 - g)

    def along(place):
        return (place * 2 + x, y, g)

    orders = [
        sorted([a for a in range(line) if a != p], key=lambda a: (-abs(a - p), min(a, line - 1 - a)))
        for p in range(line)
    ]
    order = [pick([orders[p][i] for p in range(line)], z) for i in range(line - 1)]
    text_rows, depth = tb.shape[2], tb.shape[3]
    half_cols = wb.shape[3]
    img = rows.shape[2]
    width = rows.shape[3]
    units = fb.shape[2]
    piece = units // 2
    part = units // 4

    barrier = pltpu.get_barrier_semaphore()
    for k in range(line):

        @pl.when(z != k)
        def _():
            pl.semaphore_signal(barrier, inc=1, device_id=along(k), device_id_type=MESH)

    for to in (other_x, other_y, other_g):
        pl.semaphore_signal(barrier, inc=1, device_id=to, device_id_type=MESH)
    pl.semaphore_wait(barrier, line + 2)

    def remote(src, dst, send, recv, to):
        return pltpu.make_async_remote_copy(
            src_ref=src, dst_ref=dst, send_sem=send, recv_sem=recv, device_id=to, device_id_type=MESH
        )

    def text_copy(i):
        b = order[i]
        at = pl.multiple_of((b * 2 + y) * depth, depth)
        return remote(
            text_ref.at[:, pl.ds(at, depth)], tb.at[z, y], t_send.at[i], t_recv.at[z], along(b)
        )

    def text_landed(a):
        return remote(tb.at[a, y], tb.at[a, y], t_send.at[0], t_recv.at[a], other_y)

    def text_relay(a):
        return remote(tb.at[a, y], tb.at[a, y], y_send.at[a], y_recv.at[a], other_y)

    def text_relayed(a):
        return remote(tb.at[a, 1 - y], tb.at[a, 1 - y], y_send.at[a], y_recv.at[a], other_y)

    weight_x = remote(
        weight_ref.at[:, pl.ds(pl.multiple_of(g * half_cols, half_cols), half_cols)],
        wb.at[x, g],
        x_send.at[0],
        x_recv.at[0],
        other_x,
    )
    weight_x_in = remote(wb.at[1 - x, g], wb.at[1 - x, g], x_send.at[0], x_recv.at[0], other_x)
    weight_s = remote(wb.at[1 - x, g], wb.at[1 - x, g], s_send.at[0], s_recv.at[0], other_g)
    weight_s_in = remote(wb.at[1 - x, 1 - g], wb.at[1 - x, 1 - g], s_send.at[0], s_recv.at[0], other_g)

    piece_at = pl.multiple_of(g * piece, piece)
    away_at = pl.multiple_of((1 - g) * piece, piece)

    def unit_x(ref, kind):
        return remote(
            ref.at[pl.ds(piece_at, piece)],
            fb.at[kind, x, pl.ds(piece_at, piece)],
            x_send.at[1],
            x_recv.at[1],
            other_x,
        )

    mine = fb.at[y, 1 - x, pl.ds(piece_at, piece)]
    unit_x_in = remote(mine, mine, x_send.at[1], x_recv.at[1], other_x)
    unit_s = remote(mine, mine, s_send.at[1], s_recv.at[1], other_g)
    unit_s_spot = fb.at[y, 1 - x, pl.ds(away_at, piece)]
    unit_s_in = remote(unit_s_spot, unit_s_spot, s_send.at[1], s_recv.at[1], other_g)
    unit_y = remote(mine, mine, y_send.at[line], y_recv.at[line], other_y)
    crossed = fb.at[1 - y, 1 - x, pl.ds(piece_at, piece)]
    unit_y_in = remote(crossed, crossed, y_send.at[line], y_recv.at[line], other_y)
    unit_s2 = remote(crossed, crossed, s_send.at[2], s_recv.at[2], other_g)
    unit_s2_spot = fb.at[1 - y, 1 - x, pl.ds(away_at, piece)]
    unit_s2_in = remote(unit_s2_spot, unit_s2_spot, s_send.at[2], s_recv.at[2], other_g)
    bias_x = remote(bias_ref, bb.at[x], x_send.at[2], x_recv.at[2], other_x)
    bias_x_in = remote(bb.at[1 - x], bb.at[1 - x], x_send.at[2], x_recv.at[2], other_x)

    def rows_copy(a, right, own):
        to = along(z + 1) if right else along(z - 1)
        src = rows_ref if own else rows.at[:, a]
        return remote(src, rows.at[:, a], a_send.at[1 if right else 0, a], a_recv.at[a], to)

    def rows_landed(a):
        return remote(rows.at[:, a], rows.at[:, a], a_send.at[0, a], a_recv.at[a], other_y)

    locals_ = [
        pltpu.make_async_copy(weight_ref.at[:, pl.ds(c * half_cols, half_cols)], wb.at[x, c], local_sem.at[c])
        for c in range(2)
    ] + [
        pltpu.make_async_copy(up_ref, fb.at[0, x], local_sem.at[2]),
        pltpu.make_async_copy(down_ref, fb.at[1, x], local_sem.at[3]),
        pltpu.make_async_copy(bias_ref, bb.at[x], local_sem.at[4]),
        pltpu.make_async_copy(rows_ref, rows.at[:, z], local_sem.at[5]),
    ] + [
        pltpu.make_async_copy(
            text_ref.at[:, pl.ds(pl.multiple_of((z * 2 + h) * depth, depth), depth)],
            tb.at[z, h],
            local_sem.at[6 + h],
        )
        for h in range(2)
    ]

    for i in range(line - 1):
        text_copy(i).start()
    weight_x.start()

    @pl.when(y == 0)
    def _():
        unit_x(up_ref, 0).start()

    @pl.when(y == 1)
    def _():
        unit_x(down_ref, 1).start()

    bias_x.start()

    @pl.when(z < line - 1)
    def _():
        rows_copy(z, True, True).start()

    @pl.when(z > 0)
    def _():
        rows_copy(z, False, True).start()

    for copy in locals_:
        copy.start()

    for i in reversed(range(line - 1)):
        text_landed(order[i]).wait_recv()
        text_relay(order[i]).start()
    weight_x_in.wait_recv()
    weight_s.start()
    for copy in locals_:
        copy.wait()

    def forward_rows(s):
        @pl.when(z - s >= 0)
        def _():
            rows_landed(z - s).wait_recv()

            @pl.when(z < line - 1)
            def _():
                rows_copy(z - s, True, False).start()

        @pl.when(z + s <= line - 1)
        def _():
            rows_landed(z + s).wait_recv()

            @pl.when(z > 0)
            def _():
                rows_copy(z + s, False, False).start()

    def has_incoming(a):
        return jnp.logical_or(
            jnp.logical_and(a > z, z > 0), jnp.logical_and(a < z, z < line - 1)
        )

    def next_slot(a):
        right = a > z
        to = jnp.where(right, z + 1, z - 1)
        slot = jnp.where(jnp.logical_and(to == a, jnp.logical_not(right)), line, a)
        return to, slot

    def sum_copy(a, c):
        to, slot = next_slot(a)
        return remote(psend.at[a, c], precv.at[slot, c], p_send.at[a, c], p_recv.at[slot, c], along(to))

    def sum_landed(slot, c):
        return remote(precv.at[slot, c], precv.at[slot, c], p_send.at[0, c], p_recv.at[slot, c], other_y)

    tile = 256

    def multiply(a, c, store):
        def body(t, _):
            cols = pl.ds(pl.multiple_of(t * tile, tile), tile)
            total = jnp.dot(tb[a, 0], wb[0, c, :, cols], preferred_element_type=f32)
            total = total + jnp.dot(tb[a, 1], wb[1, c, :, cols], preferred_element_type=f32)
            store(t, cols, total)
            return 0

        lax.fori_loop(0, half_cols // tile, body, 0)

    def product(i, c):
        a = order[i]

        def store(t, cols, total):
            psend[a, c, :, cols] = total.astype(bf16)

        multiply(a, c, store)

        @pl.when(jnp.logical_not(has_incoming(a)))
        def _():
            sum_copy(a, c).start()

    def add_incoming(i, c):
        a = order[i]

        @pl.when(has_incoming(a))
        def _():
            sum_landed(a, c).wait_recv()

            def body(t, _):
                r = pl.ds(pl.multiple_of(t * 16, 16), 16)
                psend[a, c, r] = (psend[a, c, r].astype(f32) + precv[a, c, r].astype(f32)).astype(bf16)
                return 0

            lax.fori_loop(0, text_rows // 16, body, 0)
            sum_copy(a, c).start()

    def products(i):
        text_relayed(order[i]).wait_recv()
        for c in range(2):
            product(i, c)

    weight_s_in.wait_recv()
    products(0)
    forward_rows(1)
    if line > 2:
        products(1)
    unit_x_in.wait_recv()
    unit_s.start()
    unit_y.start()
    for s in range(2, line):
        forward_rows(s)
    for i in range(2, line - 1):
        products(i)
    unit_y_in.wait_recv()
    unit_s2.start()
    for c in range(2):
        add_incoming(0, c)
    bias_x_in.wait_recv()
    unit_s_in.wait_recv()
    unit_s2_in.wait_recv()

    all_rows = line * img

    def up_body(q, _):
        k = q // 2
        at = pl.multiple_of((q % 2) * piece, piece)
        pre[k, pl.ds(at, piece)] = lax.dot_general(
            fb[0, k, pl.ds(at, piece)],
            rows[0].reshape(all_rows, width),
            (((1,), (1,)), ((), ())),
            preferred_element_type=f32,
        )
        return 0

    lax.fori_loop(0, 4, up_body, 0)
    for k in range(2):
        for t in range(units // 128):
            spot = slice(t * 128, (t + 1) * 128)
            bias_col[k, spot] = jnp.transpose(bb[k, :, spot])

    def gelu_body(r, _):
        k = r // (units // 16)
        at = pl.ds(pl.multiple_of((r % (units // 16)) * 16, 16), 16)
        value = pre[k, at] + bias_col[k, at, 0:1]
        phi = 0.5 * (1.0 + lax.erf(value * 0.7071067811865476))
        hid_t[k, at] = (value * phi).astype(bf16)
        pre[k, at] = phi + value * jnp.exp(-0.5 * value * value) * 0.3989422804014327
        return 0

    lax.fori_loop(0, 2 * units // 16, gelu_body, 0)

    def flip_body(t, _):
        for k in range(2):
            at = pl.ds(pl.multiple_of(t * 128, 128), 128)
            hid[k, :, at] = jnp.transpose(hid_t[k, at].astype(f32)).astype(bf16)
        return 0

    lax.fori_loop(0, units // 128, flip_body, 0)

    def down_body(t, _):
        cols = pl.ds(pl.multiple_of(t * tile, tile), tile)
        total = jnp.dot(hid[0], fb[1, 0, :, cols], preferred_element_type=f32)
        po[:, cols] = total + jnp.dot(hid[1], fb[1, 1, :, cols], preferred_element_type=f32)
        return 0

    lax.fori_loop(0, width // tile, down_body, 0)

    def state_copy(a):
        to, slot = next_slot(a)
        return remote(msend.at[a], mrecv.at[slot], m_send.at[a], m_recv.at[slot], along(to))

    def state_landed(slot):
        return remote(mrecv.at[slot], mrecv.at[slot], m_send.at[0], m_recv.at[slot], other_y)

    def send_state(i, first):
        a = order[i]
        waits = has_incoming(a)

        @pl.when(jnp.logical_not(waits) if first else waits)
        def _():
            if not first:
                state_landed(a).wait_recv()

            def body(t, _):
                r = pl.ds(pl.multiple_of(t * 16, 16), 16)
                value = po[pl.ds(pl.multiple_of(a * img + t * 16, 16), 16)]
                if not first:
                    value = value + mrecv[a, r].astype(f32)
                msend[a, r] = value.astype(bf16)
                return 0

            lax.fori_loop(0, img // 16, body, 0)
            state_copy(a).start()

    for i in range(line - 1):
        send_state(i, True)
    for i in range(1, line - 1):
        for c in range(2):
            add_incoming(i, c)
        send_state(i - 1, False)
    send_state(line - 2, False)

    def slope_body(q, _):
        k = q // 2
        at = pl.ds(pl.multiple_of((q % 2) * piece, piece), piece)
        grad = lax.dot_general(
            fb[1, k, at],
            rows[1].reshape(all_rows, width),
            (((1,), (1,)), ((), ())),
            preferred_element_type=f32,
        )
        pg_t[k, at] = (grad * pre[k, at]).astype(bf16)
        return 0

    lax.fori_loop(0, 4, slope_body, 0)

    def terms(kind, k, j, owner):
        at = pl.ds(pl.multiple_of(j * piece + owner * part, part), part)
        left = pg_t if kind == 0 else hid_t
        return jnp.dot(left[k, at], rows[kind].reshape(all_rows, width), preferred_element_type=f32)

    grads_s = remote(gs1, gr1, g_send.at[0], g_recv.at[0], other_g)
    grads_y = remote(gs2, gr2, g_send.at[1], g_recv.at[1], other_y)
    grads_x = remote(gs3, gr3, g_send.at[2], g_recv.at[2], other_x)
    for kind in range(2):

        def body(q, _, kind=kind):
            k, j = q // 2, q % 2
            gs1[kind, k, j] = terms(kind, k, j, 1 - g).astype(bf16)
            return 0

        lax.fori_loop(0, 4, body, 0)
    grads_s.start()
    grads_s.wait_recv()
    for kind in range(2):

        def body(k, _, kind=kind):
            gs2[kind, k] = (terms(kind, k, 1 - y, g) + gr1[kind, k, 1 - y].astype(f32)).astype(bf16)
            return 0

        lax.fori_loop(0, 2, body, 0)
    grads_y.start()

    for c in range(2):

        @pl.when(z > 0)
        def _():
            sum_landed(z, c).wait_recv()

        @pl.when(z < line - 1)
        def _():
            sum_landed(line, c).wait_recv()

        def store(t, cols, total, c=c):
            total = total + jnp.where(z > 0, precv[z, c, :, cols].astype(f32), 0.0)
            total = total + jnp.where(z < line - 1, precv[line, c, :, cols].astype(f32), 0.0)
            for h in range(tile // HD):
                head = total[:, h * HD : (h + 1) * HD]
                scale = lax.rsqrt(jnp.mean(head * head, axis=-1, keepdims=True) + EPSILON)
                at = pl.multiple_of(c * half_cols + t * tile + h * HD, HD)
                query_ref[:, pl.ds(at, HD)] = (head * scale).astype(bf16)

        multiply(z, c, store)

    states_ref[...] = po[pl.ds(pl.multiple_of(z * img, img), img)]

    @pl.when(z > 0)
    def _():
        state_landed(z).wait_recv()
        states_ref[...] += mrecv[z].astype(f32)

    @pl.when(z < line - 1)
    def _():
        state_landed(line).wait_recv()
        states_ref[...] += mrecv[line].astype(f32)

    grads_y.wait_recv()
    for kind in range(2):
        total = terms(kind, 1 - x, y, g) + gr1[kind, 1 - x, y].astype(f32)
        gs3[kind] = (total + gr2[kind, 1 - x].astype(f32)).astype(bf16)
    grads_x.start()
    grads_x.wait_recv()
    for kind, out in ((0, up_grad_ref), (1, down_grad_ref)):
        total = terms(kind, x, y, g) + gr1[kind, x, y].astype(f32)
        out[...] = total + gr2[kind, x].astype(f32) + gr3[kind].astype(f32)

    for i in range(line - 1):
        a = order[i]
        text_copy(i).wait_send()
        text_relay(a).wait_send()
        state_copy(a).wait_send()
        for c in range(2):
            sum_copy(a, c).wait_send()
    for copy in (weight_x, weight_s, unit_s, unit_y, unit_s2, bias_x, grads_s, grads_y, grads_x):
        copy.wait_send()
    unit_x(up_ref, 0).wait_send()

    for a in range(line):

        @pl.when(jnp.logical_and(a <= z, z < line - 1))
        def _():
            rows_copy(a, True, False).wait_send()

        @pl.when(jnp.logical_and(a >= z, z > 0))
        def _():
            rows_copy(a, False, False).wait_send()


def exchange(rows, bias, up, down, text, weight):
    line = lax.axis_size("enc") // 2
    text_rows = text.shape[0]
    depth, columns = weight.shape
    img, width = rows.shape[1:]
    units = up.shape[0]
    half = columns // 2
    f32, bf16 = jnp.float32, jnp.bfloat16
    dma = pltpu.SemaphoreType.DMA
    part = units // 4
    return pl.pallas_call(
        functools.partial(step_kernel, line),
        out_shape=[
            jax.ShapeDtypeStruct((text_rows, columns), bf16),
            jax.ShapeDtypeStruct((img, width), f32),
            jax.ShapeDtypeStruct((part, width), f32),
            jax.ShapeDtypeStruct((part, width), f32),
        ],
        in_specs=[pl.BlockSpec(memory_space=pl.ANY)] * 6,
        out_specs=[pl.BlockSpec(memory_space=pltpu.VMEM)] * 4,
        scratch_shapes=[
            pltpu.VMEM((line, 2, text_rows, depth), bf16),
            pltpu.VMEM((2, 2, depth, half), bf16),
            pltpu.VMEM((2, 2, units, width), bf16),
            pltpu.VMEM((2, 8, units), f32),
            pltpu.VMEM((2, units, 8), f32),
            pltpu.VMEM((2, line, img, width), bf16),
            pltpu.VMEM((2, units, line * img), f32),
            pltpu.VMEM((2, units, line * img), bf16),
            pltpu.VMEM((2, line * img, units), bf16),
            pltpu.VMEM((2, units, line * img), bf16),
            pltpu.VMEM((line * img, width), f32),
            pltpu.VMEM((line, 2, text_rows, half), bf16),
            pltpu.VMEM((line + 1, 2, text_rows, half), bf16),
            pltpu.VMEM((line, img, width), bf16),
            pltpu.VMEM((line + 1, img, width), bf16),
            pltpu.VMEM((2, 2, 2, part, width), bf16),
            pltpu.VMEM((2, 2, 2, part, width), bf16),
            pltpu.VMEM((2, 2, part, width), bf16),
            pltpu.VMEM((2, 2, part, width), bf16),
            pltpu.VMEM((2, part, width), bf16),
            pltpu.VMEM((2, part, width), bf16),
            dma((8,)),
            dma((line - 1,)),
            dma((line,)),
            dma((line + 1,)),
            dma((line + 1,)),
            dma((3,)),
            dma((3,)),
            dma((3,)),
            dma((3,)),
            dma((2, line)),
            dma((line,)),
            dma((line, 2)),
            dma((line + 1, 2)),
            dma((line,)),
            dma((line + 1,)),
            dma((3,)),
            dma((3,)),
        ],
        compiler_params=pltpu.CompilerParams(
            collective_id=0, has_side_effects=True, vmem_limit_bytes=67_000_000
        ),
        name="exchange",
    )(rows, bias, up, down, text, weight)


def attend(queries, keys, values, dec_tiles, links, lengths, slots, patch, length, dec_count):
    samples = links.shape[0]
    img_rows = slots * patch
    tile_index = jnp.arange(slots)
    kv_local, heads_each = queries.shape[2], queries.shape[3]
    live_keys = tile_index[None, :] < dec_tiles[:, None]
    live_keys = jnp.broadcast_to(live_keys[:, :, None], (dec_count, slots, patch)).reshape(
        dec_count, img_rows
    )
    allowed = (links[:, :, None] > 0) & live_keys[None, :, :]
    scores = jnp.einsum(
        "sqghd,jgkd->sghjkq", queries, keys, preferred_element_type=jnp.float32
    ) * HD ** (-0.5)
    weights = jnp.where(allowed[:, None, None, :, :, None], jnp.exp(scores), 0.0)
    totals = jnp.sum(weights, axis=(3, 4), keepdims=True)
    probs = (weights / totals).astype(jnp.bfloat16)
    mixed = jnp.einsum("sghjkq,jgkd->sqghd", probs, values, preferred_element_type=jnp.float32)
    valid = jnp.arange(length)[None, :] < lengths[:, None]
    return (
        jnp.where(valid[:, :, None, None, None], mixed, 0.0)
        .reshape(samples, length, kv_local * heads_each * HD)
        .astype(jnp.bfloat16)
    )


def on_column(
    images,
    ln_gain,
    ln_bias,
    fc1_weight,
    fc1_bias,
    fc2_weight,
    fc2_bias,
    key_weight,
    value_weight,
    text,
    query_weight,
    tiles,
    links,
    lengths,
    state_grads,
):
    dec_count = lax.axis_size("dec")
    enc_place = lax.axis_index("enc")
    dec_place = lax.axis_index("dec")
    grp_place = lax.axis_index("grp")
    slots, patch, width = images.shape[1:]
    img_rows = slots * patch
    samples, length = text.shape[:2]
    own_rows = images.reshape(img_rows, width)
    normed = normalize_layer(own_rows.astype(jnp.float32), ln_gain, ln_bias).astype(jnp.bfloat16)
    own_tiles = tiles[enc_place, dec_place, grp_place]
    own_live = jnp.arange(img_rows)[:, None] // patch < own_tiles
    cotangent = jnp.where(
        own_live, state_grads.reshape(img_rows, width), jnp.zeros((), state_grads.dtype)
    )
    bias = jnp.broadcast_to(fc1_bias[None, :], (8, fc1_bias.shape[0]))
    queries, summed, fc1_grad, fc2_grad = exchange(
        jnp.stack([normed, cotangent]),
        bias,
        fc1_weight,
        fc2_weight,
        text.reshape(samples * length, text.shape[2]),
        query_weight,
    )
    states = (own_rows.astype(jnp.float32) + summed + fc2_bias).astype(jnp.bfloat16)
    local_heads = query_weight.shape[1] // HD
    per_group = HEADS // KV_HEADS
    kv_local = max(1, local_heads // per_group)
    first_head = dec_place * local_heads // per_group
    keys, values = share_keys(states, key_weight, value_weight, first_head, kv_local)
    queries = queries.reshape(samples, length, kv_local, local_heads // kv_local, HD)
    context = attend(
        queries, keys, values, tiles[enc_place, :, grp_place], links, lengths, slots, patch, length, dec_count
    )
    return (context, fc1_grad, fc2_grad)


def on_device(
    images,
    ln_gain,
    ln_bias,
    fc1_weight,
    fc1_bias,
    fc2_weight,
    fc2_bias,
    key_weight,
    value_weight,
    text,
    query_weight,
    tiles,
    links,
    lengths,
    state_grads,
):
    dec_count = lax.axis_size("dec")
    grp_count = lax.axis_size("grp")
    enc_place = lax.axis_index("enc")
    dec_place = lax.axis_index("dec")
    grp_place = lax.axis_index("grp")
    slots = images.shape[1]
    patch = images.shape[2]
    width = images.shape[3]
    img_rows = slots * patch
    own_rows = images.reshape(img_rows, width)
    normed = normalize_layer(own_rows.astype(jnp.float32), ln_gain, ln_bias).astype(jnp.bfloat16)
    samples = text.shape[0]
    length = text.shape[1]
    text_rows = text.reshape(samples * length, text.shape[2])
    half = query_weight.shape[1] // grp_count
    own_half = lax.dynamic_slice_in_dim(query_weight, grp_place * half, half, 1)
    own_tiles = tiles[enc_place, dec_place, grp_place]
    tile_index = jnp.arange(slots)
    own_live = jnp.broadcast_to((tile_index < own_tiles)[:, None, None], (slots, patch, 1)).reshape(
        img_rows, 1
    )
    cotangent = jnp.where(
        own_live, state_grads.reshape(img_rows, width), jnp.zeros((), state_grads.dtype)
    )
    sent = jnp.stack([normed, cotangent])
    text_rows, own_half, _ = lax.optimization_barrier((text_rows, own_half, sent))
    both = lax.all_gather(sent, "enc", axis=1, tiled=True)
    gathered, all_cotangent = both[0], both[1]
    text_blocks = share_text(text_rows)
    pre, hidden, partial_full = encoder_rows(gathered, fc1_weight, fc1_bias, fc2_weight)
    partial_full = partial_full.astype(jnp.bfloat16)
    all_cotangent, _ = lax.optimization_barrier((all_cotangent, partial_full))
    first_term, second_term = weight_terms(gathered, pre, hidden, all_cotangent, fc2_weight)
    queries_of = project_queries(text_blocks, own_half, second_term)
    summed = lax.psum_scatter(
        partial_full, "enc", scatter_dimension=0, tiled=True
    ).astype(jnp.float32)
    states = (own_rows.astype(jnp.float32) + summed + fc2_bias).astype(jnp.bfloat16)
    local_heads = query_weight.shape[1] // HD
    per_group = HEADS // KV_HEADS
    kv_local = max(1, local_heads // per_group)
    first_head = dec_place * local_heads // per_group
    keys, values = share_keys(states, key_weight, value_weight, first_head, kv_local)
    heads_each = local_heads // kv_local
    queries = queries_of
    queries = queries.reshape(samples, length, kv_local, heads_each, HD)
    dec_tiles = tiles[enc_place, :, grp_place]
    live_keys = tile_index[None, :] < dec_tiles[:, None]
    live_keys = jnp.broadcast_to(live_keys[:, :, None], (dec_count, slots, patch)).reshape(
        dec_count, img_rows
    )
    allowed = (links[:, :, None] > 0) & live_keys[None, :, :]
    scores = jnp.einsum(
        "sqghd,jgkd->sghjkq", queries, keys, preferred_element_type=jnp.float32
    ) * HD ** (-0.5)
    weights = jnp.where(allowed[:, None, None, :, :, None], jnp.exp(scores), 0.0)
    totals = jnp.sum(weights, axis=(3, 4), keepdims=True)
    probs = (weights / totals).astype(jnp.bfloat16)
    mixed = jnp.einsum("sghjkq,jgkd->sqghd", probs, values, preferred_element_type=jnp.float32)
    valid = jnp.arange(length)[None, :] < lengths[:, None]
    context = (
        jnp.where(valid[:, :, None, None, None], mixed, 0.0)
        .reshape(samples, length, local_heads * HD)
        .astype(jnp.bfloat16)
    )
    fc1_grad, fc2_grad = share_grads(jnp.stack([first_term, second_term]))
    return (context, fc1_grad, fc2_grad)


def solution(mesh):
    in_specs = (
        P(("enc", "dec", "grp"), None, None, None),
        P(),
        P(),
        P("enc", None),
        P("enc"),
        P("enc", None),
        P(),
        P(),
        P(),
        P(("enc", "grp"), None, None),
        P("enc", "dec"),
        P(),
        P(("enc", "grp"), None),
        P(("enc", "grp")),
        P(("enc", "dec", "grp"), None, None, None),
    )
    out_specs = (
        P(("enc", "grp"), None, "dec"),
        P(("enc", "dec", "grp"), None),
        P(("enc", "dec", "grp"), None),
    )
    paired = mesh.shape["dec"] == 2 and mesh.shape["grp"] == 2 and mesh.shape["enc"] % 2 == 0
    if paired and mesh.shape["enc"] > 2:
        return jax.shard_map(
            on_column, mesh=mesh, in_specs=in_specs, out_specs=out_specs, check_vma=False
        )
    return jax.shard_map(
        on_device, mesh=mesh, in_specs=in_specs, out_specs=out_specs, check_vma=False
    )
```

```python
import functools

import jax
import jax.numpy as jnp
from jax import lax
from jax.experimental import pallas as pl
from jax.experimental.pallas import tpu as pltpu
from jax.sharding import PartitionSpec as P


HEADS = 32
KV_HEADS = 4
HD = 128


EPSILON = 1e-06


def normalize_layer(values, gain, shift):
    middle = jnp.mean(values, axis=-1, keepdims=True)
    centered = values - middle
    spread = jnp.mean(centered * centered, axis=-1, keepdims=True)
    return centered * lax.rsqrt(spread + EPSILON) * gain + shift


def normalize_heads(values):
    return values * lax.rsqrt(jnp.mean(values * values, axis=-1, keepdims=True) + EPSILON)


def gelu_slope(values):
    return (
        0.5 * (1.0 + lax.erf(values * 0.7071067811865476))
        + values * jnp.exp(-0.5 * values * values) * 0.3989422804014327
    )


def encoder_rows(rows, fc1_weight, fc1_bias, fc2_weight):
    pre = (
        lax.dot_general(
            rows, fc1_weight, (((1,), (1,)), ((), ())), preferred_element_type=jnp.float32
        )
        + fc1_bias
    )
    hidden = jax.nn.gelu(pre, approximate=False).astype(jnp.bfloat16)
    partial_sum = jnp.dot(hidden, fc2_weight, preferred_element_type=jnp.float32)
    return (pre, hidden, partial_sum)


def weight_terms(rows, pre, hidden, cotangent, fc2_weight):
    hidden_grad = lax.dot_general(
        cotangent, fc2_weight, (((1,), (1,)), ((), ())), preferred_element_type=jnp.float32
    )
    second_term = lax.dot_general(
        hidden, cotangent, (((0,), (0,)), ((), ())), preferred_element_type=jnp.float32
    )
    pre_grad = (hidden_grad * gelu_slope(pre)).astype(jnp.bfloat16)
    first_term = lax.dot_general(
        pre_grad, rows, (((0,), (0,)), ((), ())), preferred_element_type=jnp.float32
    )
    return (first_term, second_term)


def project_heads(states, key_columns, value_columns, heads):
    width = states.shape[-1]
    key_raw = jnp.einsum(
        "rd,dhe->hre",
        states,
        key_columns.reshape(width, heads, HD),
        preferred_element_type=jnp.float32,
    )
    keys = normalize_heads(key_raw).astype(jnp.bfloat16)
    values = jnp.einsum(
        "rd,dhe->hre",
        states,
        value_columns.reshape(width, heads, HD),
        preferred_element_type=jnp.float32,
    ).astype(jnp.bfloat16)
    return (keys, values)


def shifted(values, axis, step):
    size = lax.axis_size(axis)
    return lax.ppermute(values, axis, [(i, (i + step) % size) for i in range(size)])


def swapped(values):
    return lax.ppermute(values, "enc", [(i, i ^ 1) for i in range(lax.axis_size("enc"))])


def share_text(text_rows):
    enc_count = lax.axis_size("enc")
    _, depth = text_rows.shape
    side = lax.axis_index("enc") % 2
    block = depth // enc_count
    even = jnp.stack([text_rows[:, i * block : (i + 1) * block] for i in range(0, enc_count, 2)])
    odd = jnp.stack([text_rows[:, i * block : (i + 1) * block] for i in range(1, enc_count, 2)])
    own = jnp.where(side == 0, even, odd)
    away = jnp.where(side == 0, odd, even)
    arrived = swapped(away)
    pair = jnp.concatenate([arrived, own], axis=1)
    return jnp.concatenate(
        [pair] + [shifted(pair, "grp", step) for step in range(1, lax.axis_size("grp"))], axis=1
    )


def project_queries(text_blocks, weight, before):
    grp_count = lax.axis_size("grp")
    ring = lax.axis_size("enc") // 2
    enc_count = lax.axis_size("enc")
    place = lax.axis_index("enc") // 2
    total = None
    for step in range(ring):
        if step == max(0, ring - 2):
            weight, _ = lax.optimization_barrier((weight, before))
        left = lax.dynamic_index_in_dim(text_blocks, (place - step) % ring, 0, keepdims=False)
        term = jnp.dot(left, weight, preferred_element_type=jnp.float32)
        total = term if total is None else total + term
        if step < ring - 1:
            weight = lax.ppermute(
                weight, "enc", [(i, (i + 2) % enc_count) for i in range(enc_count)]
            )
    columns = total.shape[1]
    total = total.reshape(grp_count, 2, -1, columns)
    arrived = swapped(total[:, 0].astype(jnp.bfloat16))
    raw = total[:, 1] + arrived.astype(jnp.float32)
    own = normalize_heads(raw.reshape(grp_count, -1, columns // HD, HD)).astype(jnp.bfloat16)
    blocks = jnp.stack(
        [own[0]] + [shifted(own[step], "grp", -step) for step in range(1, grp_count)], axis=1
    )
    start = (grp_count - lax.axis_index("grp")) % grp_count
    blocks = lax.dynamic_slice_in_dim(
        jnp.concatenate([blocks, blocks], axis=1), start, grp_count, 1
    )
    return blocks.reshape(blocks.shape[0], grp_count * columns)


def share_keys(states, key_weight, value_weight, first_head, kv_local):
    dec_count = lax.axis_size("dec")
    rows, _ = states.shape
    if dec_count == 2 and kv_local * dec_count == KV_HEADS:
        keys, values = project_heads(states, key_weight, value_weight, KV_HEADS)
        paired = jnp.stack([keys, values])
        own = lax.dynamic_slice_in_dim(paired, first_head, kv_local, 1)
        away = lax.dynamic_slice_in_dim(paired, KV_HEADS - kv_local - first_head, kv_local, 1)
        arrived = shifted(away, "dec", 1)
        first = lax.axis_index("dec") == 0
        paired = jnp.stack(
            [jnp.where(first, own, arrived), jnp.where(first, arrived, own)], axis=1
        )
        return (paired[0], paired[1])
    key_columns = lax.dynamic_slice_in_dim(key_weight, first_head * HD, kv_local * HD, 1)
    value_columns = lax.dynamic_slice_in_dim(value_weight, first_head * HD, kv_local * HD, 1)
    piece = lax.all_gather(states, "dec", axis=0, tiled=True)
    key_part, value_part = project_heads(piece, key_columns, value_columns, kv_local)
    shape = (kv_local, dec_count, rows, HD)
    return (
        key_part.reshape(shape).transpose(1, 0, 2, 3),
        value_part.reshape(shape).transpose(1, 0, 2, 3),
    )


def share_grads(terms):
    dec_count = lax.axis_size("dec")
    grp_count = lax.axis_size("grp")
    rows = terms.shape[1] // (dec_count * grp_count)
    if dec_count == 2 and grp_count == 2:
        parts = terms.reshape(2, dec_count, grp_count, rows, -1)
        grp_place = lax.axis_index("grp")
        dec_place = lax.axis_index("dec")
        kept = lax.dynamic_index_in_dim(parts, grp_place, 2, keepdims=False)
        away = lax.dynamic_index_in_dim(parts, 1 - grp_place, 2, keepdims=False)
        kept = kept + shifted(away.astype(jnp.bfloat16), "grp", 1).astype(jnp.float32)
        away = lax.dynamic_index_in_dim(kept, 1 - dec_place, 1, keepdims=False)
        kept = lax.dynamic_index_in_dim(kept, dec_place, 1, keepdims=False)
        kept = kept + shifted(away.astype(jnp.bfloat16), "dec", 1).astype(jnp.float32)
        return (kept[0], kept[1])
    summed = lax.psum_scatter(
        terms.astype(jnp.bfloat16), ("dec", "grp"), scatter_dimension=1, tiled=True
    ).astype(jnp.float32)
    return (summed[0], summed[1])


MESH = pl.DeviceIdType.MESH


def pick(table, place):
    return sum(jnp.where(place == i, value, 0) for i, value in enumerate(table))


def step_kernel(
    line,
    rows_ref,
    bias_ref,
    up_ref,
    down_ref,
    text_ref,
    weight_ref,
    query_ref,
    states_ref,
    up_grad_ref,
    down_grad_ref,
    tb,
    wb,
    fb,
    bb,
    bias_col,
    rows,
    pre,
    hid_t,
    hid,
    pg_t,
    po,
    psend,
    precv,
    msend,
    mrecv,
    gs1,
    gr1,
    gs2,
    gr2,
    gs3,
    gr3,
    local_sem,
    t_send,
    t_recv,
    y_send,
    y_recv,
    x_send,
    x_recv,
    s_send,
    s_recv,
    a_send,
    a_recv,
    p_send,
    p_recv,
    m_send,
    m_recv,
    g_send,
    g_recv,
):
    f32 = jnp.float32
    bf16 = jnp.bfloat16
    enc = lax.axis_index("enc")
    y = lax.axis_index("dec")
    g = lax.axis_index("grp")
    z, x = enc // 2, enc % 2
    other_x = ((z * 2 + 1 - x), y, g)
    other_y = (enc, 1 - y, g)
    other_g = (enc, y, 1 - g)

    def along(place):
        return (place * 2 + x, y, g)

    orders, nearest = [], []
    for p in range(line):
        others = [a for a in range(line) if a != p]
        others.sort(key=lambda a: (-abs(a - p), min(a, line - 1 - a)))
        nearest.append(others[::-1])
        orders.append(others[-1:] + others[:-1] if p in (0, line - 1) else others)
    order = [pick([orders[p][i] for p in range(line)], z) for i in range(line - 1)]
    near = [pick([nearest[p][i] for p in range(line)], z) for i in range(line - 1)]
    text_rows, depth = tb.shape[2], tb.shape[3]
    half_cols = wb.shape[3]
    img = rows.shape[2]
    width = rows.shape[3]
    units = fb.shape[2]
    piece = units // 2
    part = units // 4

    barrier = pltpu.get_barrier_semaphore()
    for k in range(line):

        @pl.when(z != k)
        def _():
            pl.semaphore_signal(barrier, inc=1, device_id=along(k), device_id_type=MESH)

    for to in (other_x, other_y, other_g):
        pl.semaphore_signal(barrier, inc=1, device_id=to, device_id_type=MESH)
    pl.semaphore_wait(barrier, line + 2)

    def remote(src, dst, send, recv, to):
        return pltpu.make_async_remote_copy(
            src_ref=src, dst_ref=dst, send_sem=send, recv_sem=recv, device_id=to, device_id_type=MESH
        )

    def text_copy(i):
        b = near[i]
        at = pl.multiple_of((b * 2 + y) * depth, depth)
        return remote(
            text_ref.at[:, pl.ds(at, depth)], tb.at[z, y], t_send.at[i], t_recv.at[z], along(b)
        )

    def text_landed(a):
        return remote(tb.at[a, y], tb.at[a, y], t_send.at[0], t_recv.at[a], other_y)

    def text_relay(a):
        return remote(tb.at[a, y], tb.at[a, y], y_send.at[a], y_recv.at[a], other_y)

    def text_relayed(a):
        return remote(tb.at[a, 1 - y], tb.at[a, 1 - y], y_send.at[a], y_recv.at[a], other_y)

    weight_x = remote(
        weight_ref.at[:, pl.ds(pl.multiple_of(g * half_cols, half_cols), half_cols)],
        wb.at[x, g],
        x_send.at[0],
        x_recv.at[0],
        other_x,
    )
    weight_x_in = remote(wb.at[1 - x, g], wb.at[1 - x, g], x_send.at[0], x_recv.at[0], other_x)
    weight_s = remote(wb.at[1 - x, g], wb.at[1 - x, g], s_send.at[0], s_recv.at[0], other_g)
    weight_s_in = remote(wb.at[1 - x, 1 - g], wb.at[1 - x, 1 - g], s_send.at[0], s_recv.at[0], other_g)

    piece_at = pl.multiple_of(g * piece, piece)
    away_at = pl.multiple_of((1 - g) * piece, piece)

    def unit_x(ref, kind):
        return remote(
            ref.at[pl.ds(piece_at, piece)],
            fb.at[kind, x, pl.ds(piece_at, piece)],
            x_send.at[1],
            x_recv.at[1],
            other_x,
        )

    mine = fb.at[y, 1 - x, pl.ds(piece_at, piece)]
    unit_x_in = remote(mine, mine, x_send.at[1], x_recv.at[1], other_x)
    unit_s = remote(mine, mine, s_send.at[1], s_recv.at[1], other_g)
    unit_s_spot = fb.at[y, 1 - x, pl.ds(away_at, piece)]
    unit_s_in = remote(unit_s_spot, unit_s_spot, s_send.at[1], s_recv.at[1], other_g)
    unit_y = remote(mine, mine, y_send.at[line], y_recv.at[line], other_y)
    crossed = fb.at[1 - y, 1 - x, pl.ds(piece_at, piece)]
    unit_y_in = remote(crossed, crossed, y_send.at[line], y_recv.at[line], other_y)
    unit_s2 = remote(crossed, crossed, s_send.at[2], s_recv.at[2], other_g)
    unit_s2_spot = fb.at[1 - y, 1 - x, pl.ds(away_at, piece)]
    unit_s2_in = remote(unit_s2_spot, unit_s2_spot, s_send.at[2], s_recv.at[2], other_g)
    bias_x = remote(bias_ref, bb.at[x], x_send.at[2], x_recv.at[2], other_x)
    bias_x_in = remote(bb.at[1 - x], bb.at[1 - x], x_send.at[2], x_recv.at[2], other_x)

    def rows_copy(a, right, own):
        to = along(z + 1) if right else along(z - 1)
        src = rows_ref if own else rows.at[:, a]
        return remote(src, rows.at[:, a], a_send.at[1 if right else 0, a], a_recv.at[a], to)

    def rows_landed(a):
        return remote(rows.at[:, a], rows.at[:, a], a_send.at[0, a], a_recv.at[a], other_y)

    locals_ = [
        pltpu.make_async_copy(weight_ref.at[:, pl.ds(c * half_cols, half_cols)], wb.at[x, c], local_sem.at[c])
        for c in range(2)
    ] + [
        pltpu.make_async_copy(up_ref, fb.at[0, x], local_sem.at[2]),
        pltpu.make_async_copy(down_ref, fb.at[1, x], local_sem.at[3]),
        pltpu.make_async_copy(bias_ref, bb.at[x], local_sem.at[4]),
        pltpu.make_async_copy(rows_ref, rows.at[:, z], local_sem.at[5]),
    ] + [
        pltpu.make_async_copy(
            text_ref.at[:, pl.ds(pl.multiple_of((z * 2 + h) * depth, depth), depth)],
            tb.at[z, h],
            local_sem.at[6 + h],
        )
        for h in range(2)
    ]

    for i in range(line - 1):
        text_copy(i).start()
    weight_x.start()

    @pl.when(z < line - 1)
    def _():
        rows_copy(z, True, True).start()

    @pl.when(z > 0)
    def _():
        rows_copy(z, False, True).start()

    for copy in locals_:
        copy.start()

    for i in range(line - 1):
        text_landed(near[i]).wait_recv()
        text_relay(near[i]).start()
    weight_x_in.wait_recv()
    weight_s.start()
    weight_x.wait_send()

    @pl.when(y == 0)
    def _():
        unit_x(up_ref, 0).start()

    @pl.when(y == 1)
    def _():
        unit_x(down_ref, 1).start()

    bias_x.start()
    for copy in locals_:
        copy.wait()

    def forward_rows(s):
        @pl.when(z - s >= 0)
        def _():
            rows_landed(z - s).wait_recv()

            @pl.when(z < line - 1)
            def _():
                rows_copy(z - s, True, False).start()

        @pl.when(z + s <= line - 1)
        def _():
            rows_landed(z + s).wait_recv()

            @pl.when(z > 0)
            def _():
                rows_copy(z + s, False, False).start()

    def has_incoming(a):
        return jnp.logical_or(
            jnp.logical_and(a > z, z > 0), jnp.logical_and(a < z, z < line - 1)
        )

    def next_slot(a):
        right = a > z
        to = jnp.where(right, z + 1, z - 1)
        slot = jnp.where(jnp.logical_and(to == a, jnp.logical_not(right)), line, a)
        return to, slot

    def sum_copy(a, c):
        to, slot = next_slot(a)
        return remote(psend.at[a, c], precv.at[slot, c], p_send.at[a, c], p_recv.at[slot, c], along(to))

    def sum_landed(slot, c):
        return remote(precv.at[slot, c], precv.at[slot, c], p_send.at[0, c], p_recv.at[slot, c], other_y)

    tile = 256

    def multiply(a, c, store):
        def body(t, _):
            cols = pl.ds(pl.multiple_of(t * tile, tile), tile)
            total = jnp.dot(tb[a, 0], wb[0, c, :, cols], preferred_element_type=f32)
            total = total + jnp.dot(tb[a, 1], wb[1, c, :, cols], preferred_element_type=f32)
            store(t, cols, total)
            return 0

        lax.fori_loop(0, half_cols // tile, body, 0)

    def product(i, c):
        a = order[i]

        def store(t, cols, total):
            psend[a, c, :, cols] = total.astype(bf16)

        multiply(a, c, store)

    def send_product(i, c):
        a = order[i]

        @pl.when(jnp.logical_not(has_incoming(a)))
        def _():
            sum_copy(a, c).start()

    def add_incoming(i, c):
        a = order[i]

        @pl.when(has_incoming(a))
        def _():
            sum_landed(a, c).wait_recv()

            def body(t, _):
                r = pl.ds(pl.multiple_of(t * 16, 16), 16)
                psend[a, c, r] = (psend[a, c, r].astype(f32) + precv[a, c, r].astype(f32)).astype(bf16)
                return 0

            lax.fori_loop(0, text_rows // 16, body, 0)
            sum_copy(a, c).start()

    held = ((line - 2, 1),)

    def products(i):
        text_relayed(order[i]).wait_recv()
        for c in range(2):
            product(i, c)
            if (i, c) not in held:
                send_product(i, c)

    weight_s_in.wait_recv()
    products(0)
    forward_rows(1)
    unit_x_in.wait_recv()
    unit_s.start()
    unit_y.start()
    for i in range(1, line - 1):
        products(i)
    for s in range(2, line):
        forward_rows(s)
    unit_y_in.wait_recv()
    unit_s2.start()
    bias_x_in.wait_recv()
    unit_s_in.wait_recv()
    unit_s2_in.wait_recv()

    all_rows = line * img

    def up_body(q, _):
        k = q // 2
        at = pl.multiple_of((q % 2) * piece, piece)
        pre[k, pl.ds(at, piece)] = lax.dot_general(
            fb[0, k, pl.ds(at, piece)],
            rows[0].reshape(all_rows, width),
            (((1,), (1,)), ((), ())),
            preferred_element_type=f32,
        )
        return 0

    lax.fori_loop(0, 4, up_body, 0)
    for k in range(2):
        for t in range(units // 128):
            spot = slice(t * 128, (t + 1) * 128)
            bias_col[k, spot] = jnp.transpose(bb[k, :, spot])

    def gelu_body(r, _):
        k = r // (units // 16)
        at = pl.ds(pl.multiple_of((r % (units // 16)) * 16, 16), 16)
        value = pre[k, at] + bias_col[k, at, 0:1]
        phi = 0.5 * (1.0 + lax.erf(value * 0.7071067811865476))
        hid_t[k, at] = (value * phi).astype(bf16)
        pre[k, at] = phi + value * jnp.exp(-0.5 * value * value) * 0.3989422804014327
        return 0

    lax.fori_loop(0, 2 * units // 16, gelu_body, 0)
    add_incoming(0, 0)

    def flip_body(t, _):
        for k in range(2):
            at = pl.ds(pl.multiple_of(t * 128, 128), 128)
            hid[k, :, at] = jnp.transpose(hid_t[k, at].astype(f32)).astype(bf16)
        return 0

    lax.fori_loop(0, units // 128, flip_body, 0)

    def down_body(t, _):
        cols = pl.ds(pl.multiple_of(t * tile, tile), tile)
        total = jnp.dot(hid[0], fb[1, 0, :, cols], preferred_element_type=f32)
        po[:, cols] = total + jnp.dot(hid[1], fb[1, 1, :, cols], preferred_element_type=f32)
        return 0

    lax.fori_loop(0, width // tile, down_body, 0)

    def state_copy(a):
        to, slot = next_slot(a)
        return remote(msend.at[a], mrecv.at[slot], m_send.at[a], m_recv.at[slot], along(to))

    def state_landed(slot):
        return remote(mrecv.at[slot], mrecv.at[slot], m_send.at[0], m_recv.at[slot], other_y)

    def send_state(i, first):
        a = order[i]
        waits = has_incoming(a)

        @pl.when(jnp.logical_not(waits) if first else waits)
        def _():
            if not first:
                state_landed(a).wait_recv()

            def body(t, _):
                r = pl.ds(pl.multiple_of(t * 16, 16), 16)
                value = po[pl.ds(pl.multiple_of(a * img + t * 16, 16), 16)]
                if not first:
                    value = value + mrecv[a, r].astype(f32)
                msend[a, r] = value.astype(bf16)
                return 0

            lax.fori_loop(0, img // 16, body, 0)
            state_copy(a).start()

    for i in range(1, line - 1):
        send_state(i, True)
    send_product(line - 2, 1)
    send_state(0, True)

    def terms(kind, k, j, owner):
        at = pl.ds(pl.multiple_of(j * piece + owner * part, part), part)
        left = pg_t if kind == 0 else hid_t
        return jnp.dot(left[k, at], rows[kind].reshape(all_rows, width), preferred_element_type=f32)

    grads_s = [remote(gs1.at[m], gr1.at[m], g_send.at[m], g_recv.at[m], other_g) for m in range(2)]
    grads_y = remote(gs2.at[0], gr2.at[0], g_send.at[2], g_recv.at[2], other_y)
    grads_x = remote(gs2.at[1], gr2.at[1], g_send.at[3], g_recv.at[3], other_x)
    grads_x2 = remote(gs3.at[0], gr3.at[0], g_send.at[4], g_recv.at[4], other_x)
    grads_y2 = remote(gs3.at[1], gr3.at[1], g_send.at[5], g_recv.at[5], other_y)

    def share_core(kind):
        def body(q, _):
            k, j = q // 2, q % 2
            gs1[kind, k, j] = terms(kind, k, j, 1 - g).astype(bf16)
            return 0

        lax.fori_loop(0, 4, body, 0)
        grads_s[kind].start()

    share_core(1)

    def slope_body(q, _):
        k = q // 2
        at = pl.ds(pl.multiple_of((q % 2) * piece, piece), piece)
        grad = lax.dot_general(
            fb[1, k, at],
            rows[1].reshape(all_rows, width),
            (((1,), (1,)), ((), ())),
            preferred_element_type=f32,
        )
        pg_t[k, at] = (grad * pre[k, at]).astype(bf16)
        return 0

    lax.fori_loop(0, 4, slope_body, 0)
    share_core(0)
    add_incoming(0, 1)

    grads_s[1].wait_recv()

    def away_x(j, _):
        gs2[1, j] = (terms(1, 1 - x, j, g) + gr1[1, 1 - x, j].astype(f32)).astype(bf16)
        return 0

    lax.fori_loop(0, 2, away_x, 0)
    grads_x.start()
    grads_s[0].wait_recv()

    def away_y(k, _):
        gs2[0, k] = (terms(0, k, 1 - y, g) + gr1[0, k, 1 - y].astype(f32)).astype(bf16)
        return 0

    lax.fori_loop(0, 2, away_y, 0)
    grads_y.start()
    for i in range(1, line - 1):
        add_incoming(i, 0)
    for i in range(1, line - 2):
        add_incoming(i, 1)
    for i in range(line - 1):
        send_state(i, False)
    add_incoming(line - 2, 1)
    grads_x.wait_recv()
    total = terms(1, x, 1 - y, g) + gr1[1, x, 1 - y].astype(f32)
    gs3[1] = (total + gr2[1, 1 - y].astype(f32)).astype(bf16)
    grads_y2.start()
    grads_y.wait_recv()
    total = terms(0, 1 - x, y, g) + gr1[0, 1 - x, y].astype(f32)
    gs3[0] = (total + gr2[0, 1 - x].astype(f32)).astype(bf16)
    grads_x2.start()

    for c in range(2):

        @pl.when(z > 0)
        def _():
            sum_landed(z, c).wait_recv()

        @pl.when(z < line - 1)
        def _():
            sum_landed(line, c).wait_recv()

        def store(t, cols, total, c=c):
            total = total + jnp.where(z > 0, precv[z, c, :, cols].astype(f32), 0.0)
            total = total + jnp.where(z < line - 1, precv[line, c, :, cols].astype(f32), 0.0)
            for h in range(tile // HD):
                head = total[:, h * HD : (h + 1) * HD]
                scale = lax.rsqrt(jnp.mean(head * head, axis=-1, keepdims=True) + EPSILON)
                at = pl.multiple_of(c * half_cols + t * tile + h * HD, HD)
                query_ref[:, pl.ds(at, HD)] = (head * scale).astype(bf16)

        multiply(z, c, store)

    states_ref[...] = po[pl.ds(pl.multiple_of(z * img, img), img)]

    @pl.when(z > 0)
    def _():
        state_landed(z).wait_recv()
        states_ref[...] += mrecv[z].astype(f32)

    @pl.when(z < line - 1)
    def _():
        state_landed(line).wait_recv()
        states_ref[...] += mrecv[line].astype(f32)

    for kind, out in ((1, down_grad_ref), (0, up_grad_ref)):
        (grads_x2, grads_y2)[kind].wait_recv()
        total = terms(kind, x, y, g) + gr1[kind, x, y].astype(f32)
        total = total + gr2[kind, (x, y)[kind]].astype(f32)
        out[...] = total + gr3[kind].astype(f32)

    for i in range(line - 1):
        a = order[i]
        text_copy(i).wait_send()
        text_relay(a).wait_send()
        state_copy(a).wait_send()
        for c in range(2):
            sum_copy(a, c).wait_send()
    for copy in (weight_s, unit_s, unit_y, unit_s2, bias_x, *grads_s, grads_y, grads_x, grads_x2, grads_y2):
        copy.wait_send()
    unit_x(up_ref, 0).wait_send()

    for a in range(line):

        @pl.when(jnp.logical_and(a <= z, z < line - 1))
        def _():
            rows_copy(a, True, False).wait_send()

        @pl.when(jnp.logical_and(a >= z, z > 0))
        def _():
            rows_copy(a, False, False).wait_send()


def exchange(rows, bias, up, down, text, weight):
    line = lax.axis_size("enc") // 2
    text_rows = text.shape[0]
    depth, columns = weight.shape
    img, width = rows.shape[1:]
    units = up.shape[0]
    half = columns // 2
    f32, bf16 = jnp.float32, jnp.bfloat16
    dma = pltpu.SemaphoreType.DMA
    part = units // 4
    return pl.pallas_call(
        functools.partial(step_kernel, line),
        out_shape=[
            jax.ShapeDtypeStruct((text_rows, columns), bf16),
            jax.ShapeDtypeStruct((img, width), f32),
            jax.ShapeDtypeStruct((part, width), f32),
            jax.ShapeDtypeStruct((part, width), f32),
        ],
        in_specs=[pl.BlockSpec(memory_space=pl.ANY)] * 6,
        out_specs=[pl.BlockSpec(memory_space=pltpu.VMEM)] * 4,
        scratch_shapes=[
            pltpu.VMEM((line, 2, text_rows, depth), bf16),
            pltpu.VMEM((2, 2, depth, half), bf16),
            pltpu.VMEM((2, 2, units, width), bf16),
            pltpu.VMEM((2, 8, units), f32),
            pltpu.VMEM((2, units, 8), f32),
            pltpu.VMEM((2, line, img, width), bf16),
            pltpu.VMEM((2, units, line * img), f32),
            pltpu.VMEM((2, units, line * img), bf16),
            pltpu.VMEM((2, line * img, units), bf16),
            pltpu.VMEM((2, units, line * img), bf16),
            pltpu.VMEM((line * img, width), f32),
            pltpu.VMEM((line, 2, text_rows, half), bf16),
            pltpu.VMEM((line + 1, 2, text_rows, half), bf16),
            pltpu.VMEM((line, img, width), bf16),
            pltpu.VMEM((line + 1, img, width), bf16),
            pltpu.VMEM((2, 2, 2, part, width), bf16),
            pltpu.VMEM((2, 2, 2, part, width), bf16),
            pltpu.VMEM((2, 2, part, width), bf16),
            pltpu.VMEM((2, 2, part, width), bf16),
            pltpu.VMEM((2, part, width), bf16),
            pltpu.VMEM((2, part, width), bf16),
            dma((8,)),
            dma((line - 1,)),
            dma((line,)),
            dma((line + 1,)),
            dma((line + 1,)),
            dma((3,)),
            dma((3,)),
            dma((3,)),
            dma((3,)),
            dma((2, line)),
            dma((line,)),
            dma((line, 2)),
            dma((line + 1, 2)),
            dma((line,)),
            dma((line + 1,)),
            dma((6,)),
            dma((6,)),
        ],
        compiler_params=pltpu.CompilerParams(
            collective_id=0, has_side_effects=True, vmem_limit_bytes=67_000_000
        ),
        name="exchange",
    )(rows, bias, up, down, text, weight)


def attend(queries, keys, values, dec_tiles, links, lengths, slots, patch, length, dec_count):
    samples = links.shape[0]
    img_rows = slots * patch
    tile_index = jnp.arange(slots)
    kv_local, heads_each = queries.shape[2], queries.shape[3]
    live_keys = tile_index[None, :] < dec_tiles[:, None]
    live_keys = jnp.broadcast_to(live_keys[:, :, None], (dec_count, slots, patch)).reshape(
        dec_count, img_rows
    )
    allowed = (links[:, :, None] > 0) & live_keys[None, :, :]
    scores = jnp.einsum(
        "sqghd,jgkd->sghjkq", queries, keys, preferred_element_type=jnp.float32
    ) * HD ** (-0.5)
    weights = jnp.where(allowed[:, None, None, :, :, None], jnp.exp(scores), 0.0)
    totals = jnp.sum(weights, axis=(3, 4), keepdims=True)
    probs = (weights / totals).astype(jnp.bfloat16)
    mixed = jnp.einsum("sghjkq,jgkd->sqghd", probs, values, preferred_element_type=jnp.float32)
    valid = jnp.arange(length)[None, :] < lengths[:, None]
    return (
        jnp.where(valid[:, :, None, None, None], mixed, 0.0)
        .reshape(samples, length, kv_local * heads_each * HD)
        .astype(jnp.bfloat16)
    )


def on_column(
    images,
    ln_gain,
    ln_bias,
    fc1_weight,
    fc1_bias,
    fc2_weight,
    fc2_bias,
    key_weight,
    value_weight,
    text,
    query_weight,
    tiles,
    links,
    lengths,
    state_grads,
):
    dec_count = lax.axis_size("dec")
    enc_place = lax.axis_index("enc")
    dec_place = lax.axis_index("dec")
    grp_place = lax.axis_index("grp")
    slots, patch, width = images.shape[1:]
    img_rows = slots * patch
    samples, length = text.shape[:2]
    own_rows = images.reshape(img_rows, width)
    normed = normalize_layer(own_rows.astype(jnp.float32), ln_gain, ln_bias).astype(jnp.bfloat16)
    own_tiles = tiles[enc_place, dec_place, grp_place]
    own_live = jnp.arange(img_rows)[:, None] // patch < own_tiles
    cotangent = jnp.where(
        own_live, state_grads.reshape(img_rows, width), jnp.zeros((), state_grads.dtype)
    )
    bias = jnp.broadcast_to(fc1_bias[None, :], (8, fc1_bias.shape[0]))
    queries, summed, fc1_grad, fc2_grad = exchange(
        jnp.stack([normed, cotangent]),
        bias,
        fc1_weight,
        fc2_weight,
        text.reshape(samples * length, text.shape[2]),
        query_weight,
    )
    states = (own_rows.astype(jnp.float32) + summed + fc2_bias).astype(jnp.bfloat16)
    local_heads = query_weight.shape[1] // HD
    per_group = HEADS // KV_HEADS
    kv_local = max(1, local_heads // per_group)
    first_head = dec_place * local_heads // per_group
    keys, values = share_keys(states, key_weight, value_weight, first_head, kv_local)
    queries = queries.reshape(samples, length, kv_local, local_heads // kv_local, HD)
    context = attend(
        queries, keys, values, tiles[enc_place, :, grp_place], links, lengths, slots, patch, length, dec_count
    )
    return (context, fc1_grad, fc2_grad)


def on_device(
    images,
    ln_gain,
    ln_bias,
    fc1_weight,
    fc1_bias,
    fc2_weight,
    fc2_bias,
    key_weight,
    value_weight,
    text,
    query_weight,
    tiles,
    links,
    lengths,
    state_grads,
):
    dec_count = lax.axis_size("dec")
    grp_count = lax.axis_size("grp")
    enc_place = lax.axis_index("enc")
    dec_place = lax.axis_index("dec")
    grp_place = lax.axis_index("grp")
    slots = images.shape[1]
    patch = images.shape[2]
    width = images.shape[3]
    img_rows = slots * patch
    own_rows = images.reshape(img_rows, width)
    normed = normalize_layer(own_rows.astype(jnp.float32), ln_gain, ln_bias).astype(jnp.bfloat16)
    samples = text.shape[0]
    length = text.shape[1]
    text_rows = text.reshape(samples * length, text.shape[2])
    half = query_weight.shape[1] // grp_count
    own_half = lax.dynamic_slice_in_dim(query_weight, grp_place * half, half, 1)
    own_tiles = tiles[enc_place, dec_place, grp_place]
    tile_index = jnp.arange(slots)
    own_live = jnp.broadcast_to((tile_index < own_tiles)[:, None, None], (slots, patch, 1)).reshape(
        img_rows, 1
    )
    cotangent = jnp.where(
        own_live, state_grads.reshape(img_rows, width), jnp.zeros((), state_grads.dtype)
    )
    sent = jnp.stack([normed, cotangent])
    text_rows, own_half, _ = lax.optimization_barrier((text_rows, own_half, sent))
    both = lax.all_gather(sent, "enc", axis=1, tiled=True)
    gathered, all_cotangent = both[0], both[1]
    text_blocks = share_text(text_rows)
    pre, hidden, partial_full = encoder_rows(gathered, fc1_weight, fc1_bias, fc2_weight)
    partial_full = partial_full.astype(jnp.bfloat16)
    all_cotangent, _ = lax.optimization_barrier((all_cotangent, partial_full))
    first_term, second_term = weight_terms(gathered, pre, hidden, all_cotangent, fc2_weight)
    queries_of = project_queries(text_blocks, own_half, second_term)
    summed = lax.psum_scatter(
        partial_full, "enc", scatter_dimension=0, tiled=True
    ).astype(jnp.float32)
    states = (own_rows.astype(jnp.float32) + summed + fc2_bias).astype(jnp.bfloat16)
    local_heads = query_weight.shape[1] // HD
    per_group = HEADS // KV_HEADS
    kv_local = max(1, local_heads // per_group)
    first_head = dec_place * local_heads // per_group
    keys, values = share_keys(states, key_weight, value_weight, first_head, kv_local)
    heads_each = local_heads // kv_local
    queries = queries_of
    queries = queries.reshape(samples, length, kv_local, heads_each, HD)
    dec_tiles = tiles[enc_place, :, grp_place]
    live_keys = tile_index[None, :] < dec_tiles[:, None]
    live_keys = jnp.broadcast_to(live_keys[:, :, None], (dec_count, slots, patch)).reshape(
        dec_count, img_rows
    )
    allowed = (links[:, :, None] > 0) & live_keys[None, :, :]
    scores = jnp.einsum(
        "sqghd,jgkd->sghjkq", queries, keys, preferred_element_type=jnp.float32
    ) * HD ** (-0.5)
    weights = jnp.where(allowed[:, None, None, :, :, None], jnp.exp(scores), 0.0)
    totals = jnp.sum(weights, axis=(3, 4), keepdims=True)
    probs = (weights / totals).astype(jnp.bfloat16)
    mixed = jnp.einsum("sghjkq,jgkd->sqghd", probs, values, preferred_element_type=jnp.float32)
    valid = jnp.arange(length)[None, :] < lengths[:, None]
    context = (
        jnp.where(valid[:, :, None, None, None], mixed, 0.0)
        .reshape(samples, length, local_heads * HD)
        .astype(jnp.bfloat16)
    )
    fc1_grad, fc2_grad = share_grads(jnp.stack([first_term, second_term]))
    return (context, fc1_grad, fc2_grad)


def solution(mesh):
    in_specs = (
        P(("enc", "dec", "grp"), None, None, None),
        P(),
        P(),
        P("enc", None),
        P("enc"),
        P("enc", None),
        P(),
        P(),
        P(),
        P(("enc", "grp"), None, None),
        P("enc", "dec"),
        P(),
        P(("enc", "grp"), None),
        P(("enc", "grp")),
        P(("enc", "dec", "grp"), None, None, None),
    )
    out_specs = (
        P(("enc", "grp"), None, "dec"),
        P(("enc", "dec", "grp"), None),
        P(("enc", "dec", "grp"), None),
    )
    paired = mesh.shape["dec"] == 2 and mesh.shape["grp"] == 2 and mesh.shape["enc"] % 2 == 0
    if paired and mesh.shape["enc"] > 4:
        return jax.shard_map(
            on_column, mesh=mesh, in_specs=in_specs, out_specs=out_specs, check_vma=False
        )
    return jax.shard_map(
        on_device, mesh=mesh, in_specs=in_specs, out_specs=out_specs, check_vma=False
    )
```

```python
import functools

import jax
import jax.numpy as jnp
from jax import lax
from jax.experimental import pallas as pl
from jax.experimental.pallas import tpu as pltpu
from jax.sharding import PartitionSpec as P


HEADS = 32
KV_HEADS = 4
HD = 128


EPSILON = 1e-06


def normalize_layer(values, gain, shift):
    middle = jnp.mean(values, axis=-1, keepdims=True)
    centered = values - middle
    spread = jnp.mean(centered * centered, axis=-1, keepdims=True)
    return centered * lax.rsqrt(spread + EPSILON) * gain + shift


def normalize_heads(values):
    return values * lax.rsqrt(jnp.mean(values * values, axis=-1, keepdims=True) + EPSILON)


def gelu_slope(values):
    return (
        0.5 * (1.0 + lax.erf(values * 0.7071067811865476))
        + values * jnp.exp(-0.5 * values * values) * 0.3989422804014327
    )


def encoder_rows(rows, fc1_weight, fc1_bias, fc2_weight):
    pre = (
        lax.dot_general(
            rows, fc1_weight, (((1,), (1,)), ((), ())), preferred_element_type=jnp.float32
        )
        + fc1_bias
    )
    hidden = jax.nn.gelu(pre, approximate=False).astype(jnp.bfloat16)
    partial_sum = jnp.dot(hidden, fc2_weight, preferred_element_type=jnp.float32)
    return (pre, hidden, partial_sum)


def weight_terms(rows, pre, hidden, cotangent, fc2_weight):
    hidden_grad = lax.dot_general(
        cotangent, fc2_weight, (((1,), (1,)), ((), ())), preferred_element_type=jnp.float32
    )
    second_term = lax.dot_general(
        hidden, cotangent, (((0,), (0,)), ((), ())), preferred_element_type=jnp.float32
    )
    pre_grad = (hidden_grad * gelu_slope(pre)).astype(jnp.bfloat16)
    first_term = lax.dot_general(
        pre_grad, rows, (((0,), (0,)), ((), ())), preferred_element_type=jnp.float32
    )
    return (first_term, second_term)


def project_heads(states, key_columns, value_columns, heads):
    width = states.shape[-1]
    key_raw = jnp.einsum(
        "rd,dhe->hre",
        states,
        key_columns.reshape(width, heads, HD),
        preferred_element_type=jnp.float32,
    )
    keys = normalize_heads(key_raw).astype(jnp.bfloat16)
    values = jnp.einsum(
        "rd,dhe->hre",
        states,
        value_columns.reshape(width, heads, HD),
        preferred_element_type=jnp.float32,
    ).astype(jnp.bfloat16)
    return (keys, values)


def shifted(values, axis, step):
    size = lax.axis_size(axis)
    return lax.ppermute(values, axis, [(i, (i + step) % size) for i in range(size)])


def swapped(values):
    return lax.ppermute(values, "enc", [(i, i ^ 1) for i in range(lax.axis_size("enc"))])


def share_text(text_rows):
    enc_count = lax.axis_size("enc")
    _, depth = text_rows.shape
    side = lax.axis_index("enc") % 2
    block = depth // enc_count
    even = jnp.stack([text_rows[:, i * block : (i + 1) * block] for i in range(0, enc_count, 2)])
    odd = jnp.stack([text_rows[:, i * block : (i + 1) * block] for i in range(1, enc_count, 2)])
    own = jnp.where(side == 0, even, odd)
    away = jnp.where(side == 0, odd, even)
    arrived = swapped(away)
    pair = jnp.concatenate([arrived, own], axis=1)
    return jnp.concatenate(
        [pair] + [shifted(pair, "grp", step) for step in range(1, lax.axis_size("grp"))], axis=1
    )


def project_queries(text_blocks, weight, before):
    grp_count = lax.axis_size("grp")
    ring = lax.axis_size("enc") // 2
    enc_count = lax.axis_size("enc")
    place = lax.axis_index("enc") // 2
    total = None
    for step in range(ring):
        if step == max(0, ring - 2):
            weight, _ = lax.optimization_barrier((weight, before))
        left = lax.dynamic_index_in_dim(text_blocks, (place - step) % ring, 0, keepdims=False)
        term = jnp.dot(left, weight, preferred_element_type=jnp.float32)
        total = term if total is None else total + term
        if step < ring - 1:
            weight = lax.ppermute(
                weight, "enc", [(i, (i + 2) % enc_count) for i in range(enc_count)]
            )
    columns = total.shape[1]
    total = total.reshape(grp_count, 2, -1, columns)
    arrived = swapped(total[:, 0].astype(jnp.bfloat16))
    raw = total[:, 1] + arrived.astype(jnp.float32)
    own = normalize_heads(raw.reshape(grp_count, -1, columns // HD, HD)).astype(jnp.bfloat16)
    blocks = jnp.stack(
        [own[0]] + [shifted(own[step], "grp", -step) for step in range(1, grp_count)], axis=1
    )
    start = (grp_count - lax.axis_index("grp")) % grp_count
    blocks = lax.dynamic_slice_in_dim(
        jnp.concatenate([blocks, blocks], axis=1), start, grp_count, 1
    )
    return blocks.reshape(blocks.shape[0], grp_count * columns)


def share_keys(states, key_weight, value_weight, first_head, kv_local):
    dec_count = lax.axis_size("dec")
    rows, _ = states.shape
    if dec_count == 2 and kv_local * dec_count == KV_HEADS:
        keys, values = project_heads(states, key_weight, value_weight, KV_HEADS)
        paired = jnp.stack([keys, values])
        own = lax.dynamic_slice_in_dim(paired, first_head, kv_local, 1)
        away = lax.dynamic_slice_in_dim(paired, KV_HEADS - kv_local - first_head, kv_local, 1)
        arrived = shifted(away, "dec", 1)
        first = lax.axis_index("dec") == 0
        paired = jnp.stack(
            [jnp.where(first, own, arrived), jnp.where(first, arrived, own)], axis=1
        )
        return (paired[0], paired[1])
    key_columns = lax.dynamic_slice_in_dim(key_weight, first_head * HD, kv_local * HD, 1)
    value_columns = lax.dynamic_slice_in_dim(value_weight, first_head * HD, kv_local * HD, 1)
    piece = lax.all_gather(states, "dec", axis=0, tiled=True)
    key_part, value_part = project_heads(piece, key_columns, value_columns, kv_local)
    shape = (kv_local, dec_count, rows, HD)
    return (
        key_part.reshape(shape).transpose(1, 0, 2, 3),
        value_part.reshape(shape).transpose(1, 0, 2, 3),
    )


def share_grads(terms):
    dec_count = lax.axis_size("dec")
    grp_count = lax.axis_size("grp")
    rows = terms.shape[1] // (dec_count * grp_count)
    if dec_count == 2 and grp_count == 2:
        parts = terms.reshape(2, dec_count, grp_count, rows, -1)
        grp_place = lax.axis_index("grp")
        dec_place = lax.axis_index("dec")
        kept = lax.dynamic_index_in_dim(parts, grp_place, 2, keepdims=False)
        away = lax.dynamic_index_in_dim(parts, 1 - grp_place, 2, keepdims=False)
        kept = kept + shifted(away.astype(jnp.bfloat16), "grp", 1).astype(jnp.float32)
        away = lax.dynamic_index_in_dim(kept, 1 - dec_place, 1, keepdims=False)
        kept = lax.dynamic_index_in_dim(kept, dec_place, 1, keepdims=False)
        kept = kept + shifted(away.astype(jnp.bfloat16), "dec", 1).astype(jnp.float32)
        return (kept[0], kept[1])
    summed = lax.psum_scatter(
        terms.astype(jnp.bfloat16), ("dec", "grp"), scatter_dimension=1, tiled=True
    ).astype(jnp.float32)
    return (summed[0], summed[1])


MESH = pl.DeviceIdType.MESH


def pick(table, place):
    return sum(jnp.where(place == i, value, 0) for i, value in enumerate(table))


def step_kernel(
    line,
    patch,
    tiles_ref,
    links_ref,
    lengths_ref,
    images_ref,
    state_grads_ref,
    gain_ref,
    shift_ref,
    bias_ref,
    up_ref,
    down_ref,
    down_bias_ref,
    key_ref,
    value_ref,
    text_ref,
    weight_ref,
    context_ref,
    up_grad_ref,
    down_grad_ref,
    own,
    kw,
    kv_send,
    kv,
    queries,
    tb,
    wb,
    fb,
    bb,
    bias_col,
    rows,
    pre,
    hid_t,
    hid,
    pg_t,
    po,
    psend,
    precv,
    msend,
    mrecv,
    gs1,
    gr1,
    gs2,
    gr2,
    gs3,
    gr3,
    local_sem,
    t_send,
    t_recv,
    y_send,
    y_recv,
    x_send,
    x_recv,
    s_send,
    s_recv,
    a_send,
    a_recv,
    p_send,
    p_recv,
    m_send,
    m_recv,
    g_send,
    g_recv,
    k_send,
    k_recv,
):
    f32 = jnp.float32
    bf16 = jnp.bfloat16
    enc = lax.axis_index("enc")
    y = lax.axis_index("dec")
    g = lax.axis_index("grp")
    z, x = enc // 2, enc % 2
    other_x = ((z * 2 + 1 - x), y, g)
    other_y = (enc, 1 - y, g)
    other_g = (enc, y, 1 - g)

    def along(place):
        return (place * 2 + x, y, g)

    orders = []
    for p in range(line):
        others = [a for a in range(line) if a != p]
        others.sort(key=lambda a: (-abs(a - p), min(a, line - 1 - a)))
        orders.append(others)
    order = [pick([orders[p][i] for p in range(line)], z) for i in range(line - 1)]
    text_rows, depth = tb.shape[2], tb.shape[3]
    half_cols = wb.shape[3]
    img = rows.shape[2]
    width = rows.shape[3]
    units = fb.shape[2]
    piece = units // 2
    part = units // 4

    barrier = pltpu.get_barrier_semaphore()
    for k in range(line):

        @pl.when(z != k)
        def _():
            pl.semaphore_signal(barrier, inc=1, device_id=along(k), device_id_type=MESH)

    for to in (other_x, other_y, other_g):
        pl.semaphore_signal(barrier, inc=1, device_id=to, device_id_type=MESH)
    pl.semaphore_wait(barrier, line + 2)

    def remote(src, dst, send, recv, to):
        return pltpu.make_async_remote_copy(
            src_ref=src, dst_ref=dst, send_sem=send, recv_sem=recv, device_id=to, device_id_type=MESH
        )

    def text_copy(i):
        b = order[i]
        at = pl.multiple_of((b * 2 + y) * depth, depth)
        return remote(
            text_ref.at[:, pl.ds(at, depth)], tb.at[z, y], t_send.at[i], t_recv.at[z], along(b)
        )

    def text_landed(a):
        return remote(tb.at[a, y], tb.at[a, y], t_send.at[0], t_recv.at[a], other_y)

    def text_relay(a):
        return remote(tb.at[a, y], tb.at[a, y], y_send.at[a], y_recv.at[a], other_y)

    def text_relayed(a):
        return remote(tb.at[a, 1 - y], tb.at[a, 1 - y], y_send.at[a], y_recv.at[a], other_y)

    weight_x = remote(
        weight_ref.at[:, pl.ds(pl.multiple_of(g * half_cols, half_cols), half_cols)],
        wb.at[x, g],
        x_send.at[0],
        x_recv.at[0],
        other_x,
    )
    weight_x_in = remote(wb.at[1 - x, g], wb.at[1 - x, g], x_send.at[0], x_recv.at[0], other_x)
    weight_s = remote(wb.at[1 - x, g], wb.at[1 - x, g], s_send.at[0], s_recv.at[0], other_g)
    weight_s_in = remote(wb.at[1 - x, 1 - g], wb.at[1 - x, 1 - g], s_send.at[0], s_recv.at[0], other_g)

    def unit_rows(core, q):
        return pl.ds(pl.multiple_of(core * piece + q * part, part), part)

    def unit_x(ref, kind, q):
        return remote(
            ref.at[unit_rows(g, q)],
            fb.at[kind, x, unit_rows(g, q)],
            x_send.at[1 + q],
            x_recv.at[1 + q],
            other_x,
        )

    def unit_copy(kind, core, q, send, recv, to):
        spot = fb.at[kind, 1 - x, unit_rows(core, q)]
        return remote(spot, spot, send, recv, to)

    def unit_x_in(q):
        return unit_copy(y, g, q, x_send.at[1 + q], x_recv.at[1 + q], other_x)

    def unit_s(q):
        return unit_copy(y, g, q, s_send.at[1 + q], s_recv.at[1 + q], other_g)

    def unit_s_in(q):
        return unit_copy(y, 1 - g, q, s_send.at[1 + q], s_recv.at[1 + q], other_g)

    def unit_y(q):
        return unit_copy(y, g, q, y_send.at[line + q], y_recv.at[line + q], other_y)

    def unit_y_in(q):
        return unit_copy(1 - y, g, q, y_send.at[line + q], y_recv.at[line + q], other_y)

    def unit_s2(q):
        return unit_copy(1 - y, g, q, s_send.at[3 + q], s_recv.at[3 + q], other_g)

    def unit_s2_in(q):
        return unit_copy(1 - y, 1 - g, q, s_send.at[3 + q], s_recv.at[3 + q], other_g)

    bb[x] = bias_ref[...][None]
    bias_x = remote(bb.at[x], bb.at[x], x_send.at[3], x_recv.at[3], other_x)
    bias_x_in = remote(bb.at[1 - x], bb.at[1 - x], x_send.at[3], x_recv.at[3], other_x)

    def rows_copy(m, a, right):
        to = along(z + 1) if right else along(z - 1)
        spot = rows.at[m, a]
        return remote(spot, spot, a_send.at[1 if right else 0, m, a], a_recv.at[m, a], to)

    def rows_landed(m, a):
        return remote(rows.at[m, a], rows.at[m, a], a_send.at[0, m, a], a_recv.at[m, a], other_y)

    locals_ = [
        pltpu.make_async_copy(weight_ref.at[:, pl.ds(c * half_cols, half_cols)], wb.at[x, c], local_sem.at[c])
        for c in range(2)
    ] + [
        pltpu.make_async_copy(up_ref, fb.at[0, x], local_sem.at[2]),
        pltpu.make_async_copy(down_ref, fb.at[1, x], local_sem.at[3]),
        pltpu.make_async_copy(key_ref, kw.at[0], local_sem.at[5]),
        pltpu.make_async_copy(value_ref, kw.at[1], local_sem.at[8]),
    ] + [
        pltpu.make_async_copy(
            text_ref.at[:, pl.ds(pl.multiple_of((z * 2 + h) * depth, depth), depth)],
            tb.at[z, h],
            local_sem.at[6 + h],
        )
        for h in range(2)
    ]

    for i in range(line - 1):
        text_copy(i).start()
    weight_x.start()
    own_copies = [
        pltpu.make_async_copy(images_ref, own.at[0], local_sem.at[9]),
        pltpu.make_async_copy(state_grads_ref, own.at[1], local_sem.at[10]),
    ]
    for copy in own_copies + locals_:
        copy.start()
    for copy in own_copies:
        copy.wait()

    def live_rows(j):
        return tiles_ref[enc, j, g] * patch

    own_live = live_rows(y)

    def norm_body(t, _):
        r = pl.ds(pl.multiple_of(t * 16, 16), 16)
        normed = normalize_layer(own[0, r].astype(f32), gain_ref[...][None], shift_ref[...][None])
        rows[0, z, r] = normed.astype(bf16)
        row = t * 16 + lax.broadcasted_iota(jnp.int32, (16, width), 0)
        rows[1, z, r] = jnp.where(row < own_live, own[1, r].astype(f32), 0.0).astype(bf16)
        return 0

    lax.fori_loop(0, img // 16, norm_body, 0)

    for m in range(2):

        @pl.when(z < line - 1)
        def _(m=m):
            rows_copy(m, z, True).start()

        @pl.when(z > 0)
        def _(m=m):
            rows_copy(m, z, False).start()

    for i in range(line - 1):
        text_landed(order[i]).wait_recv()
        text_relay(order[i]).start()
    weight_x_in.wait_recv()
    weight_s.start()
    weight_x.wait_send()

    @pl.when(y == 0)
    def _():
        for q in range(2):
            unit_x(up_ref, 0, q).start()

    @pl.when(y == 1)
    def _():
        for q in range(2):
            unit_x(down_ref, 1, q).start()

    bias_x.start()
    for copy in locals_:
        copy.wait()

    def forward_rows(m, s):
        @pl.when(z - s >= 0)
        def _():
            rows_landed(m, z - s).wait_recv()

            @pl.when(z < line - 1)
            def _():
                rows_copy(m, z - s, True).start()

        @pl.when(z + s <= line - 1)
        def _():
            rows_landed(m, z + s).wait_recv()

            @pl.when(z > 0)
            def _():
                rows_copy(m, z + s, False).start()

    def has_incoming(a):
        return jnp.logical_or(
            jnp.logical_and(a > z, z > 0), jnp.logical_and(a < z, z < line - 1)
        )

    def next_slot(a):
        right = a > z
        to = jnp.where(right, z + 1, z - 1)
        slot = jnp.where(jnp.logical_and(to == a, jnp.logical_not(right)), line, a)
        return to, slot

    def sum_copy(a, c):
        to, slot = next_slot(a)
        return remote(psend.at[a, c], precv.at[slot, c], p_send.at[a, c], p_recv.at[slot, c], along(to))

    def sum_landed(slot, c):
        return remote(precv.at[slot, c], precv.at[slot, c], p_send.at[0, c], p_recv.at[slot, c], other_y)

    tile = 256

    def multiply(a, c, store):
        def body(t, _):
            cols = pl.ds(pl.multiple_of(t * tile, tile), tile)
            total = jnp.dot(tb[a, 0], wb[0, c, :, cols], preferred_element_type=f32)
            total = total + jnp.dot(tb[a, 1], wb[1, c, :, cols], preferred_element_type=f32)
            store(t, cols, total)
            return 0

        lax.fori_loop(0, half_cols // tile, body, 0)

    def product(i, c):
        a = order[i]

        def store(t, cols, total):
            psend[a, c, :, cols] = total.astype(bf16)

        multiply(a, c, store)

    def send_product(i, c):
        a = order[i]

        @pl.when(jnp.logical_not(has_incoming(a)))
        def _():
            sum_copy(a, c).start()

    def add_incoming(i, c):
        a = order[i]

        @pl.when(has_incoming(a))
        def _():
            sum_landed(a, c).wait_recv()

            def body(t, _):
                r = pl.ds(pl.multiple_of(t * 16, 16), 16)
                psend[a, c, r] = (psend[a, c, r].astype(f32) + precv[a, c, r].astype(f32)).astype(bf16)
                return 0

            lax.fori_loop(0, text_rows // 16, body, 0)
            sum_copy(a, c).start()

    held = ((line - 2, 0), (line - 2, 1))

    def products(i):
        text_relayed(order[i]).wait_recv()
        for c in range(2):
            product(i, c)
            if (i, c) not in held:
                send_product(i, c)

    def relay_units(q):
        unit_x_in(q).wait_recv()
        unit_s(q).start()
        unit_y(q).start()

    weight_s_in.wait_recv()
    products(0)
    forward_rows(0, 1)
    relay_units(0)
    products(1)
    add_incoming(0, 0)
    for m in range(2):
        forward_rows(m, 2 - m)
    relay_units(1)
    for i in range(2, line - 1):
        products(i)
    unit_y_in(0).wait_recv()
    unit_s2(0).start()
    add_incoming(0, 1)
    forward_rows(0, 3)
    unit_y_in(1).wait_recv()
    unit_s2(1).start()
    bias_x_in.wait_recv()
    for q in range(2):
        unit_s_in(q).wait_recv()
        unit_s2_in(q).wait_recv()

    all_rows = line * img

    def up_body(q, _):
        k = q // 2
        at = pl.multiple_of((q % 2) * piece, piece)
        pre[k, pl.ds(at, piece)] = lax.dot_general(
            fb[0, k, pl.ds(at, piece)],
            rows[0].reshape(all_rows, width),
            (((1,), (1,)), ((), ())),
            preferred_element_type=f32,
        )
        return 0

    lax.fori_loop(0, 4, up_body, 0)
    forward_rows(1, 2)
    for k in range(2):
        for t in range(units // 128):
            spot = slice(t * 128, (t + 1) * 128)
            bias_col[k, spot] = jnp.transpose(jnp.broadcast_to(bb[k, :, spot], (8, 128)))

    def gelu_body(r, _):
        k = r // (units // 16)
        at = pl.ds(pl.multiple_of((r % (units // 16)) * 16, 16), 16)
        value = pre[k, at] + bias_col[k, at, 0:1]
        phi = 0.5 * (1.0 + lax.erf(value * 0.7071067811865476))
        hid_t[k, at] = (value * phi).astype(bf16)
        pre[k, at] = phi + value * jnp.exp(-0.5 * value * value) * 0.3989422804014327
        return 0

    lax.fori_loop(0, 2 * units // 16, gelu_body, 0, unroll=4)

    def terms(kind, k, j, owner):
        at = pl.ds(pl.multiple_of(j * piece + owner * part, part), part)
        left = pg_t if kind == 0 else hid_t
        return jnp.dot(left[k, at], rows[kind].reshape(all_rows, width), preferred_element_type=f32)

    grads_s = [remote(gs1.at[m], gr1.at[m], g_send.at[m], g_recv.at[m], other_g) for m in range(2)]
    grads_y = remote(gs2.at[0], gr2.at[0], g_send.at[2], g_recv.at[2], other_y)
    grads_x = remote(gs2.at[1], gr2.at[1], g_send.at[3], g_recv.at[3], other_x)
    grads_x2 = remote(gs3.at[0], gr3.at[0], g_send.at[4], g_recv.at[4], other_x)
    grads_y2 = remote(gs3.at[1], gr3.at[1], g_send.at[5], g_recv.at[5], other_y)

    def share_core(kind):
        def body(q, _):
            k, j = q // 2, q % 2
            gs1[kind, k, j] = terms(kind, k, j, 1 - g).astype(bf16)
            return 0

        lax.fori_loop(0, 4, body, 0)
        grads_s[kind].start()

    def flip_body(t, _):
        for k in range(2):
            at = pl.ds(pl.multiple_of(t * 128, 128), 128)
            hid[k, :, at] = jnp.transpose(hid_t[k, at].astype(f32)).astype(bf16)
        return 0

    lax.fori_loop(0, units // 128, flip_body, 0)

    def down_body(t, _):
        cols = pl.ds(pl.multiple_of(t * tile, tile), tile)
        total = jnp.dot(hid[0], fb[1, 0, :, cols], preferred_element_type=f32)
        po[:, cols] = total + jnp.dot(hid[1], fb[1, 1, :, cols], preferred_element_type=f32)
        return 0

    lax.fori_loop(0, width // tile, down_body, 0)

    def state_copy(a):
        to, slot = next_slot(a)
        return remote(msend.at[a], mrecv.at[slot], m_send.at[a], m_recv.at[slot], along(to))

    def state_landed(slot):
        return remote(mrecv.at[slot], mrecv.at[slot], m_send.at[0], m_recv.at[slot], other_y)

    def send_state(i, first):
        a = order[i]
        waits = has_incoming(a)

        @pl.when(jnp.logical_not(waits) if first else waits)
        def _():
            if not first:
                state_landed(a).wait_recv()

            def body(t, _):
                r = pl.ds(pl.multiple_of(t * 16, 16), 16)
                value = po[pl.ds(pl.multiple_of(a * img + t * 16, 16), 16)]
                if not first:
                    value = value + mrecv[a, r].astype(f32)
                msend[a, r] = value.astype(bf16)
                return 0

            lax.fori_loop(0, img // 16, body, 0)
            state_copy(a).start()

    for i in range(line - 1):
        send_state(i, True)
    for c in range(2):
        send_product(line - 2, c)
    add_incoming(1, 0)
    add_incoming(2, 0)
    forward_rows(1, 3)
    share_core(1)

    def slope_body(q, _):
        k = q // 2
        at = pl.ds(pl.multiple_of((q % 2) * piece, piece), piece)
        grad = lax.dot_general(
            fb[1, k, at],
            rows[1].reshape(all_rows, width),
            (((1,), (1,)), ((), ())),
            preferred_element_type=f32,
        )
        pg_t[k, at] = (grad * pre[k, at]).astype(bf16)
        return 0

    lax.fori_loop(0, 4, slope_body, 0)
    share_core(0)

    grads_s[1].wait_recv()

    def away_x(j, _):
        gs2[1, j] = (terms(1, 1 - x, j, g) + gr1[1, 1 - x, j].astype(f32)).astype(bf16)
        return 0

    lax.fori_loop(0, 2, away_x, 0)
    grads_x.start()
    grads_s[0].wait_recv()

    def away_y(k, _):
        gs2[0, k] = (terms(0, k, 1 - y, g) + gr1[0, k, 1 - y].astype(f32)).astype(bf16)
        return 0

    lax.fori_loop(0, 2, away_y, 0)
    grads_y.start()
    add_incoming(1, 1)
    send_state(0, False)
    send_state(2, False)
    add_incoming(2, 1)
    send_state(1, False)
    grads_x.wait_recv()
    total = terms(1, x, 1 - y, g) + gr1[1, x, 1 - y].astype(f32)
    gs3[1] = (total + gr2[1, 1 - y].astype(f32)).astype(bf16)
    grads_y2.start()
    grads_y.wait_recv()
    total = terms(0, 1 - x, y, g) + gr1[0, 1 - x, y].astype(f32)
    gs3[0] = (total + gr2[0, 1 - x].astype(f32)).astype(bf16)
    grads_x2.start()

    def own_texts(c):

        @pl.when(z > 0)
        def _():
            sum_landed(z, c).wait_recv()

        @pl.when(z < line - 1)
        def _():
            sum_landed(line, c).wait_recv()

        def store(t, cols, total, c=c):
            total = total + jnp.where(z > 0, precv[z, c, :, cols].astype(f32), 0.0)
            total = total + jnp.where(z < line - 1, precv[line, c, :, cols].astype(f32), 0.0)
            for h in range(tile // HD):
                head = total[:, h * HD : (h + 1) * HD]
                scale = lax.rsqrt(jnp.mean(head * head, axis=-1, keepdims=True) + EPSILON)
                at = pl.multiple_of(c * half_cols + t * tile + h * HD, HD)
                queries[:, pl.ds(at, HD)] = (head * scale).astype(bf16)

        multiply(z, c, store)

    slot_rows = pl.ds(pl.multiple_of(z * img, img), img)
    po[slot_rows] = po[slot_rows] + own[0].astype(f32) + down_bias_ref[...][None]

    @pl.when(z > 0)
    def _():
        state_landed(z).wait_recv()
        po[slot_rows] = po[slot_rows] + mrecv[z].astype(f32)

    @pl.when(z < line - 1)
    def _():
        state_landed(line).wait_recv()
        po[slot_rows] = po[slot_rows] + mrecv[line].astype(f32)

    states = po[slot_rows].astype(bf16)
    local = kv.shape[2]
    own_rows = pl.ds(pl.multiple_of(y * img, img), img)
    away_rows = pl.ds(pl.multiple_of((1 - y) * img, img), img)
    kv_copy = remote(kv_send, kv.at[:, own_rows], k_send, k_recv, other_y)
    kv_in = remote(kv.at[:, away_rows], kv.at[:, away_rows], k_send, k_recv, other_y)
    for sent in (True, False):
        at = pl.multiple_of(((1 - y) if sent else y) * local, local)
        spot = kv_send if sent else kv.at[:, own_rows]
        raw = jnp.dot(states, kw[0, :, pl.ds(at, local)], preferred_element_type=f32)
        for h in range(local // HD):
            head = normalize_heads(raw[:, h * HD : (h + 1) * HD])
            spot[0, :, h * HD : (h + 1) * HD] = head.astype(bf16)
        raw = jnp.dot(states, kw[1, :, pl.ds(at, local)], preferred_element_type=f32)
        spot[1] = raw.astype(bf16)
        if sent:
            kv_copy.start()

    samples, length = context_ref.shape[:2]
    group = half_cols // HD

    def attend_texts(c):
        head_cols = slice(c * HD, (c + 1) * HD)
        key = lax.broadcasted_iota(jnp.int32, (length, 2 * img), 1)

        def body(n, _):
            r = pl.ds(pl.multiple_of(n * length, length), length)
            limits = [jnp.where(links_ref[n, j] > 0, live_rows(j), 0) for j in range(2)]
            allowed = key < jnp.where(key < img, limits[0], limits[1] + img)
            valid = lax.broadcasted_iota(jnp.int32, (length, HD), 0) < lengths_ref[n]
            for h in range(group):
                cols = slice(c * half_cols + h * HD, c * half_cols + (h + 1) * HD)
                score = lax.dot_general(
                    queries[r, cols],
                    kv[0, :, head_cols],
                    (((1,), (1,)), ((), ())),
                    preferred_element_type=f32,
                )
                weights = jnp.where(allowed, jnp.exp(score * HD ** (-0.5)), 0.0)
                scale = 1.0 / jnp.sum(weights, axis=-1, keepdims=True)
                mixed = jnp.dot(
                    (weights * scale).astype(bf16), kv[1, :, head_cols], preferred_element_type=f32
                )
                context_ref[n, :, cols] = jnp.where(valid, mixed, 0.0).astype(bf16)
            return 0

        lax.fori_loop(0, samples, body, 0)

    own_texts(0)
    kv_in.wait_recv()
    attend_texts(0)
    own_texts(1)
    attend_texts(1)
    for kind, out in ((1, down_grad_ref), (0, up_grad_ref)):
        (grads_x2, grads_y2)[kind].wait_recv()
        total = terms(kind, x, y, g) + gr1[kind, x, y].astype(f32)
        total = total + gr2[kind, (x, y)[kind]].astype(f32)
        out[...] = total + gr3[kind].astype(f32)

    for i in range(line - 1):
        a = order[i]
        text_copy(i).wait_send()
        text_relay(a).wait_send()
        state_copy(a).wait_send()
        for c in range(2):
            sum_copy(a, c).wait_send()
    for copy in (kv_copy, weight_s, bias_x, *grads_s, grads_y, grads_x, grads_x2, grads_y2):
        copy.wait_send()
    for q in range(2):
        for copy in (unit_x(up_ref, 0, q), unit_s(q), unit_y(q), unit_s2(q)):
            copy.wait_send()

    for a in range(line):

        @pl.when(jnp.logical_and(a <= z, z < line - 1))
        def _():
            for m in range(2):
                rows_copy(m, a, True).wait_send()

        @pl.when(jnp.logical_and(a >= z, z > 0))
        def _():
            for m in range(2):
                rows_copy(m, a, False).wait_send()


def exchange(
    tiles, links, lengths, images, state_grads, gain, shift, bias, up, down, down_bias, key, value, text, weight, patch
):
    line = lax.axis_size("enc") // 2
    text_rows = text.shape[0] * text.shape[1]
    depth, columns = weight.shape
    img, width = images.shape
    units = up.shape[0]
    half = columns // 2
    local = key.shape[1] // 2
    f32, bf16 = jnp.float32, jnp.bfloat16
    dma = pltpu.SemaphoreType.DMA
    part = units // 4
    smem = pl.BlockSpec(memory_space=pltpu.SMEM)
    vmem = pl.BlockSpec(memory_space=pltpu.VMEM)
    anywhere = pl.BlockSpec(memory_space=pl.ANY)
    return pl.pallas_call(
        functools.partial(step_kernel, line, patch),
        out_shape=[
            jax.ShapeDtypeStruct((*text.shape[:2], columns), bf16),
            jax.ShapeDtypeStruct((part, width), f32),
            jax.ShapeDtypeStruct((part, width), f32),
        ],
        in_specs=[smem] * 3 + [anywhere] * 2 + [vmem] * 3 + [anywhere] * 2 + [vmem] + [anywhere] * 4,
        out_specs=[vmem] * 3,
        scratch_shapes=[
            pltpu.VMEM((2, img, width), bf16),
            pltpu.VMEM((2, width, 2 * local), bf16),
            pltpu.VMEM((2, img, local), bf16),
            pltpu.VMEM((2, 2 * img, local), bf16),
            pltpu.VMEM((text_rows, columns), bf16),
            pltpu.VMEM((line, 2, text_rows, depth), bf16),
            pltpu.VMEM((2, 2, depth, half), bf16),
            pltpu.VMEM((2, 2, units, width), bf16),
            pltpu.VMEM((2, 1, units), f32),
            pltpu.VMEM((2, units, 8), f32),
            pltpu.VMEM((2, line, img, width), bf16),
            pltpu.VMEM((2, units, line * img), f32),
            pltpu.VMEM((2, units, line * img), bf16),
            pltpu.VMEM((2, line * img, units), bf16),
            pltpu.VMEM((2, units, line * img), bf16),
            pltpu.VMEM((line * img, width), f32),
            pltpu.VMEM((line, 2, text_rows, half), bf16),
            pltpu.VMEM((line + 1, 2, text_rows, half), bf16),
            pltpu.VMEM((line, img, width), bf16),
            pltpu.VMEM((line + 1, img, width), bf16),
            pltpu.VMEM((2, 2, 2, part, width), bf16),
            pltpu.VMEM((2, 2, 2, part, width), bf16),
            pltpu.VMEM((2, 2, part, width), bf16),
            pltpu.VMEM((2, 2, part, width), bf16),
            pltpu.VMEM((2, part, width), bf16),
            pltpu.VMEM((2, part, width), bf16),
            dma((11,)),
            dma((line - 1,)),
            dma((line,)),
            dma((line + 2,)),
            dma((line + 2,)),
            dma((4,)),
            dma((4,)),
            dma((5,)),
            dma((5,)),
            dma((2, 2, line)),
            dma((2, line)),
            dma((line, 2)),
            dma((line + 1, 2)),
            dma((line,)),
            dma((line + 1,)),
            dma((6,)),
            dma((6,)),
            dma,
            dma,
        ],
        compiler_params=pltpu.CompilerParams(
            collective_id=0, has_side_effects=True, vmem_limit_bytes=67_000_000
        ),
        name="exchange",
    )(tiles, links, lengths, images, state_grads, gain, shift, bias, up, down, down_bias, key, value, text.reshape(text_rows, -1), weight)


def on_column(
    images,
    ln_gain,
    ln_bias,
    fc1_weight,
    fc1_bias,
    fc2_weight,
    fc2_bias,
    key_weight,
    value_weight,
    text,
    query_weight,
    tiles,
    links,
    lengths,
    state_grads,
):
    slots, patch, width = images.shape[1:]
    context, fc1_grad, fc2_grad = exchange(
        tiles,
        links,
        lengths,
        images.reshape(slots * patch, width),
        state_grads.reshape(slots * patch, width),
        ln_gain,
        ln_bias,
        fc1_bias,
        fc1_weight,
        fc2_weight,
        fc2_bias,
        key_weight,
        value_weight,
        text,
        query_weight,
        patch,
    )
    return (context, fc1_grad, fc2_grad)


def on_device(
    images,
    ln_gain,
    ln_bias,
    fc1_weight,
    fc1_bias,
    fc2_weight,
    fc2_bias,
    key_weight,
    value_weight,
    text,
    query_weight,
    tiles,
    links,
    lengths,
    state_grads,
):
    dec_count = lax.axis_size("dec")
    grp_count = lax.axis_size("grp")
    enc_place = lax.axis_index("enc")
    dec_place = lax.axis_index("dec")
    grp_place = lax.axis_index("grp")
    slots = images.shape[1]
    patch = images.shape[2]
    width = images.shape[3]
    img_rows = slots * patch
    own_rows = images.reshape(img_rows, width)
    normed = normalize_layer(own_rows.astype(jnp.float32), ln_gain, ln_bias).astype(jnp.bfloat16)
    samples = text.shape[0]
    length = text.shape[1]
    text_rows = text.reshape(samples * length, text.shape[2])
    half = query_weight.shape[1] // grp_count
    own_half = lax.dynamic_slice_in_dim(query_weight, grp_place * half, half, 1)
    own_tiles = tiles[enc_place, dec_place, grp_place]
    tile_index = jnp.arange(slots)
    own_live = jnp.broadcast_to((tile_index < own_tiles)[:, None, None], (slots, patch, 1)).reshape(
        img_rows, 1
    )
    cotangent = jnp.where(
        own_live, state_grads.reshape(img_rows, width), jnp.zeros((), state_grads.dtype)
    )
    sent = jnp.stack([normed, cotangent])
    text_rows, own_half, _ = lax.optimization_barrier((text_rows, own_half, sent))
    both = lax.all_gather(sent, "enc", axis=1, tiled=True)
    gathered, all_cotangent = both[0], both[1]
    text_blocks = share_text(text_rows)
    pre, hidden, partial_full = encoder_rows(gathered, fc1_weight, fc1_bias, fc2_weight)
    partial_full = partial_full.astype(jnp.bfloat16)
    all_cotangent, _ = lax.optimization_barrier((all_cotangent, partial_full))
    first_term, second_term = weight_terms(gathered, pre, hidden, all_cotangent, fc2_weight)
    queries_of = project_queries(text_blocks, own_half, second_term)
    summed = lax.psum_scatter(
        partial_full, "enc", scatter_dimension=0, tiled=True
    ).astype(jnp.float32)
    states = (own_rows.astype(jnp.float32) + summed + fc2_bias).astype(jnp.bfloat16)
    local_heads = query_weight.shape[1] // HD
    per_group = HEADS // KV_HEADS
    kv_local = max(1, local_heads // per_group)
    first_head = dec_place * local_heads // per_group
    keys, values = share_keys(states, key_weight, value_weight, first_head, kv_local)
    heads_each = local_heads // kv_local
    queries = queries_of
    queries = queries.reshape(samples, length, kv_local, heads_each, HD)
    dec_tiles = tiles[enc_place, :, grp_place]
    live_keys = tile_index[None, :] < dec_tiles[:, None]
    live_keys = jnp.broadcast_to(live_keys[:, :, None], (dec_count, slots, patch)).reshape(
        dec_count, img_rows
    )
    allowed = (links[:, :, None] > 0) & live_keys[None, :, :]
    scores = jnp.einsum(
        "sqghd,jgkd->sghjkq", queries, keys, preferred_element_type=jnp.float32
    ) * HD ** (-0.5)
    weights = jnp.where(allowed[:, None, None, :, :, None], jnp.exp(scores), 0.0)
    totals = jnp.sum(weights, axis=(3, 4), keepdims=True)
    probs = (weights / totals).astype(jnp.bfloat16)
    mixed = jnp.einsum("sghjkq,jgkd->sqghd", probs, values, preferred_element_type=jnp.float32)
    valid = jnp.arange(length)[None, :] < lengths[:, None]
    context = (
        jnp.where(valid[:, :, None, None, None], mixed, 0.0)
        .reshape(samples, length, local_heads * HD)
        .astype(jnp.bfloat16)
    )
    fc1_grad, fc2_grad = share_grads(jnp.stack([first_term, second_term]))
    return (context, fc1_grad, fc2_grad)


def solution(mesh):
    in_specs = (
        P(("enc", "dec", "grp"), None, None, None),
        P(),
        P(),
        P("enc", None),
        P("enc"),
        P("enc", None),
        P(),
        P(),
        P(),
        P(("enc", "grp"), None, None),
        P("enc", "dec"),
        P(),
        P(("enc", "grp"), None),
        P(("enc", "grp")),
        P(("enc", "dec", "grp"), None, None, None),
    )
    out_specs = (
        P(("enc", "grp"), None, "dec"),
        P(("enc", "dec", "grp"), None),
        P(("enc", "dec", "grp"), None),
    )
    paired = mesh.shape["dec"] == 2 and mesh.shape["grp"] == 2 and mesh.shape["enc"] % 2 == 0
    if paired and mesh.shape["enc"] == 8:
        return jax.shard_map(
            on_column, mesh=mesh, in_specs=in_specs, out_specs=out_specs, check_vma=False
        )
    return jax.shard_map(
        on_device, mesh=mesh, in_specs=in_specs, out_specs=out_specs, check_vma=False
    )
```

```python
import functools

import jax
import jax.numpy as jnp
from jax import lax
from jax.experimental import pallas as pl
from jax.experimental.pallas import tpu as pltpu
from jax.sharding import PartitionSpec as P


HEADS = 32
KV_HEADS = 4
HD = 128


EPSILON = 1e-06


def normalize_layer(values, gain, shift):
    middle = jnp.mean(values, axis=-1, keepdims=True)
    centered = values - middle
    spread = jnp.mean(centered * centered, axis=-1, keepdims=True)
    return centered * lax.rsqrt(spread + EPSILON) * gain + shift


def normalize_heads(values):
    return values * lax.rsqrt(jnp.mean(values * values, axis=-1, keepdims=True) + EPSILON)


def gelu_slope(values):
    return (
        0.5 * (1.0 + lax.erf(values * 0.7071067811865476))
        + values * jnp.exp(-0.5 * values * values) * 0.3989422804014327
    )


def encoder_rows(rows, fc1_weight, fc1_bias, fc2_weight):
    pre = (
        lax.dot_general(
            rows, fc1_weight, (((1,), (1,)), ((), ())), preferred_element_type=jnp.float32
        )
        + fc1_bias
    )
    hidden = jax.nn.gelu(pre, approximate=False).astype(jnp.bfloat16)
    partial_sum = jnp.dot(hidden, fc2_weight, preferred_element_type=jnp.float32)
    return (pre, hidden, partial_sum)


def weight_terms(rows, pre, hidden, cotangent, fc2_weight):
    hidden_grad = lax.dot_general(
        cotangent, fc2_weight, (((1,), (1,)), ((), ())), preferred_element_type=jnp.float32
    )
    second_term = lax.dot_general(
        hidden, cotangent, (((0,), (0,)), ((), ())), preferred_element_type=jnp.float32
    )
    pre_grad = (hidden_grad * gelu_slope(pre)).astype(jnp.bfloat16)
    first_term = lax.dot_general(
        pre_grad, rows, (((0,), (0,)), ((), ())), preferred_element_type=jnp.float32
    )
    return (first_term, second_term)


def project_heads(states, key_columns, value_columns, heads):
    width = states.shape[-1]
    key_raw = jnp.einsum(
        "rd,dhe->hre",
        states,
        key_columns.reshape(width, heads, HD),
        preferred_element_type=jnp.float32,
    )
    keys = normalize_heads(key_raw).astype(jnp.bfloat16)
    values = jnp.einsum(
        "rd,dhe->hre",
        states,
        value_columns.reshape(width, heads, HD),
        preferred_element_type=jnp.float32,
    ).astype(jnp.bfloat16)
    return (keys, values)


def shifted(values, axis, step):
    size = lax.axis_size(axis)
    return lax.ppermute(values, axis, [(i, (i + step) % size) for i in range(size)])


def swapped(values):
    return lax.ppermute(values, "enc", [(i, i ^ 1) for i in range(lax.axis_size("enc"))])


def share_text(text_rows):
    enc_count = lax.axis_size("enc")
    _, depth = text_rows.shape
    side = lax.axis_index("enc") % 2
    block = depth // enc_count
    even = jnp.stack([text_rows[:, i * block : (i + 1) * block] for i in range(0, enc_count, 2)])
    odd = jnp.stack([text_rows[:, i * block : (i + 1) * block] for i in range(1, enc_count, 2)])
    own = jnp.where(side == 0, even, odd)
    away = jnp.where(side == 0, odd, even)
    arrived = swapped(away)
    pair = jnp.concatenate([arrived, own], axis=1)
    return jnp.concatenate(
        [pair] + [shifted(pair, "grp", step) for step in range(1, lax.axis_size("grp"))], axis=1
    )


def project_queries(text_blocks, weight, before):
    grp_count = lax.axis_size("grp")
    ring = lax.axis_size("enc") // 2
    enc_count = lax.axis_size("enc")
    place = lax.axis_index("enc") // 2
    total = None
    for step in range(ring):
        if step == max(0, ring - 2):
            weight, _ = lax.optimization_barrier((weight, before))
        left = lax.dynamic_index_in_dim(text_blocks, (place - step) % ring, 0, keepdims=False)
        term = jnp.dot(left, weight, preferred_element_type=jnp.float32)
        total = term if total is None else total + term
        if step < ring - 1:
            weight = lax.ppermute(
                weight, "enc", [(i, (i + 2) % enc_count) for i in range(enc_count)]
            )
    columns = total.shape[1]
    total = total.reshape(grp_count, 2, -1, columns)
    arrived = swapped(total[:, 0].astype(jnp.bfloat16))
    raw = total[:, 1] + arrived.astype(jnp.float32)
    own = normalize_heads(raw.reshape(grp_count, -1, columns // HD, HD)).astype(jnp.bfloat16)
    blocks = jnp.stack(
        [own[0]] + [shifted(own[step], "grp", -step) for step in range(1, grp_count)], axis=1
    )
    start = (grp_count - lax.axis_index("grp")) % grp_count
    blocks = lax.dynamic_slice_in_dim(
        jnp.concatenate([blocks, blocks], axis=1), start, grp_count, 1
    )
    return blocks.reshape(blocks.shape[0], grp_count * columns)


def share_keys(states, key_weight, value_weight, first_head, kv_local):
    dec_count = lax.axis_size("dec")
    rows, _ = states.shape
    if dec_count == 2 and kv_local * dec_count == KV_HEADS:
        keys, values = project_heads(states, key_weight, value_weight, KV_HEADS)
        paired = jnp.stack([keys, values])
        own = lax.dynamic_slice_in_dim(paired, first_head, kv_local, 1)
        away = lax.dynamic_slice_in_dim(paired, KV_HEADS - kv_local - first_head, kv_local, 1)
        arrived = shifted(away, "dec", 1)
        first = lax.axis_index("dec") == 0
        paired = jnp.stack(
            [jnp.where(first, own, arrived), jnp.where(first, arrived, own)], axis=1
        )
        return (paired[0], paired[1])
    key_columns = lax.dynamic_slice_in_dim(key_weight, first_head * HD, kv_local * HD, 1)
    value_columns = lax.dynamic_slice_in_dim(value_weight, first_head * HD, kv_local * HD, 1)
    piece = lax.all_gather(states, "dec", axis=0, tiled=True)
    key_part, value_part = project_heads(piece, key_columns, value_columns, kv_local)
    shape = (kv_local, dec_count, rows, HD)
    return (
        key_part.reshape(shape).transpose(1, 0, 2, 3),
        value_part.reshape(shape).transpose(1, 0, 2, 3),
    )


def share_grads(terms):
    dec_count = lax.axis_size("dec")
    grp_count = lax.axis_size("grp")
    rows = terms.shape[1] // (dec_count * grp_count)
    if dec_count == 2 and grp_count == 2:
        parts = terms.reshape(2, dec_count, grp_count, rows, -1)
        grp_place = lax.axis_index("grp")
        dec_place = lax.axis_index("dec")
        kept = lax.dynamic_index_in_dim(parts, grp_place, 2, keepdims=False)
        away = lax.dynamic_index_in_dim(parts, 1 - grp_place, 2, keepdims=False)
        kept = kept + shifted(away.astype(jnp.bfloat16), "grp", 1).astype(jnp.float32)
        away = lax.dynamic_index_in_dim(kept, 1 - dec_place, 1, keepdims=False)
        kept = lax.dynamic_index_in_dim(kept, dec_place, 1, keepdims=False)
        kept = kept + shifted(away.astype(jnp.bfloat16), "dec", 1).astype(jnp.float32)
        return (kept[0], kept[1])
    summed = lax.psum_scatter(
        terms.astype(jnp.bfloat16), ("dec", "grp"), scatter_dimension=1, tiled=True
    ).astype(jnp.float32)
    return (summed[0], summed[1])


MESH = pl.DeviceIdType.MESH


def pick(table, place):
    return sum(jnp.where(place == i, value, 0) for i, value in enumerate(table))


def step_kernel(
    line,
    patch,
    tiles_ref,
    links_ref,
    lengths_ref,
    images_ref,
    state_grads_ref,
    gain_ref,
    shift_ref,
    bias_ref,
    up_ref,
    down_ref,
    down_bias_ref,
    key_ref,
    value_ref,
    text_ref,
    weight_ref,
    context_ref,
    up_grad_ref,
    down_grad_ref,
    own,
    kw,
    kv_send,
    kv,
    queries,
    acc,
    tb,
    wb,
    fb,
    bb,
    bias_col,
    rows,
    pre,
    hid_t,
    hid,
    pg_t,
    po,
    psend,
    precv,
    msend,
    mrecv,
    gs1,
    gr1,
    gs2,
    gr2,
    gs3,
    gr3,
    local_sem,
    t_send,
    t_recv,
    y_send,
    y_recv,
    x_send,
    x_recv,
    s_send,
    s_recv,
    a_send,
    a_recv,
    p_send,
    p_recv,
    m_send,
    m_recv,
    g_send,
    g_recv,
    k_send,
    k_recv,
):
    f32 = jnp.float32
    bf16 = jnp.bfloat16
    enc = lax.axis_index("enc")
    y = lax.axis_index("dec")
    g = lax.axis_index("grp")
    z, x = enc // 2, enc % 2
    other_x = ((z * 2 + 1 - x), y, g)
    other_y = (enc, 1 - y, g)
    other_g = (enc, y, 1 - g)

    def along(place):
        return (place * 2 + x, y, g)

    orders = []
    for p in range(line):
        others = [a for a in range(line) if a != p]
        others.sort(key=lambda a: (-abs(a - p), min(a, line - 1 - a)))
        orders.append(others)
    order = [pick([orders[p][i] for p in range(line)], z) for i in range(line - 1)]
    text_rows, depth = tb.shape[2], tb.shape[3]
    half_cols = wb.shape[3]
    img = rows.shape[2]
    width = rows.shape[3]
    units = fb.shape[2]
    piece = units // 2
    part = units // 4

    barrier = pltpu.get_barrier_semaphore()
    for k in range(line):

        @pl.when(z != k)
        def _():
            pl.semaphore_signal(barrier, inc=1, device_id=along(k), device_id_type=MESH)

    for to in (other_x, other_y, other_g):
        pl.semaphore_signal(barrier, inc=1, device_id=to, device_id_type=MESH)
    pl.semaphore_wait(barrier, line + 2)

    def remote(src, dst, send, recv, to):
        return pltpu.make_async_remote_copy(
            src_ref=src, dst_ref=dst, send_sem=send, recv_sem=recv, device_id=to, device_id_type=MESH
        )

    def text_copy(i):
        b = order[i]
        at = pl.multiple_of((b * 2 + y) * depth, depth)
        return remote(
            text_ref.at[:, pl.ds(at, depth)], tb.at[z, y], t_send.at[i], t_recv.at[z], along(b)
        )

    def text_landed(a):
        return remote(tb.at[a, y], tb.at[a, y], t_send.at[0], t_recv.at[a], other_y)

    def text_relay(a):
        return remote(tb.at[a, y], tb.at[a, y], y_send.at[a], y_recv.at[a], other_y)

    def text_relayed(a):
        return remote(tb.at[a, 1 - y], tb.at[a, 1 - y], y_send.at[a], y_recv.at[a], other_y)

    quarter = half_cols // 2

    def weight_source(c, core):
        at = pl.multiple_of(core * half_cols + c * quarter, quarter)
        return weight_ref.at[:, pl.ds(at, quarter)]

    def weight_spot(k, c, core):
        return wb.at[k, c, :, pl.ds(pl.multiple_of(core * quarter, quarter), quarter)]

    def weight_x(c):
        return remote(
            weight_source(c, g), weight_spot(x, c, g), x_send.at[4 + c], x_recv.at[4 + c], other_x
        )

    def weight_copy(c, core, send, recv, to):
        spot = weight_spot(1 - x, c, core)
        return remote(spot, spot, send, recv, to)

    def weight_x_in(c):
        return weight_copy(c, g, x_send.at[4 + c], x_recv.at[4 + c], other_x)

    def weight_s(c):
        return weight_copy(c, g, s_send.at[5 + c], s_recv.at[5 + c], other_g)

    def weight_s_in(c):
        return weight_copy(c, 1 - g, s_send.at[5 + c], s_recv.at[5 + c], other_g)

    def unit_rows(core, q):
        return pl.ds(pl.multiple_of(core * piece + q * part, part), part)

    def unit_x(ref, kind, q):
        return remote(
            ref.at[unit_rows(g, q)],
            fb.at[kind, x, unit_rows(g, q)],
            x_send.at[1 + q],
            x_recv.at[1 + q],
            other_x,
        )

    def unit_copy(kind, core, q, send, recv, to):
        spot = fb.at[kind, 1 - x, unit_rows(core, q)]
        return remote(spot, spot, send, recv, to)

    def unit_x_in(q):
        return unit_copy(y, g, q, x_send.at[1 + q], x_recv.at[1 + q], other_x)

    def unit_s(q):
        return unit_copy(y, g, q, s_send.at[1 + q], s_recv.at[1 + q], other_g)

    def unit_s_in(q):
        return unit_copy(y, 1 - g, q, s_send.at[1 + q], s_recv.at[1 + q], other_g)

    def unit_y(q):
        return unit_copy(y, g, q, y_send.at[line + q], y_recv.at[line + q], other_y)

    def unit_y_in(q):
        return unit_copy(1 - y, g, q, y_send.at[line + q], y_recv.at[line + q], other_y)

    def unit_s2(q):
        return unit_copy(1 - y, g, q, s_send.at[3 + q], s_recv.at[3 + q], other_g)

    def unit_s2_in(q):
        return unit_copy(1 - y, 1 - g, q, s_send.at[3 + q], s_recv.at[3 + q], other_g)

    bb[x] = bias_ref[...][None]
    bias_x = remote(bb.at[x], bb.at[x], x_send.at[3], x_recv.at[3], other_x)
    bias_x_in = remote(bb.at[1 - x], bb.at[1 - x], x_send.at[3], x_recv.at[3], other_x)

    def rows_copy(m, a, right):
        to = along(z + 1) if right else along(z - 1)
        spot = rows.at[m, a]
        return remote(spot, spot, a_send.at[1 if right else 0, m, a], a_recv.at[m, a], to)

    def rows_landed(m, a):
        return remote(rows.at[m, a], rows.at[m, a], a_send.at[0, m, a], a_recv.at[m, a], other_y)

    locals_ = [
        pltpu.make_async_copy(weight_source(c, k), weight_spot(x, c, k), local_sem.at[11 + c * 2 + k])
        for c in range(2)
        for k in range(2)
    ] + [
        pltpu.make_async_copy(up_ref, fb.at[0, x], local_sem.at[2]),
        pltpu.make_async_copy(down_ref, fb.at[1, x], local_sem.at[3]),
        pltpu.make_async_copy(key_ref, kw.at[0], local_sem.at[5]),
        pltpu.make_async_copy(value_ref, kw.at[1], local_sem.at[8]),
    ] + [
        pltpu.make_async_copy(
            text_ref.at[:, pl.ds(pl.multiple_of((z * 2 + h) * depth, depth), depth)],
            tb.at[z, h],
            local_sem.at[6 + h],
        )
        for h in range(2)
    ]

    for i in range(line - 1):
        text_copy(i).start()
    for c in range(2):
        weight_x(c).start()
    own_copies = [
        pltpu.make_async_copy(images_ref, own.at[0], local_sem.at[9]),
        pltpu.make_async_copy(state_grads_ref, own.at[1], local_sem.at[10]),
    ]
    for copy in own_copies + locals_:
        copy.start()
    for copy in own_copies:
        copy.wait()

    def live_rows(j):
        return tiles_ref[j, g, enc] * patch

    own_live = live_rows(y)

    def norm_body(t, _):
        r = pl.ds(pl.multiple_of(t * 16, 16), 16)
        normed = normalize_layer(own[0, r].astype(f32), gain_ref[...][None], shift_ref[...][None])
        rows[0, z, r] = normed.astype(bf16)
        row = t * 16 + lax.broadcasted_iota(jnp.int32, (16, width), 0)
        rows[1, z, r] = jnp.where(row < own_live, own[1, r].astype(f32), 0.0).astype(bf16)
        return 0

    lax.fori_loop(0, img // 16, norm_body, 0)

    for m in range(2):

        @pl.when(z < line - 1)
        def _(m=m):
            rows_copy(m, z, True).start()

        @pl.when(z > 0)
        def _(m=m):
            rows_copy(m, z, False).start()

    def forward_rows(m, s):
        @pl.when(z - s >= 0)
        def _():
            rows_landed(m, z - s).wait_recv()

            @pl.when(z < line - 1)
            def _():
                rows_copy(m, z - s, True).start()

        @pl.when(z + s <= line - 1)
        def _():
            rows_landed(m, z + s).wait_recv()

            @pl.when(z > 0)
            def _():
                rows_copy(m, z + s, False).start()

    def has_incoming(a):
        return jnp.logical_or(
            jnp.logical_and(a > z, z > 0), jnp.logical_and(a < z, z < line - 1)
        )

    def next_slot(a):
        right = a > z
        to = jnp.where(right, z + 1, z - 1)
        slot = jnp.where(jnp.logical_and(to == a, jnp.logical_not(right)), line, a)
        return to, slot

    def sum_copy(a, c):
        to, slot = next_slot(a)
        return remote(psend.at[a, c], precv.at[slot, c], p_send.at[a, c], p_recv.at[slot, c], along(to))

    def sum_landed(slot, c):
        return remote(precv.at[slot, c], precv.at[slot, c], p_send.at[0, c], p_recv.at[slot, c], other_y)

    tile = 256

    def multiply(a, c, store):
        def body(t, _):
            cols = pl.ds(pl.multiple_of(t * tile, tile), tile)
            total = jnp.dot(tb[a, 0], wb[0, c, :, cols], preferred_element_type=f32)
            total = total + jnp.dot(tb[a, 1], wb[1, c, :, cols], preferred_element_type=f32)
            store(t, cols, total)
            return 0

        lax.fori_loop(0, half_cols // tile, body, 0)

    def product(i, c):
        a = order[i]

        def store(t, cols, total):
            psend[a, c, :, cols] = total.astype(bf16)

        multiply(a, c, store)

    def send_product(i, c):
        a = order[i]

        @pl.when(jnp.logical_not(has_incoming(a)))
        def _():
            sum_copy(a, c).start()

    def add_incoming(i, c):
        a = order[i]

        @pl.when(has_incoming(a))
        def _():
            sum_landed(a, c).wait_recv()

            def body(t, _):
                r = pl.ds(pl.multiple_of(t * 16, 16), 16)
                psend[a, c, r] = (psend[a, c, r].astype(f32) + precv[a, c, r].astype(f32)).astype(bf16)
                return 0

            lax.fori_loop(0, text_rows // 16, body, 0)
            sum_copy(a, c).start()

    held = ((line - 2, 0), (line - 2, 1))

    def products(i):
        text_relayed(order[i]).wait_recv()
        for c in range(2):
            product(i, c)
            if (i, c) not in held:
                send_product(i, c)

    def relay_units(q):
        unit_x_in(q).wait_recv()
        unit_s(q).start()
        unit_y(q).start()

    def relay_text(i):
        text_landed(order[i]).wait_recv()
        text_relay(order[i]).start()

    relay_text(0)
    weight_x_in(0).wait_recv()
    weight_s(0).start()
    for copy in locals_:
        copy.wait()
    text_relayed(order[0]).wait_recv()
    weight_s_in(0).wait_recv()
    product(0, 0)
    send_product(0, 0)
    for i in range(1, line - 1):
        relay_text(i)
    weight_x_in(1).wait_recv()
    weight_s(1).start()
    for c in range(2):
        weight_x(c).wait_send()

    @pl.when(y == 0)
    def _():
        for q in range(2):
            unit_x(up_ref, 0, q).start()

    @pl.when(y == 1)
    def _():
        for q in range(2):
            unit_x(down_ref, 1, q).start()

    bias_x.start()

    weight_s_in(1).wait_recv()
    product(0, 1)
    send_product(0, 1)
    forward_rows(0, 1)
    relay_units(0)
    products(1)
    add_incoming(0, 0)
    for m in range(2):
        forward_rows(m, 2 - m)
    relay_units(1)
    for i in range(2, line - 1):
        products(i)
    unit_y_in(0).wait_recv()
    unit_s2(0).start()
    add_incoming(0, 1)
    forward_rows(0, 3)
    unit_y_in(1).wait_recv()
    unit_s2(1).start()
    bias_x_in.wait_recv()
    for q in range(2):
        unit_s_in(q).wait_recv()
        unit_s2_in(q).wait_recv()

    all_rows = line * img

    def up_body(q, _):
        k = q // 2
        at = pl.multiple_of((q % 2) * piece, piece)
        pre[k, pl.ds(at, piece)] = lax.dot_general(
            fb[0, k, pl.ds(at, piece)],
            rows[0].reshape(all_rows, width),
            (((1,), (1,)), ((), ())),
            preferred_element_type=f32,
        )
        return 0

    lax.fori_loop(0, 4, up_body, 0)
    forward_rows(1, 2)
    for k in range(2):
        for t in range(units // 128):
            spot = slice(t * 128, (t + 1) * 128)
            bias_col[k, spot] = jnp.transpose(jnp.broadcast_to(bb[k, :, spot], (8, 128)))

    def gelu_body(r, _):
        k = r // (units // 16)
        at = pl.ds(pl.multiple_of((r % (units // 16)) * 16, 16), 16)
        value = pre[k, at] + bias_col[k, at, 0:1]
        phi = 0.5 * (1.0 + lax.erf(value * 0.7071067811865476))
        hid_t[k, at] = (value * phi).astype(bf16)
        pre[k, at] = phi + value * jnp.exp(-0.5 * value * value) * 0.3989422804014327
        return 0

    lax.fori_loop(0, 2 * units // 16, gelu_body, 0, unroll=4)

    def terms(kind, k, j, owner):
        at = pl.ds(pl.multiple_of(j * piece + owner * part, part), part)
        left = pg_t if kind == 0 else hid_t
        return jnp.dot(left[k, at], rows[kind].reshape(all_rows, width), preferred_element_type=f32)

    grads_s = [remote(gs1.at[m], gr1.at[m], g_send.at[m], g_recv.at[m], other_g) for m in range(2)]
    grads_y = remote(gs2.at[0], gr2.at[0], g_send.at[2], g_recv.at[2], other_y)
    grads_x = remote(gs2.at[1], gr2.at[1], g_send.at[3], g_recv.at[3], other_x)
    grads_x2 = remote(gs3.at[0], gr3.at[0], g_send.at[4], g_recv.at[4], other_x)
    grads_y2 = remote(gs3.at[1], gr3.at[1], g_send.at[5], g_recv.at[5], other_y)

    def share_core(kind):
        def body(q, _):
            k, j = q // 2, q % 2
            gs1[kind, k, j] = terms(kind, k, j, 1 - g).astype(bf16)
            return 0

        lax.fori_loop(0, 4, body, 0)
        grads_s[kind].start()

    def flip_body(t, _):
        for k in range(2):
            at = pl.ds(pl.multiple_of(t * 128, 128), 128)
            hid[k, :, at] = jnp.transpose(hid_t[k, at].astype(f32)).astype(bf16)
        return 0

    lax.fori_loop(0, units // 128, flip_body, 0)

    def down_body(t, _):
        cols = pl.ds(pl.multiple_of(t * tile, tile), tile)
        total = jnp.dot(hid[0], fb[1, 0, :, cols], preferred_element_type=f32)
        po[:, cols] = total + jnp.dot(hid[1], fb[1, 1, :, cols], preferred_element_type=f32)
        return 0

    lax.fori_loop(0, width // tile, down_body, 0)

    def state_copy(a):
        to, slot = next_slot(a)
        return remote(msend.at[a], mrecv.at[slot], m_send.at[a], m_recv.at[slot], along(to))

    def state_landed(slot):
        return remote(mrecv.at[slot], mrecv.at[slot], m_send.at[0], m_recv.at[slot], other_y)

    def send_state(i, first):
        a = order[i]
        waits = has_incoming(a)

        @pl.when(jnp.logical_not(waits) if first else waits)
        def _():
            if not first:
                state_landed(a).wait_recv()

            def body(t, _):
                r = pl.ds(pl.multiple_of(t * 16, 16), 16)
                value = po[pl.ds(pl.multiple_of(a * img + t * 16, 16), 16)]
                if not first:
                    value = value + mrecv[a, r].astype(f32)
                msend[a, r] = value.astype(bf16)
                return 0

            lax.fori_loop(0, img // 16, body, 0)
            state_copy(a).start()

    for i in range(line - 1):
        send_state(i, True)
    for c in range(2):
        send_product(line - 2, c)
    add_incoming(1, 0)
    add_incoming(2, 0)
    forward_rows(1, 3)
    share_core(1)

    def slope_body(q, _):
        k = q // 2
        at = pl.ds(pl.multiple_of((q % 2) * piece, piece), piece)
        grad = lax.dot_general(
            fb[1, k, at],
            rows[1].reshape(all_rows, width),
            (((1,), (1,)), ((), ())),
            preferred_element_type=f32,
        )
        pg_t[k, at] = (grad * pre[k, at]).astype(bf16)
        return 0

    lax.fori_loop(0, 4, slope_body, 0)
    share_core(0)

    grads_s[1].wait_recv()

    def away_x(j, _):
        gs2[1, j] = (terms(1, 1 - x, j, g) + gr1[1, 1 - x, j].astype(f32)).astype(bf16)
        return 0

    lax.fori_loop(0, 2, away_x, 0)
    grads_x.start()
    grads_s[0].wait_recv()

    def away_y(k, _):
        gs2[0, k] = (terms(0, k, 1 - y, g) + gr1[0, k, 1 - y].astype(f32)).astype(bf16)
        return 0

    lax.fori_loop(0, 2, away_y, 0)
    grads_y.start()
    add_incoming(1, 1)
    send_state(0, False)
    send_state(2, False)
    add_incoming(2, 1)
    send_state(1, False)
    grads_x.wait_recv()
    total = terms(1, x, 1 - y, g) + gr1[1, x, 1 - y].astype(f32)
    gs3[1] = (total + gr2[1, 1 - y].astype(f32)).astype(bf16)
    grads_y2.start()
    grads_y.wait_recv()
    total = terms(0, 1 - x, y, g) + gr1[0, 1 - x, y].astype(f32)
    gs3[0] = (total + gr2[0, 1 - x].astype(f32)).astype(bf16)
    grads_x2.start()

    def own_products(c):
        def store(t, cols, total):
            acc[c, :, cols] = total

        multiply(z, c, store)

    def own_texts(c):
        @pl.when(z > 0)
        def _():
            sum_landed(z, c).wait_recv()

        @pl.when(z < line - 1)
        def _():
            sum_landed(line, c).wait_recv()

        def body(t, _):
            r = pl.ds(pl.multiple_of(t * 32, 32), 32)
            for h in range(half_cols // HD):
                spot = slice(h * HD, (h + 1) * HD)
                head = acc[c, r, spot]
                head = head + jnp.where(z > 0, precv[z, c, r, spot].astype(f32), 0.0)
                head = head + jnp.where(z < line - 1, precv[line, c, r, spot].astype(f32), 0.0)
                queries[r, spot] = normalize_heads(head).astype(bf16)
            return 0

        lax.fori_loop(0, text_rows // 32, body, 0)

    for c in range(2):
        own_products(c)

    slot_rows = pl.ds(pl.multiple_of(z * img, img), img)
    po[slot_rows] = po[slot_rows] + own[0].astype(f32) + down_bias_ref[...][None]

    @pl.when(z > 0)
    def _():
        state_landed(z).wait_recv()
        po[slot_rows] = po[slot_rows] + mrecv[z].astype(f32)

    @pl.when(z < line - 1)
    def _():
        state_landed(line).wait_recv()
        po[slot_rows] = po[slot_rows] + mrecv[line].astype(f32)

    states = po[slot_rows].astype(bf16)
    local = kv.shape[2]
    own_rows = pl.ds(pl.multiple_of(y * img, img), img)
    away_rows = pl.ds(pl.multiple_of((1 - y) * img, img), img)
    kv_copy = remote(kv_send, kv.at[:, own_rows], k_send, k_recv, other_y)
    kv_in = remote(kv.at[:, away_rows], kv.at[:, away_rows], k_send, k_recv, other_y)
    for sent in (True, False):
        at = pl.multiple_of(((1 - y) if sent else y) * local, local)
        spot = kv_send if sent else kv.at[:, own_rows]
        raw = jnp.dot(states, kw[0, :, pl.ds(at, local)], preferred_element_type=f32)
        for h in range(local // HD):
            head = normalize_heads(raw[:, h * HD : (h + 1) * HD])
            spot[0, :, h * HD : (h + 1) * HD] = head.astype(bf16)
        raw = jnp.dot(states, kw[1, :, pl.ds(at, local)], preferred_element_type=f32)
        spot[1] = raw.astype(bf16)
        if sent:
            kv_copy.start()

    samples, length = context_ref.shape[:2]
    group = half_cols // HD

    def attend_texts(c):
        key = lax.broadcasted_iota(jnp.int32, (length, 2 * img), 1)

        def body(n, _):
            r = pl.ds(pl.multiple_of(n * length, length), length)
            limits = [jnp.where(links_ref[n, j] > 0, live_rows(j), 0) for j in range(2)]
            allowed = key < jnp.where(key < img, limits[0], limits[1] + img)
            valid = lax.broadcasted_iota(jnp.int32, (length, HD), 0) < lengths_ref[n]
            for h in range(group):
                shared = h // (group // 2)
                head_cols = slice(shared * HD, (shared + 1) * HD)
                first = shared * half_cols + c * quarter + (h % (group // 2)) * HD
                cols = slice(first, first + HD)
                score = lax.dot_general(
                    queries[r, h * HD : (h + 1) * HD],
                    kv[0, :, head_cols],
                    (((1,), (1,)), ((), ())),
                    preferred_element_type=f32,
                )
                weights = jnp.where(allowed, jnp.exp(score * HD ** (-0.5)), 0.0)
                scale = 1.0 / jnp.sum(weights, axis=-1, keepdims=True)
                mixed = jnp.dot(
                    (weights * scale).astype(bf16), kv[1, :, head_cols], preferred_element_type=f32
                )
                context_ref[n, :, cols] = jnp.where(valid, mixed, 0.0).astype(bf16)
            return 0

        lax.fori_loop(0, samples, body, 0)

    own_texts(0)
    for kind, out in ((1, down_grad_ref), (0, up_grad_ref)):
        (grads_x2, grads_y2)[kind].wait_recv()
        total = terms(kind, x, y, g) + gr1[kind, x, y].astype(f32)
        total = total + gr2[kind, (x, y)[kind]].astype(f32)
        out[...] = total + gr3[kind].astype(f32)

    kv_in.wait_recv()
    attend_texts(0)
    own_texts(1)
    attend_texts(1)
    for i in range(line - 1):
        a = order[i]
        text_copy(i).wait_send()
        text_relay(a).wait_send()
        state_copy(a).wait_send()
        for c in range(2):
            sum_copy(a, c).wait_send()
    for copy in (kv_copy, weight_s(0), weight_s(1), bias_x, *grads_s, grads_y, grads_x, grads_x2, grads_y2):
        copy.wait_send()
    for q in range(2):
        for copy in (unit_x(up_ref, 0, q), unit_s(q), unit_y(q), unit_s2(q)):
            copy.wait_send()

    for a in range(line):

        @pl.when(jnp.logical_and(a <= z, z < line - 1))
        def _():
            for m in range(2):
                rows_copy(m, a, True).wait_send()

        @pl.when(jnp.logical_and(a >= z, z > 0))
        def _():
            for m in range(2):
                rows_copy(m, a, False).wait_send()


def exchange(
    tiles, links, lengths, images, state_grads, gain, shift, bias, up, down, down_bias, key, value, text, weight, patch
):
    line = lax.axis_size("enc") // 2
    text_rows = text.shape[0] * text.shape[1]
    depth, columns = weight.shape
    img, width = images.shape
    units = up.shape[0]
    half = columns // 2
    local = key.shape[1] // 2
    f32, bf16 = jnp.float32, jnp.bfloat16
    dma = pltpu.SemaphoreType.DMA
    part = units // 4
    smem = pl.BlockSpec(memory_space=pltpu.SMEM)
    vmem = pl.BlockSpec(memory_space=pltpu.VMEM)
    anywhere = pl.BlockSpec(memory_space=pl.ANY)
    return pl.pallas_call(
        functools.partial(step_kernel, line, patch),
        out_shape=[
            jax.ShapeDtypeStruct((*text.shape[:2], columns), bf16),
            jax.ShapeDtypeStruct((part, width), f32),
            jax.ShapeDtypeStruct((part, width), f32),
        ],
        in_specs=[smem] * 3 + [anywhere] * 2 + [vmem] * 3 + [anywhere] * 2 + [vmem] + [anywhere] * 4,
        out_specs=[vmem] * 3,
        scratch_shapes=[
            pltpu.VMEM((2, img, width), bf16),
            pltpu.VMEM((2, width, 2 * local), bf16),
            pltpu.VMEM((2, img, local), bf16),
            pltpu.VMEM((2, 2 * img, local), bf16),
            pltpu.VMEM((text_rows, half), bf16),
            pltpu.VMEM((2, text_rows, half), f32),
            pltpu.VMEM((line, 2, text_rows, depth), bf16),
            pltpu.VMEM((2, 2, depth, half), bf16),
            pltpu.VMEM((2, 2, units, width), bf16),
            pltpu.VMEM((2, 1, units), f32),
            pltpu.VMEM((2, units, 8), f32),
            pltpu.VMEM((2, line, img, width), bf16),
            pltpu.VMEM((2, units, line * img), f32),
            pltpu.VMEM((2, units, line * img), bf16),
            pltpu.VMEM((2, line * img, units), bf16),
            pltpu.VMEM((2, units, line * img), bf16),
            pltpu.VMEM((line * img, width), f32),
            pltpu.VMEM((line, 2, text_rows, half), bf16),
            pltpu.VMEM((line + 1, 2, text_rows, half), bf16),
            pltpu.VMEM((line, img, width), bf16),
            pltpu.VMEM((line + 1, img, width), bf16),
            pltpu.VMEM((2, 2, 2, part, width), bf16),
            pltpu.VMEM((2, 2, 2, part, width), bf16),
            pltpu.VMEM((2, 2, part, width), bf16),
            pltpu.VMEM((2, 2, part, width), bf16),
            pltpu.VMEM((2, part, width), bf16),
            pltpu.VMEM((2, part, width), bf16),
            dma((15,)),
            dma((line - 1,)),
            dma((line,)),
            dma((line + 2,)),
            dma((line + 2,)),
            dma((6,)),
            dma((6,)),
            dma((7,)),
            dma((7,)),
            dma((2, 2, line)),
            dma((2, line)),
            dma((line, 2)),
            dma((line + 1, 2)),
            dma((line,)),
            dma((line + 1,)),
            dma((6,)),
            dma((6,)),
            dma,
            dma,
        ],
        compiler_params=pltpu.CompilerParams(
            collective_id=0, has_side_effects=True, vmem_limit_bytes=67_000_000
        ),
        name="exchange",
    )(tiles, links, lengths, images, state_grads, gain, shift, bias, up, down, down_bias, key, value, text.reshape(text_rows, -1), weight)


def on_column(
    images,
    ln_gain,
    ln_bias,
    fc1_weight,
    fc1_bias,
    fc2_weight,
    fc2_bias,
    key_weight,
    value_weight,
    text,
    query_weight,
    tiles,
    links,
    lengths,
    state_grads,
):
    slots, patch, width = images.shape[1:]
    context, fc1_grad, fc2_grad = exchange(
        tiles.transpose(1, 2, 0),
        links,
        lengths,
        images.reshape(slots * patch, width),
        state_grads.reshape(slots * patch, width),
        ln_gain,
        ln_bias,
        fc1_bias,
        fc1_weight,
        fc2_weight,
        fc2_bias,
        key_weight,
        value_weight,
        text,
        query_weight,
        patch,
    )
    return (context, fc1_grad, fc2_grad)


def on_device(
    images,
    ln_gain,
    ln_bias,
    fc1_weight,
    fc1_bias,
    fc2_weight,
    fc2_bias,
    key_weight,
    value_weight,
    text,
    query_weight,
    tiles,
    links,
    lengths,
    state_grads,
):
    dec_count = lax.axis_size("dec")
    grp_count = lax.axis_size("grp")
    enc_place = lax.axis_index("enc")
    dec_place = lax.axis_index("dec")
    grp_place = lax.axis_index("grp")
    slots = images.shape[1]
    patch = images.shape[2]
    width = images.shape[3]
    img_rows = slots * patch
    own_rows = images.reshape(img_rows, width)
    normed = normalize_layer(own_rows.astype(jnp.float32), ln_gain, ln_bias).astype(jnp.bfloat16)
    samples = text.shape[0]
    length = text.shape[1]
    text_rows = text.reshape(samples * length, text.shape[2])
    half = query_weight.shape[1] // grp_count
    own_half = lax.dynamic_slice_in_dim(query_weight, grp_place * half, half, 1)
    own_tiles = tiles[enc_place, dec_place, grp_place]
    tile_index = jnp.arange(slots)
    own_live = jnp.broadcast_to((tile_index < own_tiles)[:, None, None], (slots, patch, 1)).reshape(
        img_rows, 1
    )
    cotangent = jnp.where(
        own_live, state_grads.reshape(img_rows, width), jnp.zeros((), state_grads.dtype)
    )
    sent = jnp.stack([normed, cotangent])
    text_rows, own_half, _ = lax.optimization_barrier((text_rows, own_half, sent))
    both = lax.all_gather(sent, "enc", axis=1, tiled=True)
    gathered, all_cotangent = both[0], both[1]
    text_blocks = share_text(text_rows)
    pre, hidden, partial_full = encoder_rows(gathered, fc1_weight, fc1_bias, fc2_weight)
    partial_full = partial_full.astype(jnp.bfloat16)
    all_cotangent, _ = lax.optimization_barrier((all_cotangent, partial_full))
    first_term, second_term = weight_terms(gathered, pre, hidden, all_cotangent, fc2_weight)
    queries_of = project_queries(text_blocks, own_half, second_term)
    summed = lax.psum_scatter(
        partial_full, "enc", scatter_dimension=0, tiled=True
    ).astype(jnp.float32)
    states = (own_rows.astype(jnp.float32) + summed + fc2_bias).astype(jnp.bfloat16)
    local_heads = query_weight.shape[1] // HD
    per_group = HEADS // KV_HEADS
    kv_local = max(1, local_heads // per_group)
    first_head = dec_place * local_heads // per_group
    keys, values = share_keys(states, key_weight, value_weight, first_head, kv_local)
    heads_each = local_heads // kv_local
    queries = queries_of
    queries = queries.reshape(samples, length, kv_local, heads_each, HD)
    dec_tiles = tiles[enc_place, :, grp_place]
    live_keys = tile_index[None, :] < dec_tiles[:, None]
    live_keys = jnp.broadcast_to(live_keys[:, :, None], (dec_count, slots, patch)).reshape(
        dec_count, img_rows
    )
    allowed = (links[:, :, None] > 0) & live_keys[None, :, :]
    scores = jnp.einsum(
        "sqghd,jgkd->sghjkq", queries, keys, preferred_element_type=jnp.float32
    ) * HD ** (-0.5)
    weights = jnp.where(allowed[:, None, None, :, :, None], jnp.exp(scores), 0.0)
    totals = jnp.sum(weights, axis=(3, 4), keepdims=True)
    probs = (weights / totals).astype(jnp.bfloat16)
    mixed = jnp.einsum("sghjkq,jgkd->sqghd", probs, values, preferred_element_type=jnp.float32)
    valid = jnp.arange(length)[None, :] < lengths[:, None]
    context = (
        jnp.where(valid[:, :, None, None, None], mixed, 0.0)
        .reshape(samples, length, local_heads * HD)
        .astype(jnp.bfloat16)
    )
    fc1_grad, fc2_grad = share_grads(jnp.stack([first_term, second_term]))
    return (context, fc1_grad, fc2_grad)


def solution(mesh):
    in_specs = (
        P(("enc", "dec", "grp"), None, None, None),
        P(),
        P(),
        P("enc", None),
        P("enc"),
        P("enc", None),
        P(),
        P(),
        P(),
        P(("enc", "grp"), None, None),
        P("enc", "dec"),
        P(),
        P(("enc", "grp"), None),
        P(("enc", "grp")),
        P(("enc", "dec", "grp"), None, None, None),
    )
    out_specs = (
        P(("enc", "grp"), None, "dec"),
        P(("enc", "dec", "grp"), None),
        P(("enc", "dec", "grp"), None),
    )
    paired = mesh.shape["dec"] == 2 and mesh.shape["grp"] == 2 and mesh.shape["enc"] % 2 == 0
    if paired and mesh.shape["enc"] == 8:
        return jax.shard_map(
            on_column, mesh=mesh, in_specs=in_specs, out_specs=out_specs, check_vma=False
        )
    return jax.shard_map(
        on_device, mesh=mesh, in_specs=in_specs, out_specs=out_specs, check_vma=False
    )
```

```python
import functools

import jax
import jax.numpy as jnp
from jax import lax
from jax.experimental import pallas as pl
from jax.experimental.pallas import tpu as pltpu
from jax.sharding import PartitionSpec as P


HEADS = 32
KV_HEADS = 4
HD = 128


EPSILON = 1e-06


def normalize_layer(values, gain, shift):
    middle = jnp.mean(values, axis=-1, keepdims=True)
    centered = values - middle
    spread = jnp.mean(centered * centered, axis=-1, keepdims=True)
    return centered * lax.rsqrt(spread + EPSILON) * gain + shift


def normalize_heads(values):
    return values * lax.rsqrt(jnp.mean(values * values, axis=-1, keepdims=True) + EPSILON)


def gelu_slope(values):
    return (
        0.5 * (1.0 + lax.erf(values * 0.7071067811865476))
        + values * jnp.exp(-0.5 * values * values) * 0.3989422804014327
    )


def encoder_rows(rows, fc1_weight, fc1_bias, fc2_weight):
    pre = (
        lax.dot_general(
            rows, fc1_weight, (((1,), (1,)), ((), ())), preferred_element_type=jnp.float32
        )
        + fc1_bias
    )
    hidden = jax.nn.gelu(pre, approximate=False).astype(jnp.bfloat16)
    partial_sum = jnp.dot(hidden, fc2_weight, preferred_element_type=jnp.float32)
    return (pre, hidden, partial_sum)


def weight_terms(rows, pre, hidden, cotangent, fc2_weight):
    hidden_grad = lax.dot_general(
        cotangent, fc2_weight, (((1,), (1,)), ((), ())), preferred_element_type=jnp.float32
    )
    second_term = lax.dot_general(
        hidden, cotangent, (((0,), (0,)), ((), ())), preferred_element_type=jnp.float32
    )
    pre_grad = (hidden_grad * gelu_slope(pre)).astype(jnp.bfloat16)
    first_term = lax.dot_general(
        pre_grad, rows, (((0,), (0,)), ((), ())), preferred_element_type=jnp.float32
    )
    return (first_term, second_term)


def project_heads(states, key_columns, value_columns, heads):
    width = states.shape[-1]
    key_raw = jnp.einsum(
        "rd,dhe->hre",
        states,
        key_columns.reshape(width, heads, HD),
        preferred_element_type=jnp.float32,
    )
    keys = normalize_heads(key_raw).astype(jnp.bfloat16)
    values = jnp.einsum(
        "rd,dhe->hre",
        states,
        value_columns.reshape(width, heads, HD),
        preferred_element_type=jnp.float32,
    ).astype(jnp.bfloat16)
    return (keys, values)


def shifted(values, axis, step):
    size = lax.axis_size(axis)
    return lax.ppermute(values, axis, [(i, (i + step) % size) for i in range(size)])


def swapped(values):
    return lax.ppermute(values, "enc", [(i, i ^ 1) for i in range(lax.axis_size("enc"))])


def share_text(text_rows):
    enc_count = lax.axis_size("enc")
    _, depth = text_rows.shape
    side = lax.axis_index("enc") % 2
    block = depth // enc_count
    even = jnp.stack([text_rows[:, i * block : (i + 1) * block] for i in range(0, enc_count, 2)])
    odd = jnp.stack([text_rows[:, i * block : (i + 1) * block] for i in range(1, enc_count, 2)])
    own = jnp.where(side == 0, even, odd)
    away = jnp.where(side == 0, odd, even)
    arrived = swapped(away)
    pair = jnp.concatenate([arrived, own], axis=1)
    return jnp.concatenate(
        [pair] + [shifted(pair, "grp", step) for step in range(1, lax.axis_size("grp"))], axis=1
    )


def project_queries(text_blocks, weight, before):
    grp_count = lax.axis_size("grp")
    ring = lax.axis_size("enc") // 2
    enc_count = lax.axis_size("enc")
    place = lax.axis_index("enc") // 2
    total = None
    for step in range(ring):
        if step == max(0, ring - 2):
            weight, _ = lax.optimization_barrier((weight, before))
        left = lax.dynamic_index_in_dim(text_blocks, (place - step) % ring, 0, keepdims=False)
        term = jnp.dot(left, weight, preferred_element_type=jnp.float32)
        total = term if total is None else total + term
        if step < ring - 1:
            weight = lax.ppermute(
                weight, "enc", [(i, (i + 2) % enc_count) for i in range(enc_count)]
            )
    columns = total.shape[1]
    total = total.reshape(grp_count, 2, -1, columns)
    arrived = swapped(total[:, 0].astype(jnp.bfloat16))
    raw = total[:, 1] + arrived.astype(jnp.float32)
    own = normalize_heads(raw.reshape(grp_count, -1, columns // HD, HD)).astype(jnp.bfloat16)
    blocks = jnp.stack(
        [own[0]] + [shifted(own[step], "grp", -step) for step in range(1, grp_count)], axis=1
    )
    start = (grp_count - lax.axis_index("grp")) % grp_count
    blocks = lax.dynamic_slice_in_dim(
        jnp.concatenate([blocks, blocks], axis=1), start, grp_count, 1
    )
    return blocks.reshape(blocks.shape[0], grp_count * columns)


def share_keys(states, key_weight, value_weight, first_head, kv_local):
    dec_count = lax.axis_size("dec")
    rows, _ = states.shape
    if dec_count == 2 and kv_local * dec_count == KV_HEADS:
        keys, values = project_heads(states, key_weight, value_weight, KV_HEADS)
        paired = jnp.stack([keys, values])
        own = lax.dynamic_slice_in_dim(paired, first_head, kv_local, 1)
        away = lax.dynamic_slice_in_dim(paired, KV_HEADS - kv_local - first_head, kv_local, 1)
        arrived = shifted(away, "dec", 1)
        first = lax.axis_index("dec") == 0
        paired = jnp.stack(
            [jnp.where(first, own, arrived), jnp.where(first, arrived, own)], axis=1
        )
        return (paired[0], paired[1])
    key_columns = lax.dynamic_slice_in_dim(key_weight, first_head * HD, kv_local * HD, 1)
    value_columns = lax.dynamic_slice_in_dim(value_weight, first_head * HD, kv_local * HD, 1)
    piece = lax.all_gather(states, "dec", axis=0, tiled=True)
    key_part, value_part = project_heads(piece, key_columns, value_columns, kv_local)
    shape = (kv_local, dec_count, rows, HD)
    return (
        key_part.reshape(shape).transpose(1, 0, 2, 3),
        value_part.reshape(shape).transpose(1, 0, 2, 3),
    )


def share_grads(terms):
    dec_count = lax.axis_size("dec")
    grp_count = lax.axis_size("grp")
    rows = terms.shape[1] // (dec_count * grp_count)
    if dec_count == 2 and grp_count == 2:
        parts = terms.reshape(2, dec_count, grp_count, rows, -1)
        grp_place = lax.axis_index("grp")
        dec_place = lax.axis_index("dec")
        kept = lax.dynamic_index_in_dim(parts, grp_place, 2, keepdims=False)
        away = lax.dynamic_index_in_dim(parts, 1 - grp_place, 2, keepdims=False)
        kept = kept + shifted(away.astype(jnp.bfloat16), "grp", 1).astype(jnp.float32)
        away = lax.dynamic_index_in_dim(kept, 1 - dec_place, 1, keepdims=False)
        kept = lax.dynamic_index_in_dim(kept, dec_place, 1, keepdims=False)
        kept = kept + shifted(away.astype(jnp.bfloat16), "dec", 1).astype(jnp.float32)
        return (kept[0], kept[1])
    summed = lax.psum_scatter(
        terms.astype(jnp.bfloat16), ("dec", "grp"), scatter_dimension=1, tiled=True
    ).astype(jnp.float32)
    return (summed[0], summed[1])


MESH = pl.DeviceIdType.MESH


def pick(table, place):
    return sum(jnp.where(place == i, value, 0) for i, value in enumerate(table))


def step_kernel(
    line,
    patch,
    tiles_in,
    links_in,
    lengths_in,
    images_ref,
    state_grads_ref,
    gain_in,
    shift_in,
    bias_in,
    up_ref,
    down_ref,
    down_bias_in,
    key_ref,
    value_ref,
    text_ref,
    weight_ref,
    context_ref,
    up_grad_ref,
    down_grad_ref,
    tiles_ref,
    links_ref,
    lengths_ref,
    gain_ref,
    shift_ref,
    bias_ref,
    down_bias_ref,
    own,
    kw,
    kv_send,
    kv,
    queries,
    acc,
    tb,
    wb,
    fb,
    bb,
    bias_col,
    rows,
    pre,
    hid_t,
    hid,
    pg_t,
    po,
    psend,
    precv,
    msend,
    mrecv,
    gs1,
    gr1,
    gs2,
    gr2,
    gs3,
    gr3,
    local_sem,
    t_send,
    t_recv,
    y_send,
    y_recv,
    x_send,
    x_recv,
    s_send,
    s_recv,
    a_send,
    a_recv,
    p_send,
    p_recv,
    m_send,
    m_recv,
    g_send,
    g_recv,
    k_send,
    k_recv,
):
    f32 = jnp.float32
    bf16 = jnp.bfloat16
    enc = lax.axis_index("enc")
    y = lax.axis_index("dec")
    g = lax.axis_index("grp")
    z, x = enc // 2, enc % 2
    other_x = ((z * 2 + 1 - x), y, g)
    other_y = (enc, 1 - y, g)
    other_g = (enc, y, 1 - g)

    def along(place):
        return (place * 2 + x, y, g)

    orders = []
    for p in range(line):
        others = [a for a in range(line) if a != p]
        others.sort(key=lambda a: (-abs(a - p), min(a, line - 1 - a)))
        orders.append(others)
    order = [pick([orders[p][i] for p in range(line)], z) for i in range(line - 1)]
    text_rows, depth = tb.shape[2], tb.shape[3]
    half_cols = wb.shape[3]
    img = rows.shape[2]
    width = rows.shape[3]
    units = fb.shape[2]
    piece = units // 2
    part = units // 4

    barrier = pltpu.get_barrier_semaphore()
    for k in range(line):

        @pl.when(z != k)
        def _():
            pl.semaphore_signal(barrier, inc=1, device_id=along(k), device_id_type=MESH)

    for to in (other_x, other_y, other_g):
        pl.semaphore_signal(barrier, inc=1, device_id=to, device_id_type=MESH)
    pl.semaphore_wait(barrier, line + 2)

    def remote(src, dst, send, recv, to):
        return pltpu.make_async_remote_copy(
            src_ref=src, dst_ref=dst, send_sem=send, recv_sem=recv, device_id=to, device_id_type=MESH
        )

    def text_copy(i):
        b = order[i]
        at = pl.multiple_of((b * 2 + y) * depth, depth)
        return remote(
            text_ref.at[:, pl.ds(at, depth)], tb.at[z, y], t_send.at[i], t_recv.at[z], along(b)
        )

    def text_landed(a):
        return remote(tb.at[a, y], tb.at[a, y], t_send.at[0], t_recv.at[a], other_y)

    def text_relay(a):
        return remote(tb.at[a, y], tb.at[a, y], y_send.at[a], y_recv.at[a], other_y)

    def text_relayed(a):
        return remote(tb.at[a, 1 - y], tb.at[a, 1 - y], y_send.at[a], y_recv.at[a], other_y)

    quarter = half_cols // 2

    def weight_source(c, core):
        at = pl.multiple_of(core * half_cols + c * quarter, quarter)
        return weight_ref.at[:, pl.ds(at, quarter)]

    def weight_spot(k, c, core):
        return wb.at[k, c, :, pl.ds(pl.multiple_of(core * quarter, quarter), quarter)]

    def weight_x(c):
        return remote(
            weight_source(c, g), weight_spot(x, c, g), x_send.at[4 + c], x_recv.at[4 + c], other_x
        )

    def weight_copy(c, core, send, recv, to):
        spot = weight_spot(1 - x, c, core)
        return remote(spot, spot, send, recv, to)

    def weight_x_in(c):
        return weight_copy(c, g, x_send.at[4 + c], x_recv.at[4 + c], other_x)

    def weight_s(c):
        return weight_copy(c, g, s_send.at[5 + c], s_recv.at[5 + c], other_g)

    def weight_s_in(c):
        return weight_copy(c, 1 - g, s_send.at[5 + c], s_recv.at[5 + c], other_g)

    def unit_rows(core, q):
        return pl.ds(pl.multiple_of(core * piece + q * part, part), part)

    def unit_x(ref, kind, q):
        return remote(
            ref.at[unit_rows(g, q)],
            fb.at[kind, x, unit_rows(g, q)],
            x_send.at[1 + q],
            x_recv.at[1 + q],
            other_x,
        )

    def unit_copy(kind, core, q, send, recv, to):
        spot = fb.at[kind, 1 - x, unit_rows(core, q)]
        return remote(spot, spot, send, recv, to)

    def unit_x_in(q):
        return unit_copy(y, g, q, x_send.at[1 + q], x_recv.at[1 + q], other_x)

    def unit_s(q):
        return unit_copy(y, g, q, s_send.at[1 + q], s_recv.at[1 + q], other_g)

    def unit_s_in(q):
        return unit_copy(y, 1 - g, q, s_send.at[1 + q], s_recv.at[1 + q], other_g)

    def unit_y(q):
        return unit_copy(y, g, q, y_send.at[line + q], y_recv.at[line + q], other_y)

    def unit_y_in(q):
        return unit_copy(1 - y, g, q, y_send.at[line + q], y_recv.at[line + q], other_y)

    def unit_s2(q):
        return unit_copy(1 - y, g, q, s_send.at[3 + q], s_recv.at[3 + q], other_g)

    def unit_s2_in(q):
        return unit_copy(1 - y, 1 - g, q, s_send.at[3 + q], s_recv.at[3 + q], other_g)

    bias_x = remote(bb.at[x], bb.at[x], x_send.at[3], x_recv.at[3], other_x)
    bias_x_in = remote(bb.at[1 - x], bb.at[1 - x], x_send.at[3], x_recv.at[3], other_x)

    def rows_copy(m, a, right):
        to = along(z + 1) if right else along(z - 1)
        spot = rows.at[m, a]
        return remote(spot, spot, a_send.at[1 if right else 0, m, a], a_recv.at[m, a], to)

    def rows_landed(m, a):
        return remote(rows.at[m, a], rows.at[m, a], a_send.at[0, m, a], a_recv.at[m, a], other_y)

    locals_ = [
        pltpu.make_async_copy(weight_source(c, k), weight_spot(x, c, k), local_sem.at[11 + c * 2 + k])
        for c in range(2)
        for k in range(2)
    ] + [
        pltpu.make_async_copy(up_ref, fb.at[0, x], local_sem.at[2]),
        pltpu.make_async_copy(down_ref, fb.at[1, x], local_sem.at[3]),
        pltpu.make_async_copy(key_ref, kw.at[0], local_sem.at[5]),
        pltpu.make_async_copy(value_ref, kw.at[1], local_sem.at[8]),
    ] + [
        pltpu.make_async_copy(
            text_ref.at[:, pl.ds(pl.multiple_of((z * 2 + h) * depth, depth), depth)],
            tb.at[z, h],
            local_sem.at[6 + h],
        )
        for h in range(2)
    ]

    for i in range(line - 1):
        text_copy(i).start()
    for c in range(2):
        weight_x(c).start()
    small = (
        (tiles_in, tiles_ref),
        (links_in, links_ref),
        (lengths_in, lengths_ref),
        (gain_in, gain_ref),
        (shift_in, shift_ref),
        (bias_in, bias_ref),
        (down_bias_in, down_bias_ref),
    )
    own_copies = [
        pltpu.make_async_copy(src, dst, local_sem.at[15 + i]) for i, (src, dst) in enumerate(small)
    ] + [
        pltpu.make_async_copy(images_ref, own.at[0], local_sem.at[9]),
        pltpu.make_async_copy(state_grads_ref, own.at[1], local_sem.at[10]),
    ]
    for copy in own_copies + locals_:
        copy.start()
    for copy in own_copies:
        copy.wait()
    bb[x] = bias_ref[...][None]

    def live_rows(j):
        return tiles_ref[j, g, enc] * patch

    own_live = live_rows(y)

    def norm_body(t, _):
        r = pl.ds(pl.multiple_of(t * 16, 16), 16)
        normed = normalize_layer(own[0, r].astype(f32), gain_ref[...][None], shift_ref[...][None])
        rows[0, z, r] = normed.astype(bf16)
        row = t * 16 + lax.broadcasted_iota(jnp.int32, (16, width), 0)
        rows[1, z, r] = jnp.where(row < own_live, own[1, r].astype(f32), 0.0).astype(bf16)
        return 0

    lax.fori_loop(0, img // 16, norm_body, 0)

    for m in range(2):

        @pl.when(z < line - 1)
        def _(m=m):
            rows_copy(m, z, True).start()

        @pl.when(z > 0)
        def _(m=m):
            rows_copy(m, z, False).start()

    def forward_rows(m, s):
        @pl.when(z - s >= 0)
        def _():
            rows_landed(m, z - s).wait_recv()

            @pl.when(z < line - 1)
            def _():
                rows_copy(m, z - s, True).start()

        @pl.when(z + s <= line - 1)
        def _():
            rows_landed(m, z + s).wait_recv()

            @pl.when(z > 0)
            def _():
                rows_copy(m, z + s, False).start()

    def has_incoming(a):
        return jnp.logical_or(
            jnp.logical_and(a > z, z > 0), jnp.logical_and(a < z, z < line - 1)
        )

    def next_slot(a):
        right = a > z
        to = jnp.where(right, z + 1, z - 1)
        slot = jnp.where(jnp.logical_and(to == a, jnp.logical_not(right)), line, a)
        return to, slot

    def sum_copy(a, c):
        to, slot = next_slot(a)
        return remote(psend.at[a, c], precv.at[slot, c], p_send.at[a, c], p_recv.at[slot, c], along(to))

    def sum_landed(slot, c):
        return remote(precv.at[slot, c], precv.at[slot, c], p_send.at[0, c], p_recv.at[slot, c], other_y)

    tile = 256

    def multiply(a, c, store):
        def body(t, _):
            cols = pl.ds(pl.multiple_of(t * tile, tile), tile)
            total = jnp.dot(tb[a, 0], wb[0, c, :, cols], preferred_element_type=f32)
            total = total + jnp.dot(tb[a, 1], wb[1, c, :, cols], preferred_element_type=f32)
            store(t, cols, total)
            return 0

        lax.fori_loop(0, half_cols // tile, body, 0)

    def product(i, c):
        a = order[i]

        def store(t, cols, total):
            psend[a, c, :, cols] = total.astype(bf16)

        multiply(a, c, store)

    def send_product(i, c):
        a = order[i]

        @pl.when(jnp.logical_not(has_incoming(a)))
        def _():
            sum_copy(a, c).start()

    def add_incoming(i, c):
        a = order[i]

        @pl.when(has_incoming(a))
        def _():
            sum_landed(a, c).wait_recv()

            def body(t, _):
                r = pl.ds(pl.multiple_of(t * 16, 16), 16)
                psend[a, c, r] = (psend[a, c, r].astype(f32) + precv[a, c, r].astype(f32)).astype(bf16)
                return 0

            lax.fori_loop(0, text_rows // 16, body, 0)
            sum_copy(a, c).start()

    held = ((line - 2, 0), (line - 2, 1))

    def products(i):
        text_relayed(order[i]).wait_recv()
        for c in range(2):
            product(i, c)
            if (i, c) not in held:
                send_product(i, c)

    def relay_units(q):
        unit_x_in(q).wait_recv()
        unit_s(q).start()
        unit_y(q).start()

    def relay_text(i):
        text_landed(order[i]).wait_recv()
        text_relay(order[i]).start()

    relay_text(0)
    weight_x_in(0).wait_recv()
    weight_s(0).start()
    for copy in locals_:
        copy.wait()
    text_relayed(order[0]).wait_recv()
    weight_s_in(0).wait_recv()
    product(0, 0)
    send_product(0, 0)
    for i in range(1, line - 1):
        relay_text(i)
    weight_x_in(1).wait_recv()
    weight_s(1).start()
    for c in range(2):
        weight_x(c).wait_send()

    @pl.when(y == 0)
    def _():
        for q in range(2):
            unit_x(up_ref, 0, q).start()

    @pl.when(y == 1)
    def _():
        for q in range(2):
            unit_x(down_ref, 1, q).start()

    bias_x.start()

    weight_s_in(1).wait_recv()
    product(0, 1)
    send_product(0, 1)
    forward_rows(0, 1)
    relay_units(0)
    products(1)
    add_incoming(0, 0)
    for m in range(2):
        forward_rows(m, 2 - m)
    relay_units(1)
    for i in range(2, line - 1):
        products(i)
    unit_y_in(0).wait_recv()
    unit_s2(0).start()
    add_incoming(0, 1)
    forward_rows(0, 3)
    unit_y_in(1).wait_recv()
    unit_s2(1).start()
    bias_x_in.wait_recv()
    for q in range(2):
        unit_s_in(q).wait_recv()
        unit_s2_in(q).wait_recv()

    all_rows = line * img

    def up_body(q, _):
        k = q // 2
        at = pl.multiple_of((q % 2) * piece, piece)
        pre[k, pl.ds(at, piece)] = lax.dot_general(
            fb[0, k, pl.ds(at, piece)],
            rows[0].reshape(all_rows, width),
            (((1,), (1,)), ((), ())),
            preferred_element_type=f32,
        )
        return 0

    lax.fori_loop(0, 4, up_body, 0)
    forward_rows(1, 2)
    for k in range(2):
        for t in range(units // 128):
            spot = slice(t * 128, (t + 1) * 128)
            bias_col[k, spot] = jnp.transpose(jnp.broadcast_to(bb[k, :, spot], (8, 128)))

    def gelu_body(r, _):
        k = r // (units // 16)
        at = pl.ds(pl.multiple_of((r % (units // 16)) * 16, 16), 16)
        value = pre[k, at] + bias_col[k, at, 0:1]
        phi = 0.5 * (1.0 + lax.erf(value * 0.7071067811865476))
        hid_t[k, at] = (value * phi).astype(bf16)
        pre[k, at] = phi + value * jnp.exp(-0.5 * value * value) * 0.3989422804014327
        return 0

    lax.fori_loop(0, 2 * units // 16, gelu_body, 0, unroll=4)

    def terms(kind, k, j, owner):
        at = pl.ds(pl.multiple_of(j * piece + owner * part, part), part)
        left = pg_t if kind == 0 else hid_t
        return jnp.dot(left[k, at], rows[kind].reshape(all_rows, width), preferred_element_type=f32)

    grads_s = [remote(gs1.at[m], gr1.at[m], g_send.at[m], g_recv.at[m], other_g) for m in range(2)]
    grads_y = remote(gs2.at[0], gr2.at[0], g_send.at[2], g_recv.at[2], other_y)
    grads_x = remote(gs2.at[1], gr2.at[1], g_send.at[3], g_recv.at[3], other_x)
    grads_x2 = remote(gs3.at[0], gr3.at[0], g_send.at[4], g_recv.at[4], other_x)
    grads_y2 = remote(gs3.at[1], gr3.at[1], g_send.at[5], g_recv.at[5], other_y)

    def share_core(kind):
        def body(q, _):
            k, j = q // 2, q % 2
            gs1[kind, k, j] = terms(kind, k, j, 1 - g).astype(bf16)
            return 0

        lax.fori_loop(0, 4, body, 0)
        grads_s[kind].start()

    def flip_body(t, _):
        for k in range(2):
            at = pl.ds(pl.multiple_of(t * 128, 128), 128)
            hid[k, :, at] = jnp.transpose(hid_t[k, at].astype(f32)).astype(bf16)
        return 0

    lax.fori_loop(0, units // 128, flip_body, 0)

    def down_body(t, _):
        cols = pl.ds(pl.multiple_of(t * tile, tile), tile)
        total = jnp.dot(hid[0], fb[1, 0, :, cols], preferred_element_type=f32)
        po[:, cols] = total + jnp.dot(hid[1], fb[1, 1, :, cols], preferred_element_type=f32)
        return 0

    lax.fori_loop(0, width // tile, down_body, 0)

    def state_copy(a):
        to, slot = next_slot(a)
        return remote(msend.at[a], mrecv.at[slot], m_send.at[a], m_recv.at[slot], along(to))

    def state_landed(slot):
        return remote(mrecv.at[slot], mrecv.at[slot], m_send.at[0], m_recv.at[slot], other_y)

    def send_state(i, first):
        a = order[i]
        waits = has_incoming(a)

        @pl.when(jnp.logical_not(waits) if first else waits)
        def _():
            if not first:
                state_landed(a).wait_recv()

            def body(t, _):
                r = pl.ds(pl.multiple_of(t * 16, 16), 16)
                value = po[pl.ds(pl.multiple_of(a * img + t * 16, 16), 16)]
                if not first:
                    value = value + mrecv[a, r].astype(f32)
                msend[a, r] = value.astype(bf16)
                return 0

            lax.fori_loop(0, img // 16, body, 0)
            state_copy(a).start()

    for i in range(line - 1):
        send_state(i, True)
    for c in range(2):
        send_product(line - 2, c)
    add_incoming(1, 0)
    add_incoming(2, 0)
    forward_rows(1, 3)
    share_core(1)

    def slope_body(q, _):
        k = q // 2
        at = pl.ds(pl.multiple_of((q % 2) * piece, piece), piece)
        grad = lax.dot_general(
            fb[1, k, at],
            rows[1].reshape(all_rows, width),
            (((1,), (1,)), ((), ())),
            preferred_element_type=f32,
        )
        pg_t[k, at] = (grad * pre[k, at]).astype(bf16)
        return 0

    lax.fori_loop(0, 4, slope_body, 0)
    share_core(0)

    grads_s[1].wait_recv()

    def away_x(j, _):
        gs2[1, j] = (terms(1, 1 - x, j, g) + gr1[1, 1 - x, j].astype(f32)).astype(bf16)
        return 0

    lax.fori_loop(0, 2, away_x, 0)
    grads_x.start()
    grads_s[0].wait_recv()

    def away_y(k, _):
        gs2[0, k] = (terms(0, k, 1 - y, g) + gr1[0, k, 1 - y].astype(f32)).astype(bf16)
        return 0

    lax.fori_loop(0, 2, away_y, 0)
    grads_y.start()
    add_incoming(1, 1)
    send_state(0, False)
    send_state(2, False)
    add_incoming(2, 1)
    send_state(1, False)
    grads_x.wait_recv()
    total = terms(1, x, 1 - y, g) + gr1[1, x, 1 - y].astype(f32)
    gs3[1] = (total + gr2[1, 1 - y].astype(f32)).astype(bf16)
    grads_y2.start()
    grads_y.wait_recv()
    total = terms(0, 1 - x, y, g) + gr1[0, 1 - x, y].astype(f32)
    gs3[0] = (total + gr2[0, 1 - x].astype(f32)).astype(bf16)
    grads_x2.start()

    def own_products(c):
        def store(t, cols, total):
            acc[c, :, cols] = total

        multiply(z, c, store)

    def own_texts(c):
        @pl.when(z > 0)
        def _():
            sum_landed(z, c).wait_recv()

        @pl.when(z < line - 1)
        def _():
            sum_landed(line, c).wait_recv()

        def body(t, _):
            r = pl.ds(pl.multiple_of(t * 32, 32), 32)
            for h in range(half_cols // HD):
                spot = slice(h * HD, (h + 1) * HD)
                head = acc[c, r, spot]
                head = head + jnp.where(z > 0, precv[z, c, r, spot].astype(f32), 0.0)
                head = head + jnp.where(z < line - 1, precv[line, c, r, spot].astype(f32), 0.0)
                queries[r, spot] = normalize_heads(head).astype(bf16)
            return 0

        lax.fori_loop(0, text_rows // 32, body, 0)

    for c in range(2):
        own_products(c)

    slot_rows = pl.ds(pl.multiple_of(z * img, img), img)
    po[slot_rows] = po[slot_rows] + own[0].astype(f32) + down_bias_ref[...][None]

    @pl.when(z > 0)
    def _():
        state_landed(z).wait_recv()
        po[slot_rows] = po[slot_rows] + mrecv[z].astype(f32)

    @pl.when(z < line - 1)
    def _():
        state_landed(line).wait_recv()
        po[slot_rows] = po[slot_rows] + mrecv[line].astype(f32)

    states = po[slot_rows].astype(bf16)
    local = kv.shape[2]
    own_rows = pl.ds(pl.multiple_of(y * img, img), img)
    away_rows = pl.ds(pl.multiple_of((1 - y) * img, img), img)
    kv_copy = remote(kv_send, kv.at[:, own_rows], k_send, k_recv, other_y)
    kv_in = remote(kv.at[:, away_rows], kv.at[:, away_rows], k_send, k_recv, other_y)
    for sent in (True, False):
        at = pl.multiple_of(((1 - y) if sent else y) * local, local)
        spot = kv_send if sent else kv.at[:, own_rows]
        raw = jnp.dot(states, kw[0, :, pl.ds(at, local)], preferred_element_type=f32)
        for h in range(local // HD):
            head = normalize_heads(raw[:, h * HD : (h + 1) * HD])
            spot[0, :, h * HD : (h + 1) * HD] = head.astype(bf16)
        raw = jnp.dot(states, kw[1, :, pl.ds(at, local)], preferred_element_type=f32)
        spot[1] = raw.astype(bf16)
        if sent:
            kv_copy.start()

    samples, length = context_ref.shape[:2]
    group = half_cols // HD

    def attend_texts(c):
        key = lax.broadcasted_iota(jnp.int32, (length, 2 * img), 1)

        def body(n, _):
            r = pl.ds(pl.multiple_of(n * length, length), length)
            limits = [jnp.where(links_ref[n, j] > 0, live_rows(j), 0) for j in range(2)]
            allowed = key < jnp.where(key < img, limits[0], limits[1] + img)
            valid = lax.broadcasted_iota(jnp.int32, (length, HD), 0) < lengths_ref[n]
            for h in range(group):
                shared = h // (group // 2)
                head_cols = slice(shared * HD, (shared + 1) * HD)
                first = shared * half_cols + c * quarter + (h % (group // 2)) * HD
                cols = slice(first, first + HD)
                score = lax.dot_general(
                    queries[r, h * HD : (h + 1) * HD],
                    kv[0, :, head_cols],
                    (((1,), (1,)), ((), ())),
                    preferred_element_type=f32,
                )
                weights = jnp.where(allowed, jnp.exp(score * HD ** (-0.5)), 0.0)
                scale = 1.0 / jnp.sum(weights, axis=-1, keepdims=True)
                mixed = jnp.dot(
                    (weights * scale).astype(bf16), kv[1, :, head_cols], preferred_element_type=f32
                )
                context_ref[n, :, cols] = jnp.where(valid, mixed, 0.0).astype(bf16)
            return 0

        lax.fori_loop(0, samples, body, 0)

    own_texts(0)
    for kind, out in ((1, down_grad_ref), (0, up_grad_ref)):
        (grads_x2, grads_y2)[kind].wait_recv()
        total = terms(kind, x, y, g) + gr1[kind, x, y].astype(f32)
        total = total + gr2[kind, (x, y)[kind]].astype(f32)
        out[...] = total + gr3[kind].astype(f32)

    kv_in.wait_recv()
    attend_texts(0)
    own_texts(1)
    attend_texts(1)
    for i in range(line - 1):
        a = order[i]
        text_copy(i).wait_send()
        text_relay(a).wait_send()
        state_copy(a).wait_send()
        for c in range(2):
            sum_copy(a, c).wait_send()
    for copy in (kv_copy, weight_s(0), weight_s(1), bias_x, *grads_s, grads_y, grads_x, grads_x2, grads_y2):
        copy.wait_send()
    for q in range(2):
        for copy in (unit_x(up_ref, 0, q), unit_s(q), unit_y(q), unit_s2(q)):
            copy.wait_send()

    for a in range(line):

        @pl.when(jnp.logical_and(a <= z, z < line - 1))
        def _():
            for m in range(2):
                rows_copy(m, a, True).wait_send()

        @pl.when(jnp.logical_and(a >= z, z > 0))
        def _():
            for m in range(2):
                rows_copy(m, a, False).wait_send()


def store_kernel(*refs):
    count = len(refs) // 2
    copies = [
        pltpu.make_async_copy(refs[i], refs[count + i], refs[-1].at[i]) for i in range(count)
    ]
    for copy in copies:
        copy.start()
    for copy in copies:
        copy.wait()


def store_outputs(*values):
    anywhere = pl.BlockSpec(memory_space=pl.ANY)
    return pl.pallas_call(
        store_kernel,
        out_shape=[jax.ShapeDtypeStruct(value.shape, value.dtype) for value in values],
        in_specs=[anywhere] * len(values),
        out_specs=[anywhere] * len(values),
        scratch_shapes=[pltpu.SemaphoreType.DMA((len(values),))],
        compiler_params=pltpu.CompilerParams(vmem_limit_bytes=1 << 20),
        name="store_outputs",
    )(*values)


def exchange(
    tiles, links, lengths, images, state_grads, gain, shift, bias, up, down, down_bias, key, value, text, weight, patch
):
    line = lax.axis_size("enc") // 2
    text_rows = text.shape[0] * text.shape[1]
    depth, columns = weight.shape
    img, width = images.shape
    units = up.shape[0]
    half = columns // 2
    local = key.shape[1] // 2
    f32, bf16 = jnp.float32, jnp.bfloat16
    dma = pltpu.SemaphoreType.DMA
    part = units // 4
    vmem = pl.BlockSpec(memory_space=pltpu.VMEM)
    anywhere = pl.BlockSpec(memory_space=pl.ANY)
    return pl.pallas_call(
        functools.partial(step_kernel, line, patch),
        out_shape=[
            pltpu.VMEM((*text.shape[:2], columns), bf16),
            pltpu.VMEM((part, width), f32),
            pltpu.VMEM((part, width), f32),
        ],
        in_specs=[anywhere] * 15,
        out_specs=[vmem] * 3,
        scratch_shapes=[
            pltpu.SMEM(tiles.shape, jnp.int32),
            pltpu.SMEM(links.shape, jnp.int32),
            pltpu.SMEM(lengths.shape, jnp.int32),
            pltpu.VMEM(gain.shape, f32),
            pltpu.VMEM(shift.shape, f32),
            pltpu.VMEM(bias.shape, f32),
            pltpu.VMEM(down_bias.shape, f32),
            pltpu.VMEM((2, img, width), bf16),
            pltpu.VMEM((2, width, 2 * local), bf16),
            pltpu.VMEM((2, img, local), bf16),
            pltpu.VMEM((2, 2 * img, local), bf16),
            pltpu.VMEM((text_rows, half), bf16),
            pltpu.VMEM((2, text_rows, half), f32),
            pltpu.VMEM((line, 2, text_rows, depth), bf16),
            pltpu.VMEM((2, 2, depth, half), bf16),
            pltpu.VMEM((2, 2, units, width), bf16),
            pltpu.VMEM((2, 1, units), f32),
            pltpu.VMEM((2, units, 8), f32),
            pltpu.VMEM((2, line, img, width), bf16),
            pltpu.VMEM((2, units, line * img), f32),
            pltpu.VMEM((2, units, line * img), bf16),
            pltpu.VMEM((2, line * img, units), bf16),
            pltpu.VMEM((2, units, line * img), bf16),
            pltpu.VMEM((line * img, width), f32),
            pltpu.VMEM((line, 2, text_rows, half), bf16),
            pltpu.VMEM((line + 1, 2, text_rows, half), bf16),
            pltpu.VMEM((line, img, width), bf16),
            pltpu.VMEM((line + 1, img, width), bf16),
            pltpu.VMEM((2, 2, 2, part, width), bf16),
            pltpu.VMEM((2, 2, 2, part, width), bf16),
            pltpu.VMEM((2, 2, part, width), bf16),
            pltpu.VMEM((2, 2, part, width), bf16),
            pltpu.VMEM((2, part, width), bf16),
            pltpu.VMEM((2, part, width), bf16),
            dma((22,)),
            dma((line - 1,)),
            dma((line,)),
            dma((line + 2,)),
            dma((line + 2,)),
            dma((6,)),
            dma((6,)),
            dma((7,)),
            dma((7,)),
            dma((2, 2, line)),
            dma((2, line)),
            dma((line, 2)),
            dma((line + 1, 2)),
            dma((line,)),
            dma((line + 1,)),
            dma((6,)),
            dma((6,)),
            dma,
            dma,
        ],
        compiler_params=pltpu.CompilerParams(
            collective_id=0, has_side_effects=True, vmem_limit_bytes=64_200_000
        ),
        name="exchange",
    )(tiles, links, lengths, images, state_grads, gain, shift, bias, up, down, down_bias, key, value, text.reshape(text_rows, -1), weight)


def on_column(
    images,
    ln_gain,
    ln_bias,
    fc1_weight,
    fc1_bias,
    fc2_weight,
    fc2_bias,
    key_weight,
    value_weight,
    text,
    query_weight,
    tiles,
    links,
    lengths,
    state_grads,
):
    slots, patch, width = images.shape[1:]
    context, fc1_grad, fc2_grad = exchange(
        tiles.transpose(1, 2, 0),
        links,
        lengths,
        images.reshape(slots * patch, width),
        state_grads.reshape(slots * patch, width),
        ln_gain,
        ln_bias,
        fc1_bias,
        fc1_weight,
        fc2_weight,
        fc2_bias,
        key_weight,
        value_weight,
        text,
        query_weight,
        patch,
    )
    return tuple(store_outputs(context, fc1_grad, fc2_grad))


def on_device(
    images,
    ln_gain,
    ln_bias,
    fc1_weight,
    fc1_bias,
    fc2_weight,
    fc2_bias,
    key_weight,
    value_weight,
    text,
    query_weight,
    tiles,
    links,
    lengths,
    state_grads,
):
    dec_count = lax.axis_size("dec")
    grp_count = lax.axis_size("grp")
    enc_place = lax.axis_index("enc")
    dec_place = lax.axis_index("dec")
    grp_place = lax.axis_index("grp")
    slots = images.shape[1]
    patch = images.shape[2]
    width = images.shape[3]
    img_rows = slots * patch
    own_rows = images.reshape(img_rows, width)
    normed = normalize_layer(own_rows.astype(jnp.float32), ln_gain, ln_bias).astype(jnp.bfloat16)
    samples = text.shape[0]
    length = text.shape[1]
    text_rows = text.reshape(samples * length, text.shape[2])
    half = query_weight.shape[1] // grp_count
    own_half = lax.dynamic_slice_in_dim(query_weight, grp_place * half, half, 1)
    own_tiles = tiles[enc_place, dec_place, grp_place]
    tile_index = jnp.arange(slots)
    own_live = jnp.broadcast_to((tile_index < own_tiles)[:, None, None], (slots, patch, 1)).reshape(
        img_rows, 1
    )
    cotangent = jnp.where(
        own_live, state_grads.reshape(img_rows, width), jnp.zeros((), state_grads.dtype)
    )
    sent = jnp.stack([normed, cotangent])
    text_rows, own_half, _ = lax.optimization_barrier((text_rows, own_half, sent))
    both = lax.all_gather(sent, "enc", axis=1, tiled=True)
    gathered, all_cotangent = both[0], both[1]
    text_blocks = share_text(text_rows)
    pre, hidden, partial_full = encoder_rows(gathered, fc1_weight, fc1_bias, fc2_weight)
    partial_full = partial_full.astype(jnp.bfloat16)
    all_cotangent, _ = lax.optimization_barrier((all_cotangent, partial_full))
    first_term, second_term = weight_terms(gathered, pre, hidden, all_cotangent, fc2_weight)
    queries_of = project_queries(text_blocks, own_half, second_term)
    summed = lax.psum_scatter(
        partial_full, "enc", scatter_dimension=0, tiled=True
    ).astype(jnp.float32)
    states = (own_rows.astype(jnp.float32) + summed + fc2_bias).astype(jnp.bfloat16)
    local_heads = query_weight.shape[1] // HD
    per_group = HEADS // KV_HEADS
    kv_local = max(1, local_heads // per_group)
    first_head = dec_place * local_heads // per_group
    keys, values = share_keys(states, key_weight, value_weight, first_head, kv_local)
    heads_each = local_heads // kv_local
    queries = queries_of
    queries = queries.reshape(samples, length, kv_local, heads_each, HD)
    dec_tiles = tiles[enc_place, :, grp_place]
    live_keys = tile_index[None, :] < dec_tiles[:, None]
    live_keys = jnp.broadcast_to(live_keys[:, :, None], (dec_count, slots, patch)).reshape(
        dec_count, img_rows
    )
    allowed = (links[:, :, None] > 0) & live_keys[None, :, :]
    scores = jnp.einsum(
        "sqghd,jgkd->sghjkq", queries, keys, preferred_element_type=jnp.float32
    ) * HD ** (-0.5)
    weights = jnp.where(allowed[:, None, None, :, :, None], jnp.exp(scores), 0.0)
    totals = jnp.sum(weights, axis=(3, 4), keepdims=True)
    probs = (weights / totals).astype(jnp.bfloat16)
    mixed = jnp.einsum("sghjkq,jgkd->sqghd", probs, values, preferred_element_type=jnp.float32)
    valid = jnp.arange(length)[None, :] < lengths[:, None]
    context = (
        jnp.where(valid[:, :, None, None, None], mixed, 0.0)
        .reshape(samples, length, local_heads * HD)
        .astype(jnp.bfloat16)
    )
    fc1_grad, fc2_grad = share_grads(jnp.stack([first_term, second_term]))
    return (context, fc1_grad, fc2_grad)


def solution(mesh):
    in_specs = (
        P(("enc", "dec", "grp"), None, None, None),
        P(),
        P(),
        P("enc", None),
        P("enc"),
        P("enc", None),
        P(),
        P(),
        P(),
        P(("enc", "grp"), None, None),
        P("enc", "dec"),
        P(),
        P(("enc", "grp"), None),
        P(("enc", "grp")),
        P(("enc", "dec", "grp"), None, None, None),
    )
    out_specs = (
        P(("enc", "grp"), None, "dec"),
        P(("enc", "dec", "grp"), None),
        P(("enc", "dec", "grp"), None),
    )
    paired = mesh.shape["dec"] == 2 and mesh.shape["grp"] == 2 and mesh.shape["enc"] % 2 == 0
    if paired and mesh.shape["enc"] == 8:
        return jax.shard_map(
            on_column, mesh=mesh, in_specs=in_specs, out_specs=out_specs, check_vma=False
        )
    return jax.shard_map(
        on_device, mesh=mesh, in_specs=in_specs, out_specs=out_specs, check_vma=False
    )
```

```python
import functools

import jax
import jax.numpy as jnp
from jax import lax
from jax.experimental import pallas as pl
from jax.experimental.pallas import tpu as pltpu
from jax.sharding import PartitionSpec as P


HEADS = 32
KV_HEADS = 4
HD = 128


EPSILON = 1e-06


def normalize_layer(values, gain, shift):
    middle = jnp.mean(values, axis=-1, keepdims=True)
    centered = values - middle
    spread = jnp.mean(centered * centered, axis=-1, keepdims=True)
    return centered * lax.rsqrt(spread + EPSILON) * gain + shift


def normalize_heads(values):
    return values * lax.rsqrt(jnp.mean(values * values, axis=-1, keepdims=True) + EPSILON)


def gelu_slope(values):
    return (
        0.5 * (1.0 + lax.erf(values * 0.7071067811865476))
        + values * jnp.exp(-0.5 * values * values) * 0.3989422804014327
    )


def encoder_rows(rows, fc1_weight, fc1_bias, fc2_weight):
    pre = (
        lax.dot_general(
            rows, fc1_weight, (((1,), (1,)), ((), ())), preferred_element_type=jnp.float32
        )
        + fc1_bias
    )
    hidden = jax.nn.gelu(pre, approximate=False).astype(jnp.bfloat16)
    partial_sum = jnp.dot(hidden, fc2_weight, preferred_element_type=jnp.float32)
    return (pre, hidden, partial_sum)


def weight_terms(rows, pre, hidden, cotangent, fc2_weight):
    hidden_grad = lax.dot_general(
        cotangent, fc2_weight, (((1,), (1,)), ((), ())), preferred_element_type=jnp.float32
    )
    second_term = lax.dot_general(
        hidden, cotangent, (((0,), (0,)), ((), ())), preferred_element_type=jnp.float32
    )
    pre_grad = (hidden_grad * gelu_slope(pre)).astype(jnp.bfloat16)
    first_term = lax.dot_general(
        pre_grad, rows, (((0,), (0,)), ((), ())), preferred_element_type=jnp.float32
    )
    return (first_term, second_term)


def project_heads(states, key_columns, value_columns, heads):
    width = states.shape[-1]
    key_raw = jnp.einsum(
        "rd,dhe->hre",
        states,
        key_columns.reshape(width, heads, HD),
        preferred_element_type=jnp.float32,
    )
    keys = normalize_heads(key_raw).astype(jnp.bfloat16)
    values = jnp.einsum(
        "rd,dhe->hre",
        states,
        value_columns.reshape(width, heads, HD),
        preferred_element_type=jnp.float32,
    ).astype(jnp.bfloat16)
    return (keys, values)


def shifted(values, axis, step):
    size = lax.axis_size(axis)
    return lax.ppermute(values, axis, [(i, (i + step) % size) for i in range(size)])


def swapped(values):
    return lax.ppermute(values, "enc", [(i, i ^ 1) for i in range(lax.axis_size("enc"))])


def share_text(text_rows):
    enc_count = lax.axis_size("enc")
    _, depth = text_rows.shape
    side = lax.axis_index("enc") % 2
    block = depth // enc_count
    even = jnp.stack([text_rows[:, i * block : (i + 1) * block] for i in range(0, enc_count, 2)])
    odd = jnp.stack([text_rows[:, i * block : (i + 1) * block] for i in range(1, enc_count, 2)])
    own = jnp.where(side == 0, even, odd)
    away = jnp.where(side == 0, odd, even)
    arrived = swapped(away)
    pair = jnp.concatenate([arrived, own], axis=1)
    return jnp.concatenate(
        [pair] + [shifted(pair, "grp", step) for step in range(1, lax.axis_size("grp"))], axis=1
    )


def project_queries(text_blocks, weight, before):
    grp_count = lax.axis_size("grp")
    ring = lax.axis_size("enc") // 2
    enc_count = lax.axis_size("enc")
    place = lax.axis_index("enc") // 2
    total = None
    for step in range(ring):
        if step == max(0, ring - 2):
            weight, _ = lax.optimization_barrier((weight, before))
        left = lax.dynamic_index_in_dim(text_blocks, (place - step) % ring, 0, keepdims=False)
        term = jnp.dot(left, weight, preferred_element_type=jnp.float32)
        total = term if total is None else total + term
        if step < ring - 1:
            weight = lax.ppermute(
                weight, "enc", [(i, (i + 2) % enc_count) for i in range(enc_count)]
            )
    columns = total.shape[1]
    total = total.reshape(grp_count, 2, -1, columns)
    arrived = swapped(total[:, 0].astype(jnp.bfloat16))
    raw = total[:, 1] + arrived.astype(jnp.float32)
    own = normalize_heads(raw.reshape(grp_count, -1, columns // HD, HD)).astype(jnp.bfloat16)
    blocks = jnp.stack(
        [own[0]] + [shifted(own[step], "grp", -step) for step in range(1, grp_count)], axis=1
    )
    start = (grp_count - lax.axis_index("grp")) % grp_count
    blocks = lax.dynamic_slice_in_dim(
        jnp.concatenate([blocks, blocks], axis=1), start, grp_count, 1
    )
    return blocks.reshape(blocks.shape[0], grp_count * columns)


def share_keys(states, key_weight, value_weight, first_head, kv_local):
    dec_count = lax.axis_size("dec")
    rows, _ = states.shape
    if dec_count == 2 and kv_local * dec_count == KV_HEADS:
        keys, values = project_heads(states, key_weight, value_weight, KV_HEADS)
        paired = jnp.stack([keys, values])
        own = lax.dynamic_slice_in_dim(paired, first_head, kv_local, 1)
        away = lax.dynamic_slice_in_dim(paired, KV_HEADS - kv_local - first_head, kv_local, 1)
        arrived = shifted(away, "dec", 1)
        first = lax.axis_index("dec") == 0
        paired = jnp.stack(
            [jnp.where(first, own, arrived), jnp.where(first, arrived, own)], axis=1
        )
        return (paired[0], paired[1])
    key_columns = lax.dynamic_slice_in_dim(key_weight, first_head * HD, kv_local * HD, 1)
    value_columns = lax.dynamic_slice_in_dim(value_weight, first_head * HD, kv_local * HD, 1)
    piece = lax.all_gather(states, "dec", axis=0, tiled=True)
    key_part, value_part = project_heads(piece, key_columns, value_columns, kv_local)
    shape = (kv_local, dec_count, rows, HD)
    return (
        key_part.reshape(shape).transpose(1, 0, 2, 3),
        value_part.reshape(shape).transpose(1, 0, 2, 3),
    )


def share_grads(terms):
    dec_count = lax.axis_size("dec")
    grp_count = lax.axis_size("grp")
    rows = terms.shape[1] // (dec_count * grp_count)
    if dec_count == 2 and grp_count == 2:
        parts = terms.reshape(2, dec_count, grp_count, rows, -1)
        grp_place = lax.axis_index("grp")
        dec_place = lax.axis_index("dec")
        kept = lax.dynamic_index_in_dim(parts, grp_place, 2, keepdims=False)
        away = lax.dynamic_index_in_dim(parts, 1 - grp_place, 2, keepdims=False)
        kept = kept + shifted(away.astype(jnp.bfloat16), "grp", 1).astype(jnp.float32)
        away = lax.dynamic_index_in_dim(kept, 1 - dec_place, 1, keepdims=False)
        kept = lax.dynamic_index_in_dim(kept, dec_place, 1, keepdims=False)
        kept = kept + shifted(away.astype(jnp.bfloat16), "dec", 1).astype(jnp.float32)
        return (kept[0], kept[1])
    summed = lax.psum_scatter(
        terms.astype(jnp.bfloat16), ("dec", "grp"), scatter_dimension=1, tiled=True
    ).astype(jnp.float32)
    return (summed[0], summed[1])


MESH = pl.DeviceIdType.MESH


def pick(table, place):
    return sum(jnp.where(place == i, value, 0) for i, value in enumerate(table))


def step_kernel(
    line,
    patch,
    tiles_in,
    links_in,
    lengths_in,
    images_ref,
    state_grads_ref,
    gain_in,
    shift_in,
    bias_in,
    up_ref,
    down_ref,
    down_bias_in,
    key_ref,
    value_ref,
    text_ref,
    weight_ref,
    context_ref,
    up_grad_ref,
    down_grad_ref,
    tiles_ref,
    links_ref,
    lengths_ref,
    gain_ref,
    shift_ref,
    bias_ref,
    down_bias_ref,
    own,
    kw,
    kv_send,
    kv,
    queries,
    acc,
    tb,
    wb,
    fb,
    bb,
    bias_col,
    rows,
    pre,
    hid_t,
    hid,
    pg_t,
    po,
    psend,
    precv,
    msend,
    mrecv,
    gs1,
    gr1,
    gs2,
    gr2,
    gs3,
    gr3,
    local_sem,
    t_send,
    t_recv,
    y_send,
    y_recv,
    x_send,
    x_recv,
    s_send,
    s_recv,
    a_send,
    a_recv,
    p_send,
    p_recv,
    m_send,
    m_recv,
    g_send,
    g_recv,
    k_send,
    k_recv,
):
    f32 = jnp.float32
    bf16 = jnp.bfloat16
    enc = lax.axis_index("enc")
    y = lax.axis_index("dec")
    g = lax.axis_index("grp")
    z, x = enc // 2, enc % 2
    other_x = ((z * 2 + 1 - x), y, g)
    other_y = (enc, 1 - y, g)
    other_g = (enc, y, 1 - g)

    def along(place):
        return (place * 2 + x, y, g)

    orders = []
    for p in range(line):
        others = [a for a in range(line) if a != p]
        others.sort(key=lambda a: (-abs(a - p), min(a, line - 1 - a)))
        orders.append(others)
    order = [pick([orders[p][i] for p in range(line)], z) for i in range(line - 1)]
    text_rows, depth = tb.shape[2], tb.shape[3]
    half_cols = wb.shape[3]
    img = rows.shape[2]
    width = rows.shape[3]
    units = fb.shape[2]
    piece = units // 2
    part = units // 4

    barrier = pltpu.get_barrier_semaphore()
    for k in range(line):

        @pl.when(z != k)
        def _():
            pl.semaphore_signal(barrier, inc=1, device_id=along(k), device_id_type=MESH)

    for to in (other_x, other_y, other_g):
        pl.semaphore_signal(barrier, inc=1, device_id=to, device_id_type=MESH)
    pl.semaphore_wait(barrier, line + 2)

    def remote(src, dst, send, recv, to):
        return pltpu.make_async_remote_copy(
            src_ref=src, dst_ref=dst, send_sem=send, recv_sem=recv, device_id=to, device_id_type=MESH
        )

    def text_copy(i):
        b = order[i]
        at = pl.multiple_of((b * 2 + y) * depth, depth)
        return remote(
            text_ref.at[:, pl.ds(at, depth)], tb.at[z, y], t_send.at[i], t_recv.at[z], along(b)
        )

    def text_landed(a):
        return remote(tb.at[a, y], tb.at[a, y], t_send.at[0], t_recv.at[a], other_y)

    def text_relay(a):
        return remote(tb.at[a, y], tb.at[a, y], y_send.at[a], y_recv.at[a], other_y)

    def text_relayed(a):
        return remote(tb.at[a, 1 - y], tb.at[a, 1 - y], y_send.at[a], y_recv.at[a], other_y)

    quarter = half_cols // 2

    def weight_source(c, core):
        at = pl.multiple_of(core * half_cols + c * quarter, quarter)
        return weight_ref.at[:, pl.ds(at, quarter)]

    def weight_spot(k, c, core):
        return wb.at[k, c, :, pl.ds(pl.multiple_of(core * quarter, quarter), quarter)]

    def weight_x(c):
        return remote(
            weight_source(c, g), weight_spot(x, c, g), x_send.at[4 + c], x_recv.at[4 + c], other_x
        )

    def weight_copy(c, core, send, recv, to):
        spot = weight_spot(1 - x, c, core)
        return remote(spot, spot, send, recv, to)

    def weight_x_in(c):
        return weight_copy(c, g, x_send.at[4 + c], x_recv.at[4 + c], other_x)

    def weight_s(c):
        return weight_copy(c, g, s_send.at[5 + c], s_recv.at[5 + c], other_g)

    def weight_s_in(c):
        return weight_copy(c, 1 - g, s_send.at[5 + c], s_recv.at[5 + c], other_g)

    def unit_rows(core, q):
        return pl.ds(pl.multiple_of(core * piece + q * part, part), part)

    def unit_x(ref, kind, q):
        return remote(
            ref.at[unit_rows(g, q)],
            fb.at[kind, x, unit_rows(g, q)],
            x_send.at[1 + q],
            x_recv.at[1 + q],
            other_x,
        )

    def unit_copy(kind, core, q, send, recv, to):
        spot = fb.at[kind, 1 - x, unit_rows(core, q)]
        return remote(spot, spot, send, recv, to)

    def unit_x_in(q):
        return unit_copy(y, g, q, x_send.at[1 + q], x_recv.at[1 + q], other_x)

    def unit_s(q):
        return unit_copy(y, g, q, s_send.at[1 + q], s_recv.at[1 + q], other_g)

    def unit_s_in(q):
        return unit_copy(y, 1 - g, q, s_send.at[1 + q], s_recv.at[1 + q], other_g)

    def unit_y(q):
        return unit_copy(y, g, q, y_send.at[line + q], y_recv.at[line + q], other_y)

    def unit_y_in(q):
        return unit_copy(1 - y, g, q, y_send.at[line + q], y_recv.at[line + q], other_y)

    def unit_s2(q):
        return unit_copy(1 - y, g, q, s_send.at[3 + q], s_recv.at[3 + q], other_g)

    def unit_s2_in(q):
        return unit_copy(1 - y, 1 - g, q, s_send.at[3 + q], s_recv.at[3 + q], other_g)

    bias_x = remote(bb.at[x], bb.at[x], x_send.at[3], x_recv.at[3], other_x)
    bias_x_in = remote(bb.at[1 - x], bb.at[1 - x], x_send.at[3], x_recv.at[3], other_x)

    def rows_copy(m, a, right):
        to = along(z + 1) if right else along(z - 1)
        spot = rows.at[m, a]
        return remote(spot, spot, a_send.at[1 if right else 0, m, a], a_recv.at[m, a], to)

    def rows_landed(m, a):
        return remote(rows.at[m, a], rows.at[m, a], a_send.at[0, m, a], a_recv.at[m, a], other_y)

    locals_ = [
        pltpu.make_async_copy(weight_source(c, k), weight_spot(x, c, k), local_sem.at[11 + c * 2 + k])
        for c in range(2)
        for k in range(2)
    ] + [
        pltpu.make_async_copy(up_ref, fb.at[0, x], local_sem.at[2]),
        pltpu.make_async_copy(down_ref, fb.at[1, x], local_sem.at[3]),
        pltpu.make_async_copy(key_ref, kw.at[0], local_sem.at[5]),
        pltpu.make_async_copy(value_ref, kw.at[1], local_sem.at[8]),
    ] + [
        pltpu.make_async_copy(
            text_ref.at[:, pl.ds(pl.multiple_of((z * 2 + h) * depth, depth), depth)],
            tb.at[z, h],
            local_sem.at[6 + h],
        )
        for h in range(2)
    ]

    for i in range(line - 1):
        text_copy(i).start()
    for c in range(2):
        weight_x(c).start()
    small = (
        (tiles_in, tiles_ref),
        (links_in, links_ref),
        (lengths_in, lengths_ref),
        (gain_in, gain_ref),
        (shift_in, shift_ref),
        (bias_in, bias_ref),
        (down_bias_in, down_bias_ref),
    )
    own_copies = [
        pltpu.make_async_copy(src, dst, local_sem.at[15 + i]) for i, (src, dst) in enumerate(small)
    ] + [
        pltpu.make_async_copy(images_ref, own.at[0], local_sem.at[9]),
        pltpu.make_async_copy(state_grads_ref, own.at[1], local_sem.at[10]),
    ]
    for copy in own_copies + locals_:
        copy.start()
    for copy in own_copies:
        copy.wait()
    bb[x] = bias_ref[...][None]

    def live_rows(j):
        return tiles_ref[j, g, enc] * patch

    own_live = live_rows(y)

    def norm_body(t, _):
        r = pl.ds(pl.multiple_of(t * 16, 16), 16)
        normed = normalize_layer(own[0, r].astype(f32), gain_ref[...][None], shift_ref[...][None])
        rows[0, z, r] = normed.astype(bf16)
        row = t * 16 + lax.broadcasted_iota(jnp.int32, (16, width), 0)
        rows[1, z, r] = jnp.where(row < own_live, own[1, r].astype(f32), 0.0).astype(bf16)
        return 0

    lax.fori_loop(0, img // 16, norm_body, 0)

    for m in range(2):

        @pl.when(z < line - 1)
        def _(m=m):
            rows_copy(m, z, True).start()

        @pl.when(z > 0)
        def _(m=m):
            rows_copy(m, z, False).start()

    def forward_rows(m, s):
        @pl.when(z - s >= 0)
        def _():
            rows_landed(m, z - s).wait_recv()

            @pl.when(z < line - 1)
            def _():
                rows_copy(m, z - s, True).start()

        @pl.when(z + s <= line - 1)
        def _():
            rows_landed(m, z + s).wait_recv()

            @pl.when(z > 0)
            def _():
                rows_copy(m, z + s, False).start()

    def has_incoming(a):
        return jnp.logical_or(
            jnp.logical_and(a > z, z > 0), jnp.logical_and(a < z, z < line - 1)
        )

    def next_slot(a):
        right = a > z
        to = jnp.where(right, z + 1, z - 1)
        slot = jnp.where(jnp.logical_and(to == a, jnp.logical_not(right)), line, a)
        return to, slot

    pieces = [slice(p * quarter, (p + 1) * quarter) for p in range(2)]

    def sum_copy(a, c, p):
        to, slot = next_slot(a)
        spot = precv.at[slot, c, :, pieces[p]]
        return remote(psend.at[a, c, :, pieces[p]], spot, p_send.at[a, c, p], p_recv.at[slot, c, p], along(to))

    def sum_landed(slot, c, p):
        spot = precv.at[slot, c, :, pieces[p]]
        return remote(spot, spot, p_send.at[0, c, p], p_recv.at[slot, c, p], other_y)

    tile = 256

    def multiply(a, c, store):
        def body(t, _):
            cols = pl.ds(pl.multiple_of(t * tile, tile), tile)
            total = jnp.dot(tb[a, 0], wb[0, c, :, cols], preferred_element_type=f32)
            total = total + jnp.dot(tb[a, 1], wb[1, c, :, cols], preferred_element_type=f32)
            store(t, cols, total)
            return 0

        lax.fori_loop(0, half_cols // tile, body, 0)

    def product(i, c):
        a = order[i]

        def store(t, cols, total):
            psend[a, c, :, cols] = total.astype(bf16)

        multiply(a, c, store)

    def send_product(i, c):
        a = order[i]

        @pl.when(jnp.logical_not(has_incoming(a)))
        def _():
            for p in range(2):
                sum_copy(a, c, p).start()

    def add_incoming(i, c):
        a = order[i]

        @pl.when(has_incoming(a))
        def _():
            for p in range(2):
                sum_landed(a, c, p).wait_recv()

                def body(t, _, cols=pieces[p]):
                    r = pl.ds(pl.multiple_of(t * 32, 32), 32)
                    total = psend[a, c, r, cols].astype(f32) + precv[a, c, r, cols].astype(f32)
                    psend[a, c, r, cols] = total.astype(bf16)
                    return 0

                lax.fori_loop(0, text_rows // 32, body, 0)
                sum_copy(a, c, p).start()

    held = ((line - 2, 0), (line - 2, 1))

    def products(i):
        text_relayed(order[i]).wait_recv()
        for c in range(2):
            product(i, c)
            if (i, c) not in held:
                send_product(i, c)

    def relay_units(q):
        unit_x_in(q).wait_recv()
        unit_s(q).start()
        unit_y(q).start()

    def relay_text(i):
        text_landed(order[i]).wait_recv()
        text_relay(order[i]).start()

    relay_text(0)
    weight_x_in(0).wait_recv()
    weight_s(0).start()
    for copy in locals_:
        copy.wait()
    text_relayed(order[0]).wait_recv()
    weight_s_in(0).wait_recv()
    product(0, 0)
    send_product(0, 0)
    for i in range(1, line - 1):
        relay_text(i)
    weight_x_in(1).wait_recv()
    weight_s(1).start()
    for c in range(2):
        weight_x(c).wait_send()

    @pl.when(y == 0)
    def _():
        for q in range(2):
            unit_x(up_ref, 0, q).start()

    @pl.when(y == 1)
    def _():
        for q in range(2):
            unit_x(down_ref, 1, q).start()

    bias_x.start()

    weight_s_in(1).wait_recv()
    product(0, 1)
    send_product(0, 1)
    forward_rows(0, 1)
    relay_units(0)
    products(1)
    add_incoming(0, 0)
    for m in range(2):
        forward_rows(m, 2 - m)
    relay_units(1)
    for i in range(2, line - 1):
        products(i)
    unit_y_in(0).wait_recv()
    unit_s2(0).start()
    add_incoming(0, 1)
    forward_rows(0, 3)
    unit_y_in(1).wait_recv()
    unit_s2(1).start()
    bias_x_in.wait_recv()
    for q in range(2):
        unit_s_in(q).wait_recv()
        unit_s2_in(q).wait_recv()

    all_rows = line * img

    def up_body(q, _):
        k = q // 2
        at = pl.multiple_of((q % 2) * piece, piece)
        pre[k, pl.ds(at, piece)] = lax.dot_general(
            fb[0, k, pl.ds(at, piece)],
            rows[0].reshape(all_rows, width),
            (((1,), (1,)), ((), ())),
            preferred_element_type=f32,
        )
        return 0

    lax.fori_loop(0, 4, up_body, 0)
    forward_rows(1, 2)
    for k in range(2):
        for t in range(units // 128):
            spot = slice(t * 128, (t + 1) * 128)
            bias_col[k, spot] = jnp.transpose(jnp.broadcast_to(bb[k, :, spot], (8, 128)))

    def gelu_body(r, _):
        k = r // (units // 16)
        at = pl.ds(pl.multiple_of((r % (units // 16)) * 16, 16), 16)
        value = pre[k, at] + bias_col[k, at, 0:1]
        phi = 0.5 * (1.0 + lax.erf(value * 0.7071067811865476))
        hid_t[k, at] = (value * phi).astype(bf16)
        pre[k, at] = phi + value * jnp.exp(-0.5 * value * value) * 0.3989422804014327
        return 0

    lax.fori_loop(0, 2 * units // 16, gelu_body, 0, unroll=4)

    def terms(kind, k, j, owner):
        at = pl.ds(pl.multiple_of(j * piece + owner * part, part), part)
        left = pg_t if kind == 0 else hid_t
        return jnp.dot(left[k, at], rows[kind].reshape(all_rows, width), preferred_element_type=f32)

    grads_s = [remote(gs1.at[m], gr1.at[m], g_send.at[m], g_recv.at[m], other_g) for m in range(2)]
    grads_y = remote(gs2.at[0], gr2.at[0], g_send.at[2], g_recv.at[2], other_y)
    grads_x = remote(gs2.at[1], gr2.at[1], g_send.at[3], g_recv.at[3], other_x)
    grads_x2 = remote(gs3.at[0], gr3.at[0], g_send.at[4], g_recv.at[4], other_x)
    grads_y2 = remote(gs3.at[1], gr3.at[1], g_send.at[5], g_recv.at[5], other_y)

    def share_core(kind):
        def body(q, _):
            k, j = q // 2, q % 2
            gs1[kind, k, j] = terms(kind, k, j, 1 - g).astype(bf16)
            return 0

        lax.fori_loop(0, 4, body, 0)
        grads_s[kind].start()

    def flip_body(t, _):
        for k in range(2):
            at = pl.ds(pl.multiple_of(t * 128, 128), 128)
            hid[k, :, at] = jnp.transpose(hid_t[k, at].astype(f32)).astype(bf16)
        return 0

    lax.fori_loop(0, units // 128, flip_body, 0)

    def down_body(t, _):
        cols = pl.ds(pl.multiple_of(t * tile, tile), tile)
        total = jnp.dot(hid[0], fb[1, 0, :, cols], preferred_element_type=f32)
        po[:, cols] = total + jnp.dot(hid[1], fb[1, 1, :, cols], preferred_element_type=f32)
        return 0

    lax.fori_loop(0, width // tile, down_body, 0)

    def state_copy(a):
        to, slot = next_slot(a)
        return remote(msend.at[a], mrecv.at[slot], m_send.at[a], m_recv.at[slot], along(to))

    def state_landed(slot):
        return remote(mrecv.at[slot], mrecv.at[slot], m_send.at[0], m_recv.at[slot], other_y)

    def send_state(i, first):
        a = order[i]
        waits = has_incoming(a)

        @pl.when(jnp.logical_not(waits) if first else waits)
        def _():
            if not first:
                state_landed(a).wait_recv()

            def body(t, _):
                r = pl.ds(pl.multiple_of(t * 16, 16), 16)
                value = po[pl.ds(pl.multiple_of(a * img + t * 16, 16), 16)]
                if not first:
                    value = value + mrecv[a, r].astype(f32)
                msend[a, r] = value.astype(bf16)
                return 0

            lax.fori_loop(0, img // 16, body, 0)
            state_copy(a).start()

    for i in range(line - 1):
        send_state(i, True)
    for c in range(2):
        send_product(line - 2, c)
    add_incoming(1, 0)
    add_incoming(2, 0)
    forward_rows(1, 3)
    share_core(1)

    def slope_body(q, _):
        k = q // 2
        at = pl.ds(pl.multiple_of((q % 2) * piece, piece), piece)
        grad = lax.dot_general(
            fb[1, k, at],
            rows[1].reshape(all_rows, width),
            (((1,), (1,)), ((), ())),
            preferred_element_type=f32,
        )
        pg_t[k, at] = (grad * pre[k, at]).astype(bf16)
        return 0

    lax.fori_loop(0, 4, slope_body, 0)
    share_core(0)

    grads_s[1].wait_recv()

    def away_x(j, _):
        gs2[1, j] = (terms(1, 1 - x, j, g) + gr1[1, 1 - x, j].astype(f32)).astype(bf16)
        return 0

    lax.fori_loop(0, 2, away_x, 0)
    grads_x.start()
    grads_s[0].wait_recv()

    def away_y(k, _):
        gs2[0, k] = (terms(0, k, 1 - y, g) + gr1[0, k, 1 - y].astype(f32)).astype(bf16)
        return 0

    lax.fori_loop(0, 2, away_y, 0)
    grads_y.start()
    add_incoming(1, 1)
    send_state(0, False)
    send_state(2, False)
    add_incoming(2, 1)
    send_state(1, False)
    grads_x.wait_recv()
    total = terms(1, x, 1 - y, g) + gr1[1, x, 1 - y].astype(f32)
    gs3[1] = (total + gr2[1, 1 - y].astype(f32)).astype(bf16)
    grads_y2.start()
    grads_y.wait_recv()
    total = terms(0, 1 - x, y, g) + gr1[0, 1 - x, y].astype(f32)
    gs3[0] = (total + gr2[0, 1 - x].astype(f32)).astype(bf16)
    grads_x2.start()

    def own_products(c):
        def store(t, cols, total):
            acc[c, :, cols] = total

        multiply(z, c, store)

    def own_texts(c, p):
        @pl.when(z > 0)
        def _():
            sum_landed(z, c, p).wait_recv()

        @pl.when(z < line - 1)
        def _():
            sum_landed(line, c, p).wait_recv()

        def body(t, _):
            r = pl.ds(pl.multiple_of(t * 64, 64), 64)
            for h in range(quarter // HD):
                spot = slice(p * quarter + h * HD, p * quarter + (h + 1) * HD)
                head = acc[c, r, spot]
                head = head + jnp.where(z > 0, precv[z, c, r, spot].astype(f32), 0.0)
                head = head + jnp.where(z < line - 1, precv[line, c, r, spot].astype(f32), 0.0)
                queries[r, spot] = normalize_heads(head).astype(bf16)
            return 0

        lax.fori_loop(0, text_rows // 64, body, 0, unroll=2)

    for c in range(2):
        own_products(c)

    slot_rows = pl.ds(pl.multiple_of(z * img, img), img)
    po[slot_rows] = po[slot_rows] + own[0].astype(f32) + down_bias_ref[...][None]

    @pl.when(z > 0)
    def _():
        state_landed(z).wait_recv()
        po[slot_rows] = po[slot_rows] + mrecv[z].astype(f32)

    @pl.when(z < line - 1)
    def _():
        state_landed(line).wait_recv()
        po[slot_rows] = po[slot_rows] + mrecv[line].astype(f32)

    states = po[slot_rows].astype(bf16)
    local = kv.shape[2]
    own_rows = pl.ds(pl.multiple_of(y * img, img), img)
    away_rows = pl.ds(pl.multiple_of((1 - y) * img, img), img)
    kv_copy = remote(kv_send, kv.at[:, own_rows], k_send, k_recv, other_y)
    kv_in = remote(kv.at[:, away_rows], kv.at[:, away_rows], k_send, k_recv, other_y)
    for sent in (True, False):
        at = pl.multiple_of(((1 - y) if sent else y) * local, local)
        spot = kv_send if sent else kv.at[:, own_rows]
        raw = jnp.dot(states, kw[0, :, pl.ds(at, local)], preferred_element_type=f32)
        for h in range(local // HD):
            head = normalize_heads(raw[:, h * HD : (h + 1) * HD])
            spot[0, :, h * HD : (h + 1) * HD] = head.astype(bf16)
        raw = jnp.dot(states, kw[1, :, pl.ds(at, local)], preferred_element_type=f32)
        spot[1] = raw.astype(bf16)
        if sent:
            kv_copy.start()

    samples, length = context_ref.shape[:2]
    group = quarter // HD

    def attend_texts(c, p):
        key = lax.broadcasted_iota(jnp.int32, (length, 2 * img), 1)

        def body(n, _):
            r = pl.ds(pl.multiple_of(n * length, length), length)
            limits = [jnp.where(links_ref[n, j] > 0, live_rows(j), 0) for j in range(2)]
            allowed = key < jnp.where(key < img, limits[0], limits[1] + img)
            valid = lax.broadcasted_iota(jnp.int32, (length, HD), 0) < lengths_ref[n]
            head_cols = slice(p * HD, (p + 1) * HD)
            for h in range(group):
                first = p * half_cols + c * quarter + h * HD
                cols = slice(first, first + HD)
                score = lax.dot_general(
                    queries[r, p * quarter + h * HD : p * quarter + (h + 1) * HD],
                    kv[0, :, head_cols],
                    (((1,), (1,)), ((), ())),
                    preferred_element_type=f32,
                )
                weights = jnp.where(allowed, jnp.exp(score * HD ** (-0.5)), 0.0)
                scale = 1.0 / jnp.sum(weights, axis=-1, keepdims=True)
                mixed = jnp.dot(
                    (weights * scale).astype(bf16), kv[1, :, head_cols], preferred_element_type=f32
                )
                context_ref[n, :, cols] = jnp.where(valid, mixed, 0.0).astype(bf16)
            return 0

        lax.fori_loop(0, samples, body, 0, unroll=True)

    for p in range(2):
        own_texts(0, p)
    for kind, out in ((1, down_grad_ref), (0, up_grad_ref)):
        (grads_x2, grads_y2)[kind].wait_recv()
        total = terms(kind, x, y, g) + gr1[kind, x, y].astype(f32)
        total = total + gr2[kind, (x, y)[kind]].astype(f32)
        out[...] = total + gr3[kind].astype(f32)

    kv_in.wait_recv()
    for p in range(2):
        attend_texts(0, p)
    for p in range(2):
        own_texts(1, p)
        attend_texts(1, p)

    for i in range(line - 1):
        a = order[i]
        text_copy(i).wait_send()
        text_relay(a).wait_send()
        state_copy(a).wait_send()
        for c in range(2):
            for p in range(2):
                sum_copy(a, c, p).wait_send()
    for copy in (kv_copy, weight_s(0), weight_s(1), bias_x, *grads_s, grads_y, grads_x, grads_x2, grads_y2):
        copy.wait_send()
    for q in range(2):
        for copy in (unit_x(up_ref, 0, q), unit_s(q), unit_y(q), unit_s2(q)):
            copy.wait_send()

    for a in range(line):

        @pl.when(jnp.logical_and(a <= z, z < line - 1))
        def _():
            for m in range(2):
                rows_copy(m, a, True).wait_send()

        @pl.when(jnp.logical_and(a >= z, z > 0))
        def _():
            for m in range(2):
                rows_copy(m, a, False).wait_send()


def store_kernel(*refs):
    count = len(refs) // 2
    copies = [
        pltpu.make_async_copy(refs[i], refs[count + i], refs[-1].at[i]) for i in range(count)
    ]
    for copy in copies:
        copy.start()
    for copy in copies:
        copy.wait()


def store_outputs(*values):
    anywhere = pl.BlockSpec(memory_space=pl.ANY)
    return pl.pallas_call(
        store_kernel,
        out_shape=[jax.ShapeDtypeStruct(value.shape, value.dtype) for value in values],
        in_specs=[anywhere] * len(values),
        out_specs=[anywhere] * len(values),
        scratch_shapes=[pltpu.SemaphoreType.DMA((len(values),))],
        compiler_params=pltpu.CompilerParams(vmem_limit_bytes=1 << 20),
        name="store_outputs",
    )(*values)


def exchange(
    tiles, links, lengths, images, state_grads, gain, shift, bias, up, down, down_bias, key, value, text, weight, patch
):
    line = lax.axis_size("enc") // 2
    text_rows = text.shape[0] * text.shape[1]
    depth, columns = weight.shape
    img, width = images.shape
    units = up.shape[0]
    half = columns // 2
    local = key.shape[1] // 2
    f32, bf16 = jnp.float32, jnp.bfloat16
    dma = pltpu.SemaphoreType.DMA
    part = units // 4
    vmem = pl.BlockSpec(memory_space=pltpu.VMEM)
    anywhere = pl.BlockSpec(memory_space=pl.ANY)
    return pl.pallas_call(
        functools.partial(step_kernel, line, patch),
        out_shape=[
            pltpu.VMEM((*text.shape[:2], columns), bf16),
            pltpu.VMEM((part, width), f32),
            pltpu.VMEM((part, width), f32),
        ],
        in_specs=[anywhere] * 15,
        out_specs=[vmem] * 3,
        scratch_shapes=[
            pltpu.SMEM(tiles.shape, jnp.int32),
            pltpu.SMEM(links.shape, jnp.int32),
            pltpu.SMEM(lengths.shape, jnp.int32),
            pltpu.VMEM(gain.shape, f32),
            pltpu.VMEM(shift.shape, f32),
            pltpu.VMEM(bias.shape, f32),
            pltpu.VMEM(down_bias.shape, f32),
            pltpu.VMEM((2, img, width), bf16),
            pltpu.VMEM((2, width, 2 * local), bf16),
            pltpu.VMEM((2, img, local), bf16),
            pltpu.VMEM((2, 2 * img, local), bf16),
            pltpu.VMEM((text_rows, half), bf16),
            pltpu.VMEM((2, text_rows, half), f32),
            pltpu.VMEM((line, 2, text_rows, depth), bf16),
            pltpu.VMEM((2, 2, depth, half), bf16),
            pltpu.VMEM((2, 2, units, width), bf16),
            pltpu.VMEM((2, 1, units), f32),
            pltpu.VMEM((2, units, 8), f32),
            pltpu.VMEM((2, line, img, width), bf16),
            pltpu.VMEM((2, units, line * img), f32),
            pltpu.VMEM((2, units, line * img), bf16),
            pltpu.VMEM((2, line * img, units), bf16),
            pltpu.VMEM((2, units, line * img), bf16),
            pltpu.VMEM((line * img, width), f32),
            pltpu.VMEM((line, 2, text_rows, half), bf16),
            pltpu.VMEM((line + 1, 2, text_rows, half), bf16),
            pltpu.VMEM((line, img, width), bf16),
            pltpu.VMEM((line + 1, img, width), bf16),
            pltpu.VMEM((2, 2, 2, part, width), bf16),
            pltpu.VMEM((2, 2, 2, part, width), bf16),
            pltpu.VMEM((2, 2, part, width), bf16),
            pltpu.VMEM((2, 2, part, width), bf16),
            pltpu.VMEM((2, part, width), bf16),
            pltpu.VMEM((2, part, width), bf16),
            dma((22,)),
            dma((line - 1,)),
            dma((line,)),
            dma((line + 2,)),
            dma((line + 2,)),
            dma((6,)),
            dma((6,)),
            dma((7,)),
            dma((7,)),
            dma((2, 2, line)),
            dma((2, line)),
            dma((line, 2, 2)),
            dma((line + 1, 2, 2)),
            dma((line,)),
            dma((line + 1,)),
            dma((6,)),
            dma((6,)),
            dma,
            dma,
        ],
        compiler_params=pltpu.CompilerParams(
            collective_id=0, has_side_effects=True, vmem_limit_bytes=64_200_000
        ),
        name="exchange",
    )(tiles, links, lengths, images, state_grads, gain, shift, bias, up, down, down_bias, key, value, text.reshape(text_rows, -1), weight)


def on_column(
    images,
    ln_gain,
    ln_bias,
    fc1_weight,
    fc1_bias,
    fc2_weight,
    fc2_bias,
    key_weight,
    value_weight,
    text,
    query_weight,
    tiles,
    links,
    lengths,
    state_grads,
):
    slots, patch, width = images.shape[1:]
    context, fc1_grad, fc2_grad = exchange(
        tiles.transpose(1, 2, 0),
        links,
        lengths,
        images.reshape(slots * patch, width),
        state_grads.reshape(slots * patch, width),
        ln_gain,
        ln_bias,
        fc1_bias,
        fc1_weight,
        fc2_weight,
        fc2_bias,
        key_weight,
        value_weight,
        text,
        query_weight,
        patch,
    )
    return tuple(store_outputs(context, fc1_grad, fc2_grad))


def on_device(
    images,
    ln_gain,
    ln_bias,
    fc1_weight,
    fc1_bias,
    fc2_weight,
    fc2_bias,
    key_weight,
    value_weight,
    text,
    query_weight,
    tiles,
    links,
    lengths,
    state_grads,
):
    dec_count = lax.axis_size("dec")
    grp_count = lax.axis_size("grp")
    enc_place = lax.axis_index("enc")
    dec_place = lax.axis_index("dec")
    grp_place = lax.axis_index("grp")
    slots = images.shape[1]
    patch = images.shape[2]
    width = images.shape[3]
    img_rows = slots * patch
    own_rows = images.reshape(img_rows, width)
    normed = normalize_layer(own_rows.astype(jnp.float32), ln_gain, ln_bias).astype(jnp.bfloat16)
    samples = text.shape[0]
    length = text.shape[1]
    text_rows = text.reshape(samples * length, text.shape[2])
    half = query_weight.shape[1] // grp_count
    own_half = lax.dynamic_slice_in_dim(query_weight, grp_place * half, half, 1)
    own_tiles = tiles[enc_place, dec_place, grp_place]
    tile_index = jnp.arange(slots)
    own_live = jnp.broadcast_to((tile_index < own_tiles)[:, None, None], (slots, patch, 1)).reshape(
        img_rows, 1
    )
    cotangent = jnp.where(
        own_live, state_grads.reshape(img_rows, width), jnp.zeros((), state_grads.dtype)
    )
    sent = jnp.stack([normed, cotangent])
    text_rows, own_half, _ = lax.optimization_barrier((text_rows, own_half, sent))
    both = lax.all_gather(sent, "enc", axis=1, tiled=True)
    gathered, all_cotangent = both[0], both[1]
    text_blocks = share_text(text_rows)
    pre, hidden, partial_full = encoder_rows(gathered, fc1_weight, fc1_bias, fc2_weight)
    partial_full = partial_full.astype(jnp.bfloat16)
    all_cotangent, _ = lax.optimization_barrier((all_cotangent, partial_full))
    first_term, second_term = weight_terms(gathered, pre, hidden, all_cotangent, fc2_weight)
    queries_of = project_queries(text_blocks, own_half, second_term)
    summed = lax.psum_scatter(
        partial_full, "enc", scatter_dimension=0, tiled=True
    ).astype(jnp.float32)
    states = (own_rows.astype(jnp.float32) + summed + fc2_bias).astype(jnp.bfloat16)
    local_heads = query_weight.shape[1] // HD
    per_group = HEADS // KV_HEADS
    kv_local = max(1, local_heads // per_group)
    first_head = dec_place * local_heads // per_group
    keys, values = share_keys(states, key_weight, value_weight, first_head, kv_local)
    heads_each = local_heads // kv_local
    queries = queries_of
    queries = queries.reshape(samples, length, kv_local, heads_each, HD)
    dec_tiles = tiles[enc_place, :, grp_place]
    live_keys = tile_index[None, :] < dec_tiles[:, None]
    live_keys = jnp.broadcast_to(live_keys[:, :, None], (dec_count, slots, patch)).reshape(
        dec_count, img_rows
    )
    allowed = (links[:, :, None] > 0) & live_keys[None, :, :]
    scores = jnp.einsum(
        "sqghd,jgkd->sghjkq", queries, keys, preferred_element_type=jnp.float32
    ) * HD ** (-0.5)
    weights = jnp.where(allowed[:, None, None, :, :, None], jnp.exp(scores), 0.0)
    totals = jnp.sum(weights, axis=(3, 4), keepdims=True)
    probs = (weights / totals).astype(jnp.bfloat16)
    mixed = jnp.einsum("sghjkq,jgkd->sqghd", probs, values, preferred_element_type=jnp.float32)
    valid = jnp.arange(length)[None, :] < lengths[:, None]
    context = (
        jnp.where(valid[:, :, None, None, None], mixed, 0.0)
        .reshape(samples, length, local_heads * HD)
        .astype(jnp.bfloat16)
    )
    fc1_grad, fc2_grad = share_grads(jnp.stack([first_term, second_term]))
    return (context, fc1_grad, fc2_grad)


def solution(mesh):
    in_specs = (
        P(("enc", "dec", "grp"), None, None, None),
        P(),
        P(),
        P("enc", None),
        P("enc"),
        P("enc", None),
        P(),
        P(),
        P(),
        P(("enc", "grp"), None, None),
        P("enc", "dec"),
        P(),
        P(("enc", "grp"), None),
        P(("enc", "grp")),
        P(("enc", "dec", "grp"), None, None, None),
    )
    out_specs = (
        P(("enc", "grp"), None, "dec"),
        P(("enc", "dec", "grp"), None),
        P(("enc", "dec", "grp"), None),
    )
    paired = mesh.shape["dec"] == 2 and mesh.shape["grp"] == 2 and mesh.shape["enc"] % 2 == 0
    if paired and mesh.shape["enc"] == 8:
        return jax.shard_map(
            on_column, mesh=mesh, in_specs=in_specs, out_specs=out_specs, check_vma=False
        )
    return jax.shard_map(
        on_device, mesh=mesh, in_specs=in_specs, out_specs=out_specs, check_vma=False
    )
```

```python
import functools

import jax
import jax.numpy as jnp
from jax import lax
from jax.experimental import pallas as pl
from jax.experimental.pallas import tpu as pltpu
from jax.sharding import PartitionSpec as P


HEADS = 32
KV_HEADS = 4
HD = 128


EPSILON = 1e-06


def normalize_layer(values, gain, shift):
    middle = jnp.mean(values, axis=-1, keepdims=True)
    centered = values - middle
    spread = jnp.mean(centered * centered, axis=-1, keepdims=True)
    return centered * lax.rsqrt(spread + EPSILON) * gain + shift


def normalize_heads(values):
    return values * lax.rsqrt(jnp.mean(values * values, axis=-1, keepdims=True) + EPSILON)


def gelu_slope(values):
    return (
        0.5 * (1.0 + lax.erf(values * 0.7071067811865476))
        + values * jnp.exp(-0.5 * values * values) * 0.3989422804014327
    )


def encoder_rows(rows, fc1_weight, fc1_bias, fc2_weight):
    pre = (
        lax.dot_general(
            rows, fc1_weight, (((1,), (1,)), ((), ())), preferred_element_type=jnp.float32
        )
        + fc1_bias
    )
    hidden = jax.nn.gelu(pre, approximate=False).astype(jnp.bfloat16)
    partial_sum = jnp.dot(hidden, fc2_weight, preferred_element_type=jnp.float32)
    return (pre, hidden, partial_sum)


def weight_terms(rows, pre, hidden, cotangent, fc2_weight):
    hidden_grad = lax.dot_general(
        cotangent, fc2_weight, (((1,), (1,)), ((), ())), preferred_element_type=jnp.float32
    )
    second_term = lax.dot_general(
        hidden, cotangent, (((0,), (0,)), ((), ())), preferred_element_type=jnp.float32
    )
    pre_grad = (hidden_grad * gelu_slope(pre)).astype(jnp.bfloat16)
    first_term = lax.dot_general(
        pre_grad, rows, (((0,), (0,)), ((), ())), preferred_element_type=jnp.float32
    )
    return (first_term, second_term)


def project_heads(states, key_columns, value_columns, heads):
    width = states.shape[-1]
    key_raw = jnp.einsum(
        "rd,dhe->hre",
        states,
        key_columns.reshape(width, heads, HD),
        preferred_element_type=jnp.float32,
    )
    keys = normalize_heads(key_raw).astype(jnp.bfloat16)
    values = jnp.einsum(
        "rd,dhe->hre",
        states,
        value_columns.reshape(width, heads, HD),
        preferred_element_type=jnp.float32,
    ).astype(jnp.bfloat16)
    return (keys, values)


def shifted(values, axis, step):
    size = lax.axis_size(axis)
    return lax.ppermute(values, axis, [(i, (i + step) % size) for i in range(size)])


def swapped(values):
    return lax.ppermute(values, "enc", [(i, i ^ 1) for i in range(lax.axis_size("enc"))])


def share_text(text_rows):
    enc_count = lax.axis_size("enc")
    _, depth = text_rows.shape
    side = lax.axis_index("enc") % 2
    block = depth // enc_count
    even = jnp.stack([text_rows[:, i * block : (i + 1) * block] for i in range(0, enc_count, 2)])
    odd = jnp.stack([text_rows[:, i * block : (i + 1) * block] for i in range(1, enc_count, 2)])
    own = jnp.where(side == 0, even, odd)
    away = jnp.where(side == 0, odd, even)
    arrived = swapped(away)
    pair = jnp.concatenate([arrived, own], axis=1)
    return jnp.concatenate(
        [pair] + [shifted(pair, "grp", step) for step in range(1, lax.axis_size("grp"))], axis=1
    )


def project_queries(text_blocks, weight, before):
    grp_count = lax.axis_size("grp")
    ring = lax.axis_size("enc") // 2
    enc_count = lax.axis_size("enc")
    place = lax.axis_index("enc") // 2
    total = None
    for step in range(ring):
        if step == max(0, ring - 2):
            weight, _ = lax.optimization_barrier((weight, before))
        left = lax.dynamic_index_in_dim(text_blocks, (place - step) % ring, 0, keepdims=False)
        term = jnp.dot(left, weight, preferred_element_type=jnp.float32)
        total = term if total is None else total + term
        if step < ring - 1:
            weight = lax.ppermute(
                weight, "enc", [(i, (i + 2) % enc_count) for i in range(enc_count)]
            )
    columns = total.shape[1]
    total = total.reshape(grp_count, 2, -1, columns)
    arrived = swapped(total[:, 0].astype(jnp.bfloat16))
    raw = total[:, 1] + arrived.astype(jnp.float32)
    own = normalize_heads(raw.reshape(grp_count, -1, columns // HD, HD)).astype(jnp.bfloat16)
    blocks = jnp.stack(
        [own[0]] + [shifted(own[step], "grp", -step) for step in range(1, grp_count)], axis=1
    )
    start = (grp_count - lax.axis_index("grp")) % grp_count
    blocks = lax.dynamic_slice_in_dim(
        jnp.concatenate([blocks, blocks], axis=1), start, grp_count, 1
    )
    return blocks.reshape(blocks.shape[0], grp_count * columns)


def share_keys(states, key_weight, value_weight, first_head, kv_local):
    dec_count = lax.axis_size("dec")
    rows, _ = states.shape
    if dec_count == 2 and kv_local * dec_count == KV_HEADS:
        keys, values = project_heads(states, key_weight, value_weight, KV_HEADS)
        paired = jnp.stack([keys, values])
        own = lax.dynamic_slice_in_dim(paired, first_head, kv_local, 1)
        away = lax.dynamic_slice_in_dim(paired, KV_HEADS - kv_local - first_head, kv_local, 1)
        arrived = shifted(away, "dec", 1)
        first = lax.axis_index("dec") == 0
        paired = jnp.stack(
            [jnp.where(first, own, arrived), jnp.where(first, arrived, own)], axis=1
        )
        return (paired[0], paired[1])
    key_columns = lax.dynamic_slice_in_dim(key_weight, first_head * HD, kv_local * HD, 1)
    value_columns = lax.dynamic_slice_in_dim(value_weight, first_head * HD, kv_local * HD, 1)
    piece = lax.all_gather(states, "dec", axis=0, tiled=True)
    key_part, value_part = project_heads(piece, key_columns, value_columns, kv_local)
    shape = (kv_local, dec_count, rows, HD)
    return (
        key_part.reshape(shape).transpose(1, 0, 2, 3),
        value_part.reshape(shape).transpose(1, 0, 2, 3),
    )


def share_grads(terms):
    dec_count = lax.axis_size("dec")
    grp_count = lax.axis_size("grp")
    rows = terms.shape[1] // (dec_count * grp_count)
    if dec_count == 2 and grp_count == 2:
        parts = terms.reshape(2, dec_count, grp_count, rows, -1)
        grp_place = lax.axis_index("grp")
        dec_place = lax.axis_index("dec")
        kept = lax.dynamic_index_in_dim(parts, grp_place, 2, keepdims=False)
        away = lax.dynamic_index_in_dim(parts, 1 - grp_place, 2, keepdims=False)
        kept = kept + shifted(away.astype(jnp.bfloat16), "grp", 1).astype(jnp.float32)
        away = lax.dynamic_index_in_dim(kept, 1 - dec_place, 1, keepdims=False)
        kept = lax.dynamic_index_in_dim(kept, dec_place, 1, keepdims=False)
        kept = kept + shifted(away.astype(jnp.bfloat16), "dec", 1).astype(jnp.float32)
        return (kept[0], kept[1])
    summed = lax.psum_scatter(
        terms.astype(jnp.bfloat16), ("dec", "grp"), scatter_dimension=1, tiled=True
    ).astype(jnp.float32)
    return (summed[0], summed[1])


MESH = pl.DeviceIdType.MESH


def pick(table, place):
    return sum(jnp.where(place == i, value, 0) for i, value in enumerate(table))


def step_kernel(
    line,
    patch,
    tiles_in,
    links_in,
    lengths_in,
    images_ref,
    state_grads_ref,
    gain_in,
    shift_in,
    bias_in,
    up_ref,
    down_ref,
    down_bias_in,
    key_ref,
    value_ref,
    text_ref,
    weight_ref,
    context_ref,
    up_grad_ref,
    down_grad_ref,
    tiles_ref,
    links_ref,
    lengths_ref,
    gain_ref,
    shift_ref,
    bias_ref,
    down_bias_ref,
    own,
    kw,
    kv_send,
    kv,
    queries,
    acc,
    tb,
    wb,
    fb,
    bb,
    bias_col,
    rows,
    pre,
    hid_t,
    hid,
    pg_t,
    po,
    psend,
    precv,
    msend,
    mrecv,
    gs1,
    gr1,
    gs2,
    gr2,
    gs3,
    gr3,
    local_sem,
    t_send,
    t_recv,
    y_send,
    y_recv,
    x_send,
    x_recv,
    s_send,
    s_recv,
    a_send,
    a_recv,
    p_send,
    p_recv,
    m_send,
    m_recv,
    g_send,
    g_recv,
    k_send,
    k_recv,
):
    f32 = jnp.float32
    bf16 = jnp.bfloat16
    enc = lax.axis_index("enc")
    y = lax.axis_index("dec")
    g = lax.axis_index("grp")
    z, x = enc // 2, enc % 2
    other_x = ((z * 2 + 1 - x), y, g)
    other_y = (enc, 1 - y, g)
    other_g = (enc, y, 1 - g)

    def along(place):
        return (place * 2 + x, y, g)

    orders = []
    for p in range(line):
        others = [a for a in range(line) if a != p]
        others.sort(key=lambda a: (-abs(a - p), min(a, line - 1 - a)))
        orders.append(others)
    order = [pick([orders[p][i] for p in range(line)], z) for i in range(line - 1)]
    text_rows, depth = tb.shape[2], tb.shape[3]
    half_cols = wb.shape[3]
    img = rows.shape[2]
    width = rows.shape[3]
    units = fb.shape[2]
    piece = units // 2
    part = units // 4

    barrier = pltpu.get_barrier_semaphore()
    for k in range(line):

        @pl.when(z != k)
        def _():
            pl.semaphore_signal(barrier, inc=1, device_id=along(k), device_id_type=MESH)

    for to in (other_x, other_y, other_g):
        pl.semaphore_signal(barrier, inc=1, device_id=to, device_id_type=MESH)
    pl.semaphore_wait(barrier, line + 2)

    def remote(src, dst, send, recv, to):
        return pltpu.make_async_remote_copy(
            src_ref=src, dst_ref=dst, send_sem=send, recv_sem=recv, device_id=to, device_id_type=MESH
        )

    def text_copy(i):
        b = order[i]
        at = pl.multiple_of((b * 2 + y) * depth, depth)
        return remote(
            text_ref.at[:, pl.ds(at, depth)], tb.at[z, y], t_send.at[i], t_recv.at[z], along(b)
        )

    def text_landed(a):
        return remote(tb.at[a, y], tb.at[a, y], t_send.at[0], t_recv.at[a], other_y)

    def text_relay(a):
        return remote(tb.at[a, y], tb.at[a, y], y_send.at[a], y_recv.at[a], other_y)

    def text_relayed(a):
        return remote(tb.at[a, 1 - y], tb.at[a, 1 - y], y_send.at[a], y_recv.at[a], other_y)

    quarter = half_cols // 2

    def weight_source(c, core):
        at = pl.multiple_of(core * half_cols + c * quarter, quarter)
        return weight_ref.at[:, pl.ds(at, quarter)]

    def weight_spot(k, c, core):
        return wb.at[k, c, :, pl.ds(pl.multiple_of(core * quarter, quarter), quarter)]

    def weight_x(c):
        return remote(
            weight_source(c, g), weight_spot(x, c, g), x_send.at[4 + c], x_recv.at[4 + c], other_x
        )

    def weight_copy(c, core, send, recv, to):
        spot = weight_spot(1 - x, c, core)
        return remote(spot, spot, send, recv, to)

    def weight_x_in(c):
        return weight_copy(c, g, x_send.at[4 + c], x_recv.at[4 + c], other_x)

    def weight_s(c):
        return weight_copy(c, g, s_send.at[5 + c], s_recv.at[5 + c], other_g)

    def weight_s_in(c):
        return weight_copy(c, 1 - g, s_send.at[5 + c], s_recv.at[5 + c], other_g)

    def unit_rows(core, q):
        return pl.ds(pl.multiple_of(core * piece + q * part, part), part)

    def unit_x(ref, kind, q):
        return remote(
            ref.at[unit_rows(g, q)],
            fb.at[kind, x, unit_rows(g, q)],
            x_send.at[1 + q],
            x_recv.at[1 + q],
            other_x,
        )

    def unit_copy(kind, core, q, send, recv, to):
        spot = fb.at[kind, 1 - x, unit_rows(core, q)]
        return remote(spot, spot, send, recv, to)

    def unit_x_in(q):
        return unit_copy(y, g, q, x_send.at[1 + q], x_recv.at[1 + q], other_x)

    def unit_s(q):
        return unit_copy(y, g, q, s_send.at[1 + q], s_recv.at[1 + q], other_g)

    def unit_s_in(q):
        return unit_copy(y, 1 - g, q, s_send.at[1 + q], s_recv.at[1 + q], other_g)

    def unit_y(q):
        return unit_copy(y, g, q, y_send.at[line + q], y_recv.at[line + q], other_y)

    def unit_y_in(q):
        return unit_copy(1 - y, g, q, y_send.at[line + q], y_recv.at[line + q], other_y)

    def unit_s2(q):
        return unit_copy(1 - y, g, q, s_send.at[3 + q], s_recv.at[3 + q], other_g)

    def unit_s2_in(q):
        return unit_copy(1 - y, 1 - g, q, s_send.at[3 + q], s_recv.at[3 + q], other_g)

    bias_x = remote(bb.at[x], bb.at[x], x_send.at[3], x_recv.at[3], other_x)
    bias_x_in = remote(bb.at[1 - x], bb.at[1 - x], x_send.at[3], x_recv.at[3], other_x)

    def rows_copy(m, a, right):
        to = along(z + 1) if right else along(z - 1)
        spot = rows.at[m, a]
        return remote(spot, spot, a_send.at[1 if right else 0], a_recv.at[m, a], to)

    def rows_landed(m, a):
        return remote(rows.at[m, a], rows.at[m, a], a_send.at[0], a_recv.at[m, a], other_y)

    locals_ = [
        pltpu.make_async_copy(weight_source(c, k), weight_spot(x, c, k), local_sem.at[11 + c * 2 + k])
        for c in range(2)
        for k in range(2)
    ] + [
        pltpu.make_async_copy(up_ref, fb.at[0, x], local_sem.at[2]),
        pltpu.make_async_copy(down_ref, fb.at[1, x], local_sem.at[3]),
        pltpu.make_async_copy(key_ref, kw.at[0], local_sem.at[5]),
        pltpu.make_async_copy(value_ref, kw.at[1], local_sem.at[8]),
    ] + [
        pltpu.make_async_copy(
            text_ref.at[:, pl.ds(pl.multiple_of((z * 2 + h) * depth, depth), depth)],
            tb.at[z, h],
            local_sem.at[6 + h],
        )
        for h in range(2)
    ]

    for i in range(line - 1):
        text_copy(i).start()
    for c in range(2):
        weight_x(c).start()
    small = (
        (tiles_in, tiles_ref),
        (links_in, links_ref),
        (lengths_in, lengths_ref),
        (gain_in, gain_ref),
        (shift_in, shift_ref),
        (bias_in, bias_ref),
        (down_bias_in, down_bias_ref),
    )
    own_copies = [
        pltpu.make_async_copy(src, dst, local_sem.at[15 + i]) for i, (src, dst) in enumerate(small)
    ] + [
        pltpu.make_async_copy(images_ref, own.at[0], local_sem.at[9]),
        pltpu.make_async_copy(state_grads_ref, own.at[1], local_sem.at[10]),
    ]
    for copy in own_copies + locals_:
        copy.start()
    for copy in own_copies:
        copy.wait()
    bb[x] = bias_ref[...][None]

    def live_rows(j):
        return tiles_ref[j, g, enc] * patch

    own_live = live_rows(y)

    def norm_body(t, _):
        r = pl.ds(pl.multiple_of(t * 16, 16), 16)
        normed = normalize_layer(own[0, r].astype(f32), gain_ref[...][None], shift_ref[...][None])
        rows[0, z, r] = normed.astype(bf16)
        row = t * 16 + lax.broadcasted_iota(jnp.int32, (16, width), 0)
        rows[1, z, r] = jnp.where(row < own_live, own[1, r].astype(f32), 0.0).astype(bf16)
        return 0

    lax.fori_loop(0, img // 16, norm_body, 0)

    for m in range(2):

        @pl.when(z < line - 1)
        def _(m=m):
            rows_copy(m, z, True).start()

        @pl.when(z > 0)
        def _(m=m):
            rows_copy(m, z, False).start()

    def forward_rows(m, s):
        @pl.when(z - s >= 0)
        def _():
            rows_landed(m, z - s).wait_recv()

            @pl.when(z < line - 1)
            def _():
                rows_copy(m, z - s, True).start()

        @pl.when(z + s <= line - 1)
        def _():
            rows_landed(m, z + s).wait_recv()

            @pl.when(z > 0)
            def _():
                rows_copy(m, z + s, False).start()

    def has_incoming(a):
        return jnp.logical_or(
            jnp.logical_and(a > z, z > 0), jnp.logical_and(a < z, z < line - 1)
        )

    def next_slot(a):
        right = a > z
        to = jnp.where(right, z + 1, z - 1)
        slot = jnp.where(jnp.logical_and(to == a, jnp.logical_not(right)), line, a)
        return to, slot

    pieces = [slice(p * quarter, (p + 1) * quarter) for p in range(2)]

    def sum_copy(a, c, p):
        to, slot = next_slot(a)
        spot = precv.at[slot, c, :, pieces[p]]
        return remote(psend.at[a, c, :, pieces[p]], spot, p_send, p_recv.at[slot, c, p], along(to))

    def sum_landed(slot, c, p):
        spot = precv.at[slot, c, :, pieces[p]]
        return remote(spot, spot, p_send, p_recv.at[slot, c, p], other_y)

    tile = 256

    def multiply(a, c, store):
        def body(t, _):
            cols = pl.ds(pl.multiple_of(t * tile, tile), tile)
            total = jnp.dot(tb[a, 0], wb[0, c, :, cols], preferred_element_type=f32)
            total = total + jnp.dot(tb[a, 1], wb[1, c, :, cols], preferred_element_type=f32)
            store(t, cols, total)
            return 0

        lax.fori_loop(0, half_cols // tile, body, 0)

    def product(i, c):
        a = order[i]

        def store(t, cols, total):
            psend[a, c, :, cols] = total.astype(bf16)

        multiply(a, c, store)

    def send_product(i, c):
        a = order[i]

        @pl.when(jnp.logical_not(has_incoming(a)))
        def _():
            for p in range(2):
                sum_copy(a, c, p).start()

    def add_incoming(i, c):
        a = order[i]

        @pl.when(has_incoming(a))
        def _():
            for p in range(2):
                sum_landed(a, c, p).wait_recv()

                def body(t, _, cols=pieces[p]):
                    r = pl.ds(pl.multiple_of(t * 32, 32), 32)
                    total = psend[a, c, r, cols].astype(f32) + precv[a, c, r, cols].astype(f32)
                    psend[a, c, r, cols] = total.astype(bf16)
                    return 0

                lax.fori_loop(0, text_rows // 32, body, 0)
                sum_copy(a, c, p).start()

    held = ((line - 2, 0), (line - 2, 1))

    def products(i):
        text_relayed(order[i]).wait_recv()
        for c in range(2):
            product(i, c)
            if (i, c) not in held:
                send_product(i, c)

    def relay_units(q):
        unit_x_in(q).wait_recv()
        unit_s(q).start()
        unit_y(q).start()

    def relay_text(i):
        text_landed(order[i]).wait_recv()
        text_relay(order[i]).start()

    relay_text(0)
    weight_x_in(0).wait_recv()
    weight_s(0).start()
    for copy in locals_:
        copy.wait()
    text_relayed(order[0]).wait_recv()
    weight_s_in(0).wait_recv()
    product(0, 0)
    send_product(0, 0)
    for i in range(1, line - 1):
        relay_text(i)
    weight_x_in(1).wait_recv()
    weight_s(1).start()
    for c in range(2):
        weight_x(c).wait_send()

    @pl.when(y == 0)
    def _():
        for q in range(2):
            unit_x(up_ref, 0, q).start()

    @pl.when(y == 1)
    def _():
        for q in range(2):
            unit_x(down_ref, 1, q).start()

    bias_x.start()

    weight_s_in(1).wait_recv()
    product(0, 1)
    send_product(0, 1)
    forward_rows(0, 1)
    relay_units(0)
    products(1)
    add_incoming(0, 0)
    for m in range(2):
        forward_rows(m, 2 - m)
    relay_units(1)
    for i in range(2, line - 1):
        products(i)
    unit_y_in(0).wait_recv()
    unit_s2(0).start()
    add_incoming(0, 1)
    forward_rows(0, 3)
    unit_y_in(1).wait_recv()
    unit_s2(1).start()
    bias_x_in.wait_recv()
    for q in range(2):
        unit_s_in(q).wait_recv()
        unit_s2_in(q).wait_recv()

    all_rows = line * img

    def up_body(q, _):
        k = q // 2
        at = pl.multiple_of((q % 2) * piece, piece)
        pre[k, pl.ds(at, piece)] = lax.dot_general(
            fb[0, k, pl.ds(at, piece)],
            rows[0].reshape(all_rows, width),
            (((1,), (1,)), ((), ())),
            preferred_element_type=f32,
        )
        return 0

    lax.fori_loop(0, 4, up_body, 0)
    forward_rows(1, 2)
    for k in range(2):
        for t in range(units // 128):
            spot = slice(t * 128, (t + 1) * 128)
            bias_col[k, spot] = jnp.transpose(jnp.broadcast_to(bb[k, :, spot], (8, 128)))

    def gelu_body(r, _):
        k = r // (units // 16)
        at = pl.ds(pl.multiple_of((r % (units // 16)) * 16, 16), 16)
        value = pre[k, at] + bias_col[k, at, 0:1]
        phi = 0.5 * (1.0 + lax.erf(value * 0.7071067811865476))
        hid_t[k, at] = (value * phi).astype(bf16)
        pre[k, at] = phi + value * jnp.exp(-0.5 * value * value) * 0.3989422804014327
        return 0

    lax.fori_loop(0, 2 * units // 16, gelu_body, 0, unroll=4)

    def terms(kind, k, j, owner):
        at = pl.ds(pl.multiple_of(j * piece + owner * part, part), part)
        left = pg_t if kind == 0 else hid_t
        return jnp.dot(left[k, at], rows[kind].reshape(all_rows, width), preferred_element_type=f32)

    grads_s = [remote(gs1.at[m], gr1.at[m], g_send.at[m], g_recv.at[m], other_g) for m in range(2)]
    grads_y = remote(gs2.at[0], gr2.at[0], g_send.at[2], g_recv.at[2], other_y)
    grads_x = remote(gs2.at[1], gr2.at[1], g_send.at[3], g_recv.at[3], other_x)
    grads_x2 = remote(gs3.at[0], gr3.at[0], g_send.at[4], g_recv.at[4], other_x)
    grads_y2 = remote(gs3.at[1], gr3.at[1], g_send.at[5], g_recv.at[5], other_y)

    def share_core(kind):
        def body(q, _):
            k, j = q // 2, q % 2
            gs1[kind, k, j] = terms(kind, k, j, 1 - g).astype(bf16)
            return 0

        lax.fori_loop(0, 4, body, 0)
        grads_s[kind].start()

    def flip_body(t, _):
        for k in range(2):
            at = pl.ds(pl.multiple_of(t * 128, 128), 128)
            hid[k, :, at] = jnp.transpose(hid_t[k, at].astype(f32)).astype(bf16)
        return 0

    lax.fori_loop(0, units // 128, flip_body, 0)

    def down_body(t, _):
        cols = pl.ds(pl.multiple_of(t * tile, tile), tile)
        total = jnp.dot(hid[0], fb[1, 0, :, cols], preferred_element_type=f32)
        po[:, cols] = total + jnp.dot(hid[1], fb[1, 1, :, cols], preferred_element_type=f32)
        return 0

    lax.fori_loop(0, width // tile, down_body, 0)

    def state_copy(a):
        to, slot = next_slot(a)
        return remote(msend.at[a], mrecv.at[slot], m_send.at[a], m_recv.at[slot], along(to))

    def state_landed(slot):
        return remote(mrecv.at[slot], mrecv.at[slot], m_send.at[0], m_recv.at[slot], other_y)

    def send_state(i, first):
        a = order[i]
        waits = has_incoming(a)

        @pl.when(jnp.logical_not(waits) if first else waits)
        def _():
            if not first:
                state_landed(a).wait_recv()

            def body(t, _):
                r = pl.ds(pl.multiple_of(t * 16, 16), 16)
                value = po[pl.ds(pl.multiple_of(a * img + t * 16, 16), 16)]
                if not first:
                    value = value + mrecv[a, r].astype(f32)
                msend[a, r] = value.astype(bf16)
                return 0

            lax.fori_loop(0, img // 16, body, 0)
            state_copy(a).start()

    for i in range(line - 1):
        send_state(i, True)
    for c in range(2):
        send_product(line - 2, c)
    add_incoming(1, 0)
    add_incoming(2, 0)
    forward_rows(1, 3)
    share_core(1)

    def slope_body(q, _):
        k = q // 2
        at = pl.ds(pl.multiple_of((q % 2) * piece, piece), piece)
        grad = lax.dot_general(
            fb[1, k, at],
            rows[1].reshape(all_rows, width),
            (((1,), (1,)), ((), ())),
            preferred_element_type=f32,
        )
        pg_t[k, at] = (grad * pre[k, at]).astype(bf16)
        return 0

    lax.fori_loop(0, 4, slope_body, 0)
    share_core(0)

    grads_s[1].wait_recv()

    def away_x(j, _):
        gs2[1, j] = (terms(1, 1 - x, j, g) + gr1[1, 1 - x, j].astype(f32)).astype(bf16)
        return 0

    lax.fori_loop(0, 2, away_x, 0)
    grads_x.start()
    grads_s[0].wait_recv()

    def away_y(k, _):
        gs2[0, k] = (terms(0, k, 1 - y, g) + gr1[0, k, 1 - y].astype(f32)).astype(bf16)
        return 0

    lax.fori_loop(0, 2, away_y, 0)
    grads_y.start()
    add_incoming(1, 1)
    send_state(0, False)
    send_state(2, False)
    add_incoming(2, 1)
    send_state(1, False)
    grads_x.wait_recv()
    total = terms(1, x, 1 - y, g) + gr1[1, x, 1 - y].astype(f32)
    gs3[1] = (total + gr2[1, 1 - y].astype(f32)).astype(bf16)
    grads_y2.start()
    grads_y.wait_recv()
    total = terms(0, 1 - x, y, g) + gr1[0, 1 - x, y].astype(f32)
    gs3[0] = (total + gr2[0, 1 - x].astype(f32)).astype(bf16)
    grads_x2.start()

    def own_products(c):
        def store(t, cols, total):
            acc[c, :, cols] = total

        multiply(z, c, store)

    def own_texts(c, p):
        @pl.when(z > 0)
        def _():
            sum_landed(z, c, p).wait_recv()

        @pl.when(z < line - 1)
        def _():
            sum_landed(line, c, p).wait_recv()

        def body(t, _):
            r = pl.ds(pl.multiple_of(t * 64, 64), 64)
            for h in range(quarter // HD):
                spot = slice(p * quarter + h * HD, p * quarter + (h + 1) * HD)
                head = acc[c, r, spot]
                head = head + jnp.where(z > 0, precv[z, c, r, spot].astype(f32), 0.0)
                head = head + jnp.where(z < line - 1, precv[line, c, r, spot].astype(f32), 0.0)
                queries[r, spot] = normalize_heads(head).astype(bf16)
            return 0

        lax.fori_loop(0, text_rows // 64, body, 0, unroll=2)

    for c in range(2):
        own_products(c)

    slot_rows = pl.ds(pl.multiple_of(z * img, img), img)
    po[slot_rows] = po[slot_rows] + own[0].astype(f32) + down_bias_ref[...][None]

    @pl.when(z > 0)
    def _():
        state_landed(z).wait_recv()
        po[slot_rows] = po[slot_rows] + mrecv[z].astype(f32)

    @pl.when(z < line - 1)
    def _():
        state_landed(line).wait_recv()
        po[slot_rows] = po[slot_rows] + mrecv[line].astype(f32)

    states = po[slot_rows].astype(bf16)
    local = kv.shape[2]
    own_rows = pl.ds(pl.multiple_of(y * img, img), img)
    away_rows = pl.ds(pl.multiple_of((1 - y) * img, img), img)
    kv_copy = remote(kv_send, kv.at[:, own_rows], k_send, k_recv, other_y)
    kv_in = remote(kv.at[:, away_rows], kv.at[:, away_rows], k_send, k_recv, other_y)
    for sent in (True, False):
        at = pl.multiple_of(((1 - y) if sent else y) * local, local)
        spot = kv_send if sent else kv.at[:, own_rows]
        raw = jnp.dot(states, kw[0, :, pl.ds(at, local)], preferred_element_type=f32)
        for h in range(local // HD):
            head = normalize_heads(raw[:, h * HD : (h + 1) * HD])
            spot[0, :, h * HD : (h + 1) * HD] = head.astype(bf16)
        raw = jnp.dot(states, kw[1, :, pl.ds(at, local)], preferred_element_type=f32)
        spot[1] = raw.astype(bf16)
        if sent:
            kv_copy.start()

    samples, length = context_ref.shape[:2]
    group = quarter // HD

    def attend_texts(c, p):
        key = lax.broadcasted_iota(jnp.int32, (length, 2 * img), 1)

        def body(n, _):
            r = pl.ds(pl.multiple_of(n * length, length), length)
            limits = [jnp.where(links_ref[n, j] > 0, live_rows(j), 0) for j in range(2)]
            allowed = key < jnp.where(key < img, limits[0], limits[1] + img)
            valid = lax.broadcasted_iota(jnp.int32, (length, HD), 0) < lengths_ref[n]
            head_cols = slice(p * HD, (p + 1) * HD)
            for h in range(group):
                first = p * half_cols + c * quarter + h * HD
                cols = slice(first, first + HD)
                score = lax.dot_general(
                    queries[r, p * quarter + h * HD : p * quarter + (h + 1) * HD],
                    kv[0, :, head_cols],
                    (((1,), (1,)), ((), ())),
                    preferred_element_type=f32,
                )
                weights = jnp.where(allowed, jnp.exp(score * HD ** (-0.5)), 0.0)
                scale = 1.0 / jnp.sum(weights, axis=-1, keepdims=True)
                mixed = jnp.dot(
                    (weights * scale).astype(bf16), kv[1, :, head_cols], preferred_element_type=f32
                )
                context_ref[n, :, cols] = jnp.where(valid, mixed, 0.0).astype(bf16)
            return 0

        lax.fori_loop(0, samples, body, 0, unroll=True)

    for p in range(2):
        own_texts(0, p)
    for kind, out in ((1, down_grad_ref), (0, up_grad_ref)):
        (grads_x2, grads_y2)[kind].wait_recv()
        total = terms(kind, x, y, g) + gr1[kind, x, y].astype(f32)
        total = total + gr2[kind, (x, y)[kind]].astype(f32)
        out[...] = total + gr3[kind].astype(f32)

    kv_in.wait_recv()
    for p in range(2):
        attend_texts(0, p)
    for p in range(2):
        own_texts(1, p)
        attend_texts(1, p)

    sums = psend.at[pl.ds(0, line - 1)]
    remote(sums, sums, p_send, p_recv.at[0, 0, 0], other_y).wait_send()
    for i in range(line - 1):
        a = order[i]
        text_copy(i).wait_send()
        text_relay(a).wait_send()
        state_copy(a).wait_send()
    for copy in (kv_copy, weight_s(0), weight_s(1), bias_x, *grads_s, grads_y, grads_x, grads_x2, grads_y2):
        copy.wait_send()
    for q in range(2):
        for copy in (unit_x(up_ref, 0, q), unit_s(q), unit_y(q), unit_s2(q)):
            copy.wait_send()

    def rows_gone(way, first, count):
        spot = rows.at[:, pl.ds(first, count)]
        remote(spot, spot, a_send.at[way], a_recv.at[0, 0], other_y).wait_send()

    for k in range(line):

        @pl.when(z == k)
        def _(k=k):
            if k < line - 1:
                rows_gone(1, 0, k + 1)
            if k > 0:
                rows_gone(0, k, line - k)


def store_kernel(*refs):
    count = len(refs) // 2
    copies = [
        pltpu.make_async_copy(refs[i], refs[count + i], refs[-1].at[i]) for i in range(count)
    ]
    for copy in copies:
        copy.start()
    for copy in copies:
        copy.wait()


def store_outputs(*values):
    anywhere = pl.BlockSpec(memory_space=pl.ANY)
    return pl.pallas_call(
        store_kernel,
        out_shape=[jax.ShapeDtypeStruct(value.shape, value.dtype) for value in values],
        in_specs=[anywhere] * len(values),
        out_specs=[anywhere] * len(values),
        scratch_shapes=[pltpu.SemaphoreType.DMA((len(values),))],
        compiler_params=pltpu.CompilerParams(vmem_limit_bytes=1 << 20),
        name="store_outputs",
    )(*values)


def exchange(
    tiles, links, lengths, images, state_grads, gain, shift, bias, up, down, down_bias, key, value, text, weight, patch
):
    line = lax.axis_size("enc") // 2
    text_rows = text.shape[0] * text.shape[1]
    depth, columns = weight.shape
    img, width = images.shape
    units = up.shape[0]
    half = columns // 2
    local = key.shape[1] // 2
    f32, bf16 = jnp.float32, jnp.bfloat16
    dma = pltpu.SemaphoreType.DMA
    part = units // 4
    vmem = pl.BlockSpec(memory_space=pltpu.VMEM)
    anywhere = pl.BlockSpec(memory_space=pl.ANY)
    return pl.pallas_call(
        functools.partial(step_kernel, line, patch),
        out_shape=[
            pltpu.VMEM((*text.shape[:2], columns), bf16),
            pltpu.VMEM((part, width), f32),
            pltpu.VMEM((part, width), f32),
        ],
        in_specs=[anywhere] * 15,
        out_specs=[vmem] * 3,
        scratch_shapes=[
            pltpu.SMEM(tiles.shape, jnp.int32),
            pltpu.SMEM(links.shape, jnp.int32),
            pltpu.SMEM(lengths.shape, jnp.int32),
            pltpu.VMEM(gain.shape, f32),
            pltpu.VMEM(shift.shape, f32),
            pltpu.VMEM(bias.shape, f32),
            pltpu.VMEM(down_bias.shape, f32),
            pltpu.VMEM((2, img, width), bf16),
            pltpu.VMEM((2, width, 2 * local), bf16),
            pltpu.VMEM((2, img, local), bf16),
            pltpu.VMEM((2, 2 * img, local), bf16),
            pltpu.VMEM((text_rows, half), bf16),
            pltpu.VMEM((2, text_rows, half), f32),
            pltpu.VMEM((line, 2, text_rows, depth), bf16),
            pltpu.VMEM((2, 2, depth, half), bf16),
            pltpu.VMEM((2, 2, units, width), bf16),
            pltpu.VMEM((2, 1, units), f32),
            pltpu.VMEM((2, units, 8), f32),
            pltpu.VMEM((2, line, img, width), bf16),
            pltpu.VMEM((2, units, line * img), f32),
            pltpu.VMEM((2, units, line * img), bf16),
            pltpu.VMEM((2, line * img, units), bf16),
            pltpu.VMEM((2, units, line * img), bf16),
            pltpu.VMEM((line * img, width), f32),
            pltpu.VMEM((line, 2, text_rows, half), bf16),
            pltpu.VMEM((line + 1, 2, text_rows, half), bf16),
            pltpu.VMEM((line, img, width), bf16),
            pltpu.VMEM((line + 1, img, width), bf16),
            pltpu.VMEM((2, 2, 2, part, width), bf16),
            pltpu.VMEM((2, 2, 2, part, width), bf16),
            pltpu.VMEM((2, 2, part, width), bf16),
            pltpu.VMEM((2, 2, part, width), bf16),
            pltpu.VMEM((2, part, width), bf16),
            pltpu.VMEM((2, part, width), bf16),
            dma((22,)),
            dma((line - 1,)),
            dma((line,)),
            dma((line + 2,)),
            dma((line + 2,)),
            dma((6,)),
            dma((6,)),
            dma((7,)),
            dma((7,)),
            dma((2,)),
            dma((2, line)),
            dma,
            dma((line + 1, 2, 2)),
            dma((line,)),
            dma((line + 1,)),
            dma((6,)),
            dma((6,)),
            dma,
            dma,
        ],
        compiler_params=pltpu.CompilerParams(
            collective_id=0, has_side_effects=True, vmem_limit_bytes=64_200_000
        ),
        name="exchange",
    )(tiles, links, lengths, images, state_grads, gain, shift, bias, up, down, down_bias, key, value, text.reshape(text_rows, -1), weight)


def on_column(
    images,
    ln_gain,
    ln_bias,
    fc1_weight,
    fc1_bias,
    fc2_weight,
    fc2_bias,
    key_weight,
    value_weight,
    text,
    query_weight,
    tiles,
    links,
    lengths,
    state_grads,
):
    slots, patch, width = images.shape[1:]
    context, fc1_grad, fc2_grad = exchange(
        tiles.transpose(1, 2, 0),
        links,
        lengths,
        images.reshape(slots * patch, width),
        state_grads.reshape(slots * patch, width),
        ln_gain,
        ln_bias,
        fc1_bias,
        fc1_weight,
        fc2_weight,
        fc2_bias,
        key_weight,
        value_weight,
        text,
        query_weight,
        patch,
    )
    return tuple(store_outputs(context, fc1_grad, fc2_grad))


def on_device(
    images,
    ln_gain,
    ln_bias,
    fc1_weight,
    fc1_bias,
    fc2_weight,
    fc2_bias,
    key_weight,
    value_weight,
    text,
    query_weight,
    tiles,
    links,
    lengths,
    state_grads,
):
    dec_count = lax.axis_size("dec")
    grp_count = lax.axis_size("grp")
    enc_place = lax.axis_index("enc")
    dec_place = lax.axis_index("dec")
    grp_place = lax.axis_index("grp")
    slots = images.shape[1]
    patch = images.shape[2]
    width = images.shape[3]
    img_rows = slots * patch
    own_rows = images.reshape(img_rows, width)
    normed = normalize_layer(own_rows.astype(jnp.float32), ln_gain, ln_bias).astype(jnp.bfloat16)
    samples = text.shape[0]
    length = text.shape[1]
    text_rows = text.reshape(samples * length, text.shape[2])
    half = query_weight.shape[1] // grp_count
    own_half = lax.dynamic_slice_in_dim(query_weight, grp_place * half, half, 1)
    own_tiles = tiles[enc_place, dec_place, grp_place]
    tile_index = jnp.arange(slots)
    own_live = jnp.broadcast_to((tile_index < own_tiles)[:, None, None], (slots, patch, 1)).reshape(
        img_rows, 1
    )
    cotangent = jnp.where(
        own_live, state_grads.reshape(img_rows, width), jnp.zeros((), state_grads.dtype)
    )
    sent = jnp.stack([normed, cotangent])
    text_rows, own_half, _ = lax.optimization_barrier((text_rows, own_half, sent))
    both = lax.all_gather(sent, "enc", axis=1, tiled=True)
    gathered, all_cotangent = both[0], both[1]
    text_blocks = share_text(text_rows)
    pre, hidden, partial_full = encoder_rows(gathered, fc1_weight, fc1_bias, fc2_weight)
    partial_full = partial_full.astype(jnp.bfloat16)
    all_cotangent, _ = lax.optimization_barrier((all_cotangent, partial_full))
    first_term, second_term = weight_terms(gathered, pre, hidden, all_cotangent, fc2_weight)
    queries_of = project_queries(text_blocks, own_half, second_term)
    summed = lax.psum_scatter(
        partial_full, "enc", scatter_dimension=0, tiled=True
    ).astype(jnp.float32)
    states = (own_rows.astype(jnp.float32) + summed + fc2_bias).astype(jnp.bfloat16)
    local_heads = query_weight.shape[1] // HD
    per_group = HEADS // KV_HEADS
    kv_local = max(1, local_heads // per_group)
    first_head = dec_place * local_heads // per_group
    keys, values = share_keys(states, key_weight, value_weight, first_head, kv_local)
    heads_each = local_heads // kv_local
    queries = queries_of
    queries = queries.reshape(samples, length, kv_local, heads_each, HD)
    dec_tiles = tiles[enc_place, :, grp_place]
    live_keys = tile_index[None, :] < dec_tiles[:, None]
    live_keys = jnp.broadcast_to(live_keys[:, :, None], (dec_count, slots, patch)).reshape(
        dec_count, img_rows
    )
    allowed = (links[:, :, None] > 0) & live_keys[None, :, :]
    scores = jnp.einsum(
        "sqghd,jgkd->sghjkq", queries, keys, preferred_element_type=jnp.float32
    ) * HD ** (-0.5)
    weights = jnp.where(allowed[:, None, None, :, :, None], jnp.exp(scores), 0.0)
    totals = jnp.sum(weights, axis=(3, 4), keepdims=True)
    probs = (weights / totals).astype(jnp.bfloat16)
    mixed = jnp.einsum("sghjkq,jgkd->sqghd", probs, values, preferred_element_type=jnp.float32)
    valid = jnp.arange(length)[None, :] < lengths[:, None]
    context = (
        jnp.where(valid[:, :, None, None, None], mixed, 0.0)
        .reshape(samples, length, local_heads * HD)
        .astype(jnp.bfloat16)
    )
    fc1_grad, fc2_grad = share_grads(jnp.stack([first_term, second_term]))
    return (context, fc1_grad, fc2_grad)


def solution(mesh):
    in_specs = (
        P(("enc", "dec", "grp"), None, None, None),
        P(),
        P(),
        P("enc", None),
        P("enc"),
        P("enc", None),
        P(),
        P(),
        P(),
        P(("enc", "grp"), None, None),
        P("enc", "dec"),
        P(),
        P(("enc", "grp"), None),
        P(("enc", "grp")),
        P(("enc", "dec", "grp"), None, None, None),
    )
    out_specs = (
        P(("enc", "grp"), None, "dec"),
        P(("enc", "dec", "grp"), None),
        P(("enc", "dec", "grp"), None),
    )
    paired = mesh.shape["dec"] == 2 and mesh.shape["grp"] == 2 and mesh.shape["enc"] % 2 == 0
    if paired and mesh.shape["enc"] == 8:
        return jax.shard_map(
            on_column, mesh=mesh, in_specs=in_specs, out_specs=out_specs, check_vma=False
        )
    return jax.shard_map(
        on_device, mesh=mesh, in_specs=in_specs, out_specs=out_specs, check_vma=False
    )
```

```python
import functools

import jax
import jax.numpy as jnp
from jax import lax
from jax.experimental import pallas as pl
from jax.experimental.pallas import tpu as pltpu
from jax.sharding import PartitionSpec as P


HEADS = 32
KV_HEADS = 4
HD = 128


EPSILON = 1e-06


def normalize_layer(values, gain, shift):
    middle = jnp.mean(values, axis=-1, keepdims=True)
    centered = values - middle
    spread = jnp.mean(centered * centered, axis=-1, keepdims=True)
    return centered * lax.rsqrt(spread + EPSILON) * gain + shift


def normalize_heads(values):
    return values * lax.rsqrt(jnp.mean(values * values, axis=-1, keepdims=True) + EPSILON)


def gelu_slope(values):
    return (
        0.5 * (1.0 + lax.erf(values * 0.7071067811865476))
        + values * jnp.exp(-0.5 * values * values) * 0.3989422804014327
    )


def encoder_rows(rows, fc1_weight, fc1_bias, fc2_weight):
    pre = (
        lax.dot_general(
            rows, fc1_weight, (((1,), (1,)), ((), ())), preferred_element_type=jnp.float32
        )
        + fc1_bias
    )
    hidden = jax.nn.gelu(pre, approximate=False).astype(jnp.bfloat16)
    partial_sum = jnp.dot(hidden, fc2_weight, preferred_element_type=jnp.float32)
    return (pre, hidden, partial_sum)


def weight_terms(rows, pre, hidden, cotangent, fc2_weight):
    hidden_grad = lax.dot_general(
        cotangent, fc2_weight, (((1,), (1,)), ((), ())), preferred_element_type=jnp.float32
    )
    second_term = lax.dot_general(
        hidden, cotangent, (((0,), (0,)), ((), ())), preferred_element_type=jnp.float32
    )
    pre_grad = (hidden_grad * gelu_slope(pre)).astype(jnp.bfloat16)
    first_term = lax.dot_general(
        pre_grad, rows, (((0,), (0,)), ((), ())), preferred_element_type=jnp.float32
    )
    return (first_term, second_term)


def project_heads(states, key_columns, value_columns, heads):
    width = states.shape[-1]
    key_raw = jnp.einsum(
        "rd,dhe->hre",
        states,
        key_columns.reshape(width, heads, HD),
        preferred_element_type=jnp.float32,
    )
    keys = normalize_heads(key_raw).astype(jnp.bfloat16)
    values = jnp.einsum(
        "rd,dhe->hre",
        states,
        value_columns.reshape(width, heads, HD),
        preferred_element_type=jnp.float32,
    ).astype(jnp.bfloat16)
    return (keys, values)


def shifted(values, axis, step):
    size = lax.axis_size(axis)
    return lax.ppermute(values, axis, [(i, (i + step) % size) for i in range(size)])


def swapped(values):
    return lax.ppermute(values, "enc", [(i, i ^ 1) for i in range(lax.axis_size("enc"))])


def share_text(text_rows):
    enc_count = lax.axis_size("enc")
    _, depth = text_rows.shape
    side = lax.axis_index("enc") % 2
    block = depth // enc_count
    even = jnp.stack([text_rows[:, i * block : (i + 1) * block] for i in range(0, enc_count, 2)])
    odd = jnp.stack([text_rows[:, i * block : (i + 1) * block] for i in range(1, enc_count, 2)])
    own = jnp.where(side == 0, even, odd)
    away = jnp.where(side == 0, odd, even)
    arrived = swapped(away)
    pair = jnp.concatenate([arrived, own], axis=1)
    return jnp.concatenate(
        [pair] + [shifted(pair, "grp", step) for step in range(1, lax.axis_size("grp"))], axis=1
    )


def project_queries(text_blocks, weight, before):
    grp_count = lax.axis_size("grp")
    ring = lax.axis_size("enc") // 2
    enc_count = lax.axis_size("enc")
    place = lax.axis_index("enc") // 2
    total = None
    for step in range(ring):
        if step == max(0, ring - 2):
            weight, _ = lax.optimization_barrier((weight, before))
        left = lax.dynamic_index_in_dim(text_blocks, (place - step) % ring, 0, keepdims=False)
        term = jnp.dot(left, weight, preferred_element_type=jnp.float32)
        total = term if total is None else total + term
        if step < ring - 1:
            weight = lax.ppermute(
                weight, "enc", [(i, (i + 2) % enc_count) for i in range(enc_count)]
            )
    columns = total.shape[1]
    total = total.reshape(grp_count, 2, -1, columns)
    arrived = swapped(total[:, 0].astype(jnp.bfloat16))
    raw = total[:, 1] + arrived.astype(jnp.float32)
    own = normalize_heads(raw.reshape(grp_count, -1, columns // HD, HD)).astype(jnp.bfloat16)
    blocks = jnp.stack(
        [own[0]] + [shifted(own[step], "grp", -step) for step in range(1, grp_count)], axis=1
    )
    start = (grp_count - lax.axis_index("grp")) % grp_count
    blocks = lax.dynamic_slice_in_dim(
        jnp.concatenate([blocks, blocks], axis=1), start, grp_count, 1
    )
    return blocks.reshape(blocks.shape[0], grp_count * columns)


def share_keys(states, key_weight, value_weight, first_head, kv_local):
    dec_count = lax.axis_size("dec")
    rows, _ = states.shape
    if dec_count == 2 and kv_local * dec_count == KV_HEADS:
        keys, values = project_heads(states, key_weight, value_weight, KV_HEADS)
        paired = jnp.stack([keys, values])
        own = lax.dynamic_slice_in_dim(paired, first_head, kv_local, 1)
        away = lax.dynamic_slice_in_dim(paired, KV_HEADS - kv_local - first_head, kv_local, 1)
        arrived = shifted(away, "dec", 1)
        first = lax.axis_index("dec") == 0
        paired = jnp.stack(
            [jnp.where(first, own, arrived), jnp.where(first, arrived, own)], axis=1
        )
        return (paired[0], paired[1])
    key_columns = lax.dynamic_slice_in_dim(key_weight, first_head * HD, kv_local * HD, 1)
    value_columns = lax.dynamic_slice_in_dim(value_weight, first_head * HD, kv_local * HD, 1)
    piece = lax.all_gather(states, "dec", axis=0, tiled=True)
    key_part, value_part = project_heads(piece, key_columns, value_columns, kv_local)
    shape = (kv_local, dec_count, rows, HD)
    return (
        key_part.reshape(shape).transpose(1, 0, 2, 3),
        value_part.reshape(shape).transpose(1, 0, 2, 3),
    )


def share_grads(terms):
    dec_count = lax.axis_size("dec")
    grp_count = lax.axis_size("grp")
    rows = terms.shape[1] // (dec_count * grp_count)
    if dec_count == 2 and grp_count == 2:
        parts = terms.reshape(2, dec_count, grp_count, rows, -1)
        grp_place = lax.axis_index("grp")
        dec_place = lax.axis_index("dec")
        kept = lax.dynamic_index_in_dim(parts, grp_place, 2, keepdims=False)
        away = lax.dynamic_index_in_dim(parts, 1 - grp_place, 2, keepdims=False)
        kept = kept + shifted(away.astype(jnp.bfloat16), "grp", 1).astype(jnp.float32)
        away = lax.dynamic_index_in_dim(kept, 1 - dec_place, 1, keepdims=False)
        kept = lax.dynamic_index_in_dim(kept, dec_place, 1, keepdims=False)
        kept = kept + shifted(away.astype(jnp.bfloat16), "dec", 1).astype(jnp.float32)
        return (kept[0], kept[1])
    summed = lax.psum_scatter(
        terms.astype(jnp.bfloat16), ("dec", "grp"), scatter_dimension=1, tiled=True
    ).astype(jnp.float32)
    return (summed[0], summed[1])


MESH = pl.DeviceIdType.MESH


def pick(table, place):
    return sum(jnp.where(place == i, value, 0) for i, value in enumerate(table))


def step_kernel(
    line,
    patch,
    tiles_in,
    links_in,
    lengths_in,
    images_ref,
    state_grads_ref,
    gain_in,
    shift_in,
    bias_in,
    up_ref,
    down_ref,
    down_bias_in,
    key_ref,
    value_ref,
    text_ref,
    weight_ref,
    context_ref,
    up_grad_ref,
    down_grad_ref,
    tiles_ref,
    links_ref,
    lengths_ref,
    gain_ref,
    shift_ref,
    bias_ref,
    down_bias_ref,
    own,
    kw,
    kv_send,
    kv,
    queries,
    acc,
    tb,
    wb,
    fb,
    bb,
    bias_col,
    rows,
    pre,
    hid_t,
    hid,
    pg_t,
    po,
    psend,
    precv,
    msend,
    mrecv,
    gs1,
    gr1,
    gs2,
    gr2,
    gs3,
    gr3,
    local_sem,
    t_send,
    t_recv,
    y_send,
    y_recv,
    x_send,
    x_recv,
    s_send,
    s_recv,
    a_send,
    a_recv,
    p_send,
    p_recv,
    m_send,
    m_recv,
    g_send,
    g_recv,
    k_send,
    k_recv,
):
    f32 = jnp.float32
    bf16 = jnp.bfloat16
    enc = lax.axis_index("enc")
    y = lax.axis_index("dec")
    g = lax.axis_index("grp")
    z, x = enc // 2, enc % 2
    other_x = ((z * 2 + 1 - x), y, g)
    other_y = (enc, 1 - y, g)
    other_g = (enc, y, 1 - g)

    def along(place):
        return (place * 2 + x, y, g)

    orders = []
    for p in range(line):
        others = [a for a in range(line) if a != p]
        others.sort(key=lambda a: (-abs(a - p), min(a, line - 1 - a)))
        orders.append(others)
    order = [pick([orders[p][i] for p in range(line)], z) for i in range(line - 1)]
    text_rows, depth = tb.shape[2], tb.shape[3]
    half_cols = wb.shape[3]
    img = rows.shape[2]
    width = rows.shape[3]
    units = fb.shape[2]
    piece = units // 2
    part = units // 4

    barrier = pltpu.get_barrier_semaphore()
    for k in range(line):

        @pl.when(z != k)
        def _():
            pl.semaphore_signal(barrier, inc=1, device_id=along(k), device_id_type=MESH)

    for to in (other_x, other_y, other_g):
        pl.semaphore_signal(barrier, inc=1, device_id=to, device_id_type=MESH)
    pl.semaphore_wait(barrier, line + 2)

    def remote(src, dst, send, recv, to):
        return pltpu.make_async_remote_copy(
            src_ref=src, dst_ref=dst, send_sem=send, recv_sem=recv, device_id=to, device_id_type=MESH
        )

    def text_copy(i):
        b = order[i]
        at = pl.multiple_of((b * 2 + y) * depth, depth)
        return remote(
            text_ref.at[:, pl.ds(at, depth)], tb.at[z, y], t_send, t_recv.at[z], along(b)
        )

    def text_landed(a):
        return remote(tb.at[a, y], tb.at[a, y], t_send, t_recv.at[a], other_y)

    def text_relay(a):
        return remote(tb.at[a, y], tb.at[a, y], y_send.at[a], y_recv.at[a], other_y)

    def text_relayed(a):
        return remote(tb.at[a, 1 - y], tb.at[a, 1 - y], y_send.at[a], y_recv.at[a], other_y)

    quarter = half_cols // 2

    def weight_source(c, core):
        at = pl.multiple_of(core * half_cols + c * quarter, quarter)
        return weight_ref.at[:, pl.ds(at, quarter)]

    def weight_spot(k, c, core):
        return wb.at[k, c, :, pl.ds(pl.multiple_of(core * quarter, quarter), quarter)]

    def weight_x(c):
        return remote(
            weight_source(c, g), weight_spot(x, c, g), x_send.at[4 + c], x_recv.at[4 + c], other_x
        )

    def weight_copy(c, core, send, recv, to):
        spot = weight_spot(1 - x, c, core)
        return remote(spot, spot, send, recv, to)

    def weight_x_in(c):
        return weight_copy(c, g, x_send.at[4 + c], x_recv.at[4 + c], other_x)

    def weight_s(c):
        return weight_copy(c, g, s_send.at[5 + c], s_recv.at[5 + c], other_g)

    def weight_s_in(c):
        return weight_copy(c, 1 - g, s_send.at[5 + c], s_recv.at[5 + c], other_g)

    def unit_rows(core, q):
        return pl.ds(pl.multiple_of(core * piece + q * part, part), part)

    def unit_x(ref, kind, q):
        return remote(
            ref.at[unit_rows(g, q)],
            fb.at[kind, x, unit_rows(g, q)],
            x_send.at[1 + q],
            x_recv.at[1 + q],
            other_x,
        )

    def unit_copy(kind, core, q, send, recv, to):
        spot = fb.at[kind, 1 - x, unit_rows(core, q)]
        return remote(spot, spot, send, recv, to)

    def unit_x_in(q):
        return unit_copy(y, g, q, x_send.at[1 + q], x_recv.at[1 + q], other_x)

    def unit_s(q):
        return unit_copy(y, g, q, s_send.at[1 + q], s_recv.at[1 + q], other_g)

    def unit_s_in(q):
        return unit_copy(y, 1 - g, q, s_send.at[1 + q], s_recv.at[1 + q], other_g)

    def unit_y(q):
        return unit_copy(y, g, q, y_send.at[line + q], y_recv.at[line + q], other_y)

    def unit_y_in(q):
        return unit_copy(1 - y, g, q, y_send.at[line + q], y_recv.at[line + q], other_y)

    def unit_s2(q):
        return unit_copy(1 - y, g, q, s_send.at[3 + q], s_recv.at[3 + q], other_g)

    def unit_s2_in(q):
        return unit_copy(1 - y, 1 - g, q, s_send.at[3 + q], s_recv.at[3 + q], other_g)

    bias_x = remote(bb.at[x], bb.at[x], x_send.at[3], x_recv.at[3], other_x)
    bias_x_in = remote(bb.at[1 - x], bb.at[1 - x], x_send.at[3], x_recv.at[3], other_x)

    def rows_copy(m, a, right):
        to = along(z + 1) if right else along(z - 1)
        spot = rows.at[m, a]
        return remote(spot, spot, a_send.at[1 if right else 0], a_recv.at[m, a], to)

    def rows_landed(m, a):
        return remote(rows.at[m, a], rows.at[m, a], a_send.at[0], a_recv.at[m, a], other_y)

    locals_ = [
        pltpu.make_async_copy(weight_source(c, k), weight_spot(x, c, k), local_sem.at[11 + c * 2 + k])
        for c in range(2)
        for k in range(2)
    ] + [
        pltpu.make_async_copy(up_ref, fb.at[0, x], local_sem.at[2]),
        pltpu.make_async_copy(down_ref, fb.at[1, x], local_sem.at[3]),
        pltpu.make_async_copy(key_ref, kw.at[0], local_sem.at[5]),
        pltpu.make_async_copy(value_ref, kw.at[1], local_sem.at[8]),
    ] + [
        pltpu.make_async_copy(
            text_ref.at[:, pl.ds(pl.multiple_of((z * 2 + h) * depth, depth), depth)],
            tb.at[z, h],
            local_sem.at[6 + h],
        )
        for h in range(2)
    ]

    for i in range(line - 1):
        text_copy(i).start()
    for c in range(2):
        weight_x(c).start()
    small = (
        (tiles_in, tiles_ref),
        (links_in, links_ref),
        (lengths_in, lengths_ref),
        (gain_in, gain_ref),
        (shift_in, shift_ref),
        (bias_in, bias_ref),
        (down_bias_in, down_bias_ref),
    )
    own_copies = [
        pltpu.make_async_copy(src, dst, local_sem.at[15 + i]) for i, (src, dst) in enumerate(small)
    ] + [
        pltpu.make_async_copy(images_ref, own.at[0], local_sem.at[9]),
        pltpu.make_async_copy(state_grads_ref, own.at[1], local_sem.at[10]),
    ]
    for copy in own_copies + locals_:
        copy.start()
    for copy in own_copies:
        copy.wait()
    bb[x] = bias_ref[...][None]

    def live_rows(j):
        return tiles_ref[j, g, enc] * patch

    own_live = live_rows(y)

    def norm_body(t, _):
        r = pl.ds(pl.multiple_of(t * 16, 16), 16)
        normed = normalize_layer(own[0, r].astype(f32), gain_ref[...][None], shift_ref[...][None])
        rows[0, z, r] = normed.astype(bf16)
        row = t * 16 + lax.broadcasted_iota(jnp.int32, (16, width), 0)
        rows[1, z, r] = jnp.where(row < own_live, own[1, r].astype(f32), 0.0).astype(bf16)
        return 0

    lax.fori_loop(0, img // 16, norm_body, 0)

    for m in range(2):

        @pl.when(z < line - 1)
        def _(m=m):
            rows_copy(m, z, True).start()

        @pl.when(z > 0)
        def _(m=m):
            rows_copy(m, z, False).start()

    def forward_rows(m, s):
        @pl.when(z - s >= 0)
        def _():
            rows_landed(m, z - s).wait_recv()

            @pl.when(z < line - 1)
            def _():
                rows_copy(m, z - s, True).start()

        @pl.when(z + s <= line - 1)
        def _():
            rows_landed(m, z + s).wait_recv()

            @pl.when(z > 0)
            def _():
                rows_copy(m, z + s, False).start()

    def has_incoming(a):
        return jnp.logical_or(
            jnp.logical_and(a > z, z > 0), jnp.logical_and(a < z, z < line - 1)
        )

    def next_slot(a):
        right = a > z
        to = jnp.where(right, z + 1, z - 1)
        slot = jnp.where(jnp.logical_and(to == a, jnp.logical_not(right)), line, a)
        return to, slot

    pieces = [slice(p * quarter, (p + 1) * quarter) for p in range(2)]

    def sum_copy(a, c, p):
        to, slot = next_slot(a)
        spot = precv.at[slot, c, :, pieces[p]]
        return remote(psend.at[a, c, :, pieces[p]], spot, p_send, p_recv.at[slot, c, p], along(to))

    def sum_landed(slot, c, p):
        spot = precv.at[slot, c, :, pieces[p]]
        return remote(spot, spot, p_send, p_recv.at[slot, c, p], other_y)

    tile = 256

    def multiply(a, c, store):
        def body(t, _):
            cols = pl.ds(pl.multiple_of(t * tile, tile), tile)
            total = jnp.dot(tb[a, 0], wb[0, c, :, cols], preferred_element_type=f32)
            total = total + jnp.dot(tb[a, 1], wb[1, c, :, cols], preferred_element_type=f32)
            store(t, cols, total)
            return 0

        lax.fori_loop(0, half_cols // tile, body, 0)

    def product(i, c):
        a = order[i]

        def store(t, cols, total):
            psend[a, c, :, cols] = total.astype(bf16)

        multiply(a, c, store)

    def send_product(i, c):
        a = order[i]

        @pl.when(jnp.logical_not(has_incoming(a)))
        def _():
            for p in range(2):
                sum_copy(a, c, p).start()

    def add_incoming(i, c):
        a = order[i]

        @pl.when(has_incoming(a))
        def _():
            for p in range(2):
                sum_landed(a, c, p).wait_recv()

                def body(t, _, cols=pieces[p]):
                    r = pl.ds(pl.multiple_of(t * 32, 32), 32)
                    total = psend[a, c, r, cols].astype(f32) + precv[a, c, r, cols].astype(f32)
                    psend[a, c, r, cols] = total.astype(bf16)
                    return 0

                lax.fori_loop(0, text_rows // 32, body, 0)
                sum_copy(a, c, p).start()

    held = ((line - 2, 0), (line - 2, 1))

    def products(i):
        text_relayed(order[i]).wait_recv()
        for c in range(2):
            product(i, c)
            if (i, c) not in held:
                send_product(i, c)

    def relay_units(q):
        unit_x_in(q).wait_recv()
        unit_s(q).start()
        unit_y(q).start()

    def relay_text(i):
        text_landed(order[i]).wait_recv()
        text_relay(order[i]).start()

    relay_text(0)
    weight_x_in(0).wait_recv()
    weight_s(0).start()
    for copy in locals_:
        copy.wait()
    text_relayed(order[0]).wait_recv()
    weight_s_in(0).wait_recv()
    product(0, 0)
    send_product(0, 0)
    for i in range(1, line - 1):
        relay_text(i)
    weight_x_in(1).wait_recv()
    weight_s(1).start()
    for c in range(2):
        weight_x(c).wait_send()

    @pl.when(y == 0)
    def _():
        for q in range(2):
            unit_x(up_ref, 0, q).start()

    @pl.when(y == 1)
    def _():
        for q in range(2):
            unit_x(down_ref, 1, q).start()

    bias_x.start()

    weight_s_in(1).wait_recv()
    product(0, 1)
    send_product(0, 1)
    forward_rows(0, 1)
    relay_units(0)
    products(1)
    add_incoming(0, 0)
    for m in range(2):
        forward_rows(m, 2 - m)
    relay_units(1)
    for i in range(2, line - 1):
        products(i)
    unit_y_in(0).wait_recv()
    unit_s2(0).start()
    add_incoming(0, 1)
    forward_rows(0, 3)
    unit_y_in(1).wait_recv()
    unit_s2(1).start()
    bias_x_in.wait_recv()
    for q in range(2):
        unit_s_in(q).wait_recv()
        unit_s2_in(q).wait_recv()

    all_rows = line * img

    def up_body(q, _):
        k = q // 2
        at = pl.multiple_of((q % 2) * piece, piece)
        pre[k, pl.ds(at, piece)] = lax.dot_general(
            fb[0, k, pl.ds(at, piece)],
            rows[0].reshape(all_rows, width),
            (((1,), (1,)), ((), ())),
            preferred_element_type=f32,
        )
        return 0

    lax.fori_loop(0, 4, up_body, 0)
    forward_rows(1, 2)
    for k in range(2):
        for t in range(units // 128):
            spot = slice(t * 128, (t + 1) * 128)
            bias_col[k, spot] = jnp.transpose(jnp.broadcast_to(bb[k, :, spot], (8, 128)))

    def gelu_body(r, _):
        k = r // (units // 16)
        at = pl.ds(pl.multiple_of((r % (units // 16)) * 16, 16), 16)
        value = pre[k, at] + bias_col[k, at, 0:1]
        phi = 0.5 * (1.0 + lax.erf(value * 0.7071067811865476))
        hid_t[k, at] = (value * phi).astype(bf16)
        pre[k, at] = phi + value * jnp.exp(-0.5 * value * value) * 0.3989422804014327
        return 0

    lax.fori_loop(0, 2 * units // 16, gelu_body, 0, unroll=4)

    def terms(kind, k, j, owner):
        at = pl.ds(pl.multiple_of(j * piece + owner * part, part), part)
        left = pg_t if kind == 0 else hid_t
        return jnp.dot(left[k, at], rows[kind].reshape(all_rows, width), preferred_element_type=f32)

    grads_s = [remote(gs1.at[m], gr1.at[m], g_send.at[m], g_recv.at[m], other_g) for m in range(2)]
    grads_y = remote(gs2.at[0], gr2.at[0], g_send.at[2], g_recv.at[2], other_y)
    grads_x = remote(gs2.at[1], gr2.at[1], g_send.at[3], g_recv.at[3], other_x)
    grads_x2 = remote(gs3.at[0], gr3.at[0], g_send.at[4], g_recv.at[4], other_x)
    grads_y2 = remote(gs3.at[1], gr3.at[1], g_send.at[5], g_recv.at[5], other_y)

    def share_core(kind):
        def body(q, _):
            k, j = q // 2, q % 2
            gs1[kind, k, j] = terms(kind, k, j, 1 - g).astype(bf16)
            return 0

        lax.fori_loop(0, 4, body, 0)
        grads_s[kind].start()

    def flip_body(t, _):
        for k in range(2):
            at = pl.ds(pl.multiple_of(t * 128, 128), 128)
            hid[k, :, at] = jnp.transpose(hid_t[k, at].astype(f32)).astype(bf16)
        return 0

    lax.fori_loop(0, units // 128, flip_body, 0)

    def down_body(t, _):
        cols = pl.ds(pl.multiple_of(t * tile, tile), tile)
        total = jnp.dot(hid[0], fb[1, 0, :, cols], preferred_element_type=f32)
        po[:, cols] = total + jnp.dot(hid[1], fb[1, 1, :, cols], preferred_element_type=f32)
        return 0

    lax.fori_loop(0, width // tile, down_body, 0)

    def state_copy(a):
        to, slot = next_slot(a)
        return remote(msend.at[a], mrecv.at[slot], m_send, m_recv.at[slot], along(to))

    def state_landed(slot):
        return remote(mrecv.at[slot], mrecv.at[slot], m_send, m_recv.at[slot], other_y)

    def send_state(i, first):
        a = order[i]
        waits = has_incoming(a)

        @pl.when(jnp.logical_not(waits) if first else waits)
        def _():
            if not first:
                state_landed(a).wait_recv()

            def body(t, _):
                r = pl.ds(pl.multiple_of(t * 16, 16), 16)
                value = po[pl.ds(pl.multiple_of(a * img + t * 16, 16), 16)]
                if not first:
                    value = value + mrecv[a, r].astype(f32)
                msend[a, r] = value.astype(bf16)
                return 0

            lax.fori_loop(0, img // 16, body, 0)
            state_copy(a).start()

    for i in range(line - 1):
        send_state(i, True)
    for c in range(2):
        send_product(line - 2, c)
    add_incoming(1, 0)
    add_incoming(2, 0)
    forward_rows(1, 3)
    share_core(1)

    def slope_body(q, _):
        k = q // 2
        at = pl.ds(pl.multiple_of((q % 2) * piece, piece), piece)
        grad = lax.dot_general(
            fb[1, k, at],
            rows[1].reshape(all_rows, width),
            (((1,), (1,)), ((), ())),
            preferred_element_type=f32,
        )
        pg_t[k, at] = (grad * pre[k, at]).astype(bf16)
        return 0

    lax.fori_loop(0, 4, slope_body, 0)
    share_core(0)

    grads_s[1].wait_recv()

    def away_x(j, _):
        gs2[1, j] = (terms(1, 1 - x, j, g) + gr1[1, 1 - x, j].astype(f32)).astype(bf16)
        return 0

    lax.fori_loop(0, 2, away_x, 0)
    grads_x.start()
    grads_s[0].wait_recv()

    def away_y(k, _):
        gs2[0, k] = (terms(0, k, 1 - y, g) + gr1[0, k, 1 - y].astype(f32)).astype(bf16)
        return 0

    lax.fori_loop(0, 2, away_y, 0)
    grads_y.start()
    add_incoming(1, 1)
    send_state(0, False)
    send_state(2, False)
    add_incoming(2, 1)
    send_state(1, False)
    grads_x.wait_recv()
    total = terms(1, x, 1 - y, g) + gr1[1, x, 1 - y].astype(f32)
    gs3[1] = (total + gr2[1, 1 - y].astype(f32)).astype(bf16)
    grads_y2.start()
    grads_y.wait_recv()
    total = terms(0, 1 - x, y, g) + gr1[0, 1 - x, y].astype(f32)
    gs3[0] = (total + gr2[0, 1 - x].astype(f32)).astype(bf16)
    grads_x2.start()

    def own_products(c):
        def store(t, cols, total):
            acc[c, :, cols] = total

        multiply(z, c, store)

    def own_texts(c, p):
        @pl.when(z > 0)
        def _():
            sum_landed(z, c, p).wait_recv()

        @pl.when(z < line - 1)
        def _():
            sum_landed(line, c, p).wait_recv()

        def body(t, _):
            r = pl.ds(pl.multiple_of(t * 64, 64), 64)
            for h in range(quarter // HD):
                spot = slice(p * quarter + h * HD, p * quarter + (h + 1) * HD)
                head = acc[c, r, spot]
                head = head + jnp.where(z > 0, precv[z, c, r, spot].astype(f32), 0.0)
                head = head + jnp.where(z < line - 1, precv[line, c, r, spot].astype(f32), 0.0)
                queries[r, spot] = normalize_heads(head).astype(bf16)
            return 0

        lax.fori_loop(0, text_rows // 64, body, 0, unroll=2)

    for c in range(2):
        own_products(c)

    slot_rows = pl.ds(pl.multiple_of(z * img, img), img)
    po[slot_rows] = po[slot_rows] + own[0].astype(f32) + down_bias_ref[...][None]

    @pl.when(z > 0)
    def _():
        state_landed(z).wait_recv()
        po[slot_rows] = po[slot_rows] + mrecv[z].astype(f32)

    @pl.when(z < line - 1)
    def _():
        state_landed(line).wait_recv()
        po[slot_rows] = po[slot_rows] + mrecv[line].astype(f32)

    states = po[slot_rows].astype(bf16)
    local = kv.shape[2]
    own_rows = pl.ds(pl.multiple_of(y * img, img), img)
    away_rows = pl.ds(pl.multiple_of((1 - y) * img, img), img)
    kv_copy = remote(kv_send, kv.at[:, own_rows], k_send, k_recv, other_y)
    kv_in = remote(kv.at[:, away_rows], kv.at[:, away_rows], k_send, k_recv, other_y)
    for sent in (True, False):
        at = pl.multiple_of(((1 - y) if sent else y) * local, local)
        spot = kv_send if sent else kv.at[:, own_rows]
        raw = jnp.dot(states, kw[0, :, pl.ds(at, local)], preferred_element_type=f32)
        for h in range(local // HD):
            head = normalize_heads(raw[:, h * HD : (h + 1) * HD])
            spot[0, :, h * HD : (h + 1) * HD] = head.astype(bf16)
        raw = jnp.dot(states, kw[1, :, pl.ds(at, local)], preferred_element_type=f32)
        spot[1] = raw.astype(bf16)
        if sent:
            kv_copy.start()

    samples, length = context_ref.shape[:2]
    group = quarter // HD

    def attend_texts(c, p):
        key = lax.broadcasted_iota(jnp.int32, (length, 2 * img), 1)

        def body(n, _):
            r = pl.ds(pl.multiple_of(n * length, length), length)
            limits = [jnp.where(links_ref[n, j] > 0, live_rows(j), 0) for j in range(2)]
            allowed = key < jnp.where(key < img, limits[0], limits[1] + img)
            valid = lax.broadcasted_iota(jnp.int32, (length, HD), 0) < lengths_ref[n]
            head_cols = slice(p * HD, (p + 1) * HD)
            for h in range(group):
                first = p * half_cols + c * quarter + h * HD
                cols = slice(first, first + HD)
                score = lax.dot_general(
                    queries[r, p * quarter + h * HD : p * quarter + (h + 1) * HD],
                    kv[0, :, head_cols],
                    (((1,), (1,)), ((), ())),
                    preferred_element_type=f32,
                )
                weights = jnp.where(allowed, jnp.exp(score * HD ** (-0.5)), 0.0)
                scale = 1.0 / jnp.sum(weights, axis=-1, keepdims=True)
                mixed = jnp.dot(
                    (weights * scale).astype(bf16), kv[1, :, head_cols], preferred_element_type=f32
                )
                context_ref[n, :, cols] = jnp.where(valid, mixed, 0.0).astype(bf16)
            return 0

        lax.fori_loop(0, samples, body, 0, unroll=True)

    for p in range(2):
        own_texts(0, p)
    for kind, out in ((1, down_grad_ref), (0, up_grad_ref)):
        (grads_x2, grads_y2)[kind].wait_recv()
        total = terms(kind, x, y, g) + gr1[kind, x, y].astype(f32)
        total = total + gr2[kind, (x, y)[kind]].astype(f32)
        out[...] = total + gr3[kind].astype(f32)

    kv_in.wait_recv()
    for p in range(2):
        attend_texts(0, p)
    for p in range(2):
        own_texts(1, p)
        attend_texts(1, p)

    texts = tb.at[pl.ds(0, line - 1), 0]
    remote(texts, texts, t_send, t_recv.at[0], other_y).wait_send()
    sums = msend.at[pl.ds(0, line - 1)]
    remote(sums, sums, m_send, m_recv.at[0], other_y).wait_send()
    sums = psend.at[pl.ds(0, line - 1)]
    remote(sums, sums, p_send, p_recv.at[0, 0, 0], other_y).wait_send()
    for i in range(line - 1):
        a = order[i]
        text_relay(a).wait_send()
    for copy in (kv_copy, weight_s(0), weight_s(1), bias_x, *grads_s, grads_y, grads_x, grads_x2, grads_y2):
        copy.wait_send()
    for q in range(2):
        for copy in (unit_x(up_ref, 0, q), unit_s(q), unit_y(q), unit_s2(q)):
            copy.wait_send()

    def rows_gone(way, first, count):
        spot = rows.at[:, pl.ds(first, count)]
        remote(spot, spot, a_send.at[way], a_recv.at[0, 0], other_y).wait_send()

    for k in range(line):

        @pl.when(z == k)
        def _(k=k):
            if k < line - 1:
                rows_gone(1, 0, k + 1)
            if k > 0:
                rows_gone(0, k, line - k)


def store_kernel(*refs):
    count = len(refs) // 2
    copies = [
        pltpu.make_async_copy(refs[i], refs[count + i], refs[-1].at[i]) for i in range(count)
    ]
    for copy in copies:
        copy.start()
    for copy in copies:
        copy.wait()


def store_outputs(*values):
    anywhere = pl.BlockSpec(memory_space=pl.ANY)
    return pl.pallas_call(
        store_kernel,
        out_shape=[jax.ShapeDtypeStruct(value.shape, value.dtype) for value in values],
        in_specs=[anywhere] * len(values),
        out_specs=[anywhere] * len(values),
        scratch_shapes=[pltpu.SemaphoreType.DMA((len(values),))],
        compiler_params=pltpu.CompilerParams(vmem_limit_bytes=1 << 20),
        name="store_outputs",
    )(*values)


def exchange(
    tiles, links, lengths, images, state_grads, gain, shift, bias, up, down, down_bias, key, value, text, weight, patch
):
    line = lax.axis_size("enc") // 2
    text_rows = text.shape[0] * text.shape[1]
    depth, columns = weight.shape
    img, width = images.shape
    units = up.shape[0]
    half = columns // 2
    local = key.shape[1] // 2
    f32, bf16 = jnp.float32, jnp.bfloat16
    dma = pltpu.SemaphoreType.DMA
    part = units // 4
    vmem = pl.BlockSpec(memory_space=pltpu.VMEM)
    anywhere = pl.BlockSpec(memory_space=pl.ANY)
    return pl.pallas_call(
        functools.partial(step_kernel, line, patch),
        out_shape=[
            pltpu.VMEM((*text.shape[:2], columns), bf16),
            pltpu.VMEM((part, width), f32),
            pltpu.VMEM((part, width), f32),
        ],
        in_specs=[anywhere] * 15,
        out_specs=[vmem] * 3,
        scratch_shapes=[
            pltpu.SMEM(tiles.shape, jnp.int32),
            pltpu.SMEM(links.shape, jnp.int32),
            pltpu.SMEM(lengths.shape, jnp.int32),
            pltpu.VMEM(gain.shape, f32),
            pltpu.VMEM(shift.shape, f32),
            pltpu.VMEM(bias.shape, f32),
            pltpu.VMEM(down_bias.shape, f32),
            pltpu.VMEM((2, img, width), bf16),
            pltpu.VMEM((2, width, 2 * local), bf16),
            pltpu.VMEM((2, img, local), bf16),
            pltpu.VMEM((2, 2 * img, local), bf16),
            pltpu.VMEM((text_rows, half), bf16),
            pltpu.VMEM((2, text_rows, half), f32),
            pltpu.VMEM((line, 2, text_rows, depth), bf16),
            pltpu.VMEM((2, 2, depth, half), bf16),
            pltpu.VMEM((2, 2, units, width), bf16),
            pltpu.VMEM((2, 1, units), f32),
            pltpu.VMEM((2, units, 8), f32),
            pltpu.VMEM((2, line, img, width), bf16),
            pltpu.VMEM((2, units, line * img), f32),
            pltpu.VMEM((2, units, line * img), bf16),
            pltpu.VMEM((2, line * img, units), bf16),
            pltpu.VMEM((2, units, line * img), bf16),
            pltpu.VMEM((line * img, width), f32),
            pltpu.VMEM((line, 2, text_rows, half), bf16),
            pltpu.VMEM((line + 1, 2, text_rows, half), bf16),
            pltpu.VMEM((line, img, width), bf16),
            pltpu.VMEM((line + 1, img, width), bf16),
            pltpu.VMEM((2, 2, 2, part, width), bf16),
            pltpu.VMEM((2, 2, 2, part, width), bf16),
            pltpu.VMEM((2, 2, part, width), bf16),
            pltpu.VMEM((2, 2, part, width), bf16),
            pltpu.VMEM((2, part, width), bf16),
            pltpu.VMEM((2, part, width), bf16),
            dma((22,)),
            dma,
            dma((line,)),
            dma((line + 2,)),
            dma((line + 2,)),
            dma((6,)),
            dma((6,)),
            dma((7,)),
            dma((7,)),
            dma((2,)),
            dma((2, line)),
            dma,
            dma((line + 1, 2, 2)),
            dma,
            dma((line + 1,)),
            dma((6,)),
            dma((6,)),
            dma,
            dma,
        ],
        compiler_params=pltpu.CompilerParams(
            collective_id=0, has_side_effects=True, vmem_limit_bytes=64_200_000
        ),
        name="exchange",
    )(tiles, links, lengths, images, state_grads, gain, shift, bias, up, down, down_bias, key, value, text.reshape(text_rows, -1), weight)


def on_column(
    images,
    ln_gain,
    ln_bias,
    fc1_weight,
    fc1_bias,
    fc2_weight,
    fc2_bias,
    key_weight,
    value_weight,
    text,
    query_weight,
    tiles,
    links,
    lengths,
    state_grads,
):
    slots, patch, width = images.shape[1:]
    context, fc1_grad, fc2_grad = exchange(
        tiles.transpose(1, 2, 0),
        links,
        lengths,
        images.reshape(slots * patch, width),
        state_grads.reshape(slots * patch, width),
        ln_gain,
        ln_bias,
        fc1_bias,
        fc1_weight,
        fc2_weight,
        fc2_bias,
        key_weight,
        value_weight,
        text,
        query_weight,
        patch,
    )
    return tuple(store_outputs(context, fc1_grad, fc2_grad))


def on_device(
    images,
    ln_gain,
    ln_bias,
    fc1_weight,
    fc1_bias,
    fc2_weight,
    fc2_bias,
    key_weight,
    value_weight,
    text,
    query_weight,
    tiles,
    links,
    lengths,
    state_grads,
):
    dec_count = lax.axis_size("dec")
    grp_count = lax.axis_size("grp")
    enc_place = lax.axis_index("enc")
    dec_place = lax.axis_index("dec")
    grp_place = lax.axis_index("grp")
    slots = images.shape[1]
    patch = images.shape[2]
    width = images.shape[3]
    img_rows = slots * patch
    own_rows = images.reshape(img_rows, width)
    normed = normalize_layer(own_rows.astype(jnp.float32), ln_gain, ln_bias).astype(jnp.bfloat16)
    samples = text.shape[0]
    length = text.shape[1]
    text_rows = text.reshape(samples * length, text.shape[2])
    half = query_weight.shape[1] // grp_count
    own_half = lax.dynamic_slice_in_dim(query_weight, grp_place * half, half, 1)
    own_tiles = tiles[enc_place, dec_place, grp_place]
    tile_index = jnp.arange(slots)
    own_live = jnp.broadcast_to((tile_index < own_tiles)[:, None, None], (slots, patch, 1)).reshape(
        img_rows, 1
    )
    cotangent = jnp.where(
        own_live, state_grads.reshape(img_rows, width), jnp.zeros((), state_grads.dtype)
    )
    sent = jnp.stack([normed, cotangent])
    text_rows, own_half, _ = lax.optimization_barrier((text_rows, own_half, sent))
    both = lax.all_gather(sent, "enc", axis=1, tiled=True)
    gathered, all_cotangent = both[0], both[1]
    text_blocks = share_text(text_rows)
    pre, hidden, partial_full = encoder_rows(gathered, fc1_weight, fc1_bias, fc2_weight)
    partial_full = partial_full.astype(jnp.bfloat16)
    all_cotangent, _ = lax.optimization_barrier((all_cotangent, partial_full))
    first_term, second_term = weight_terms(gathered, pre, hidden, all_cotangent, fc2_weight)
    queries_of = project_queries(text_blocks, own_half, second_term)
    summed = lax.psum_scatter(
        partial_full, "enc", scatter_dimension=0, tiled=True
    ).astype(jnp.float32)
    states = (own_rows.astype(jnp.float32) + summed + fc2_bias).astype(jnp.bfloat16)
    local_heads = query_weight.shape[1] // HD
    per_group = HEADS // KV_HEADS
    kv_local = max(1, local_heads // per_group)
    first_head = dec_place * local_heads // per_group
    keys, values = share_keys(states, key_weight, value_weight, first_head, kv_local)
    heads_each = local_heads // kv_local
    queries = queries_of
    queries = queries.reshape(samples, length, kv_local, heads_each, HD)
    dec_tiles = tiles[enc_place, :, grp_place]
    live_keys = tile_index[None, :] < dec_tiles[:, None]
    live_keys = jnp.broadcast_to(live_keys[:, :, None], (dec_count, slots, patch)).reshape(
        dec_count, img_rows
    )
    allowed = (links[:, :, None] > 0) & live_keys[None, :, :]
    scores = jnp.einsum(
        "sqghd,jgkd->sghjkq", queries, keys, preferred_element_type=jnp.float32
    ) * HD ** (-0.5)
    weights = jnp.where(allowed[:, None, None, :, :, None], jnp.exp(scores), 0.0)
    totals = jnp.sum(weights, axis=(3, 4), keepdims=True)
    probs = (weights / totals).astype(jnp.bfloat16)
    mixed = jnp.einsum("sghjkq,jgkd->sqghd", probs, values, preferred_element_type=jnp.float32)
    valid = jnp.arange(length)[None, :] < lengths[:, None]
    context = (
        jnp.where(valid[:, :, None, None, None], mixed, 0.0)
        .reshape(samples, length, local_heads * HD)
        .astype(jnp.bfloat16)
    )
    fc1_grad, fc2_grad = share_grads(jnp.stack([first_term, second_term]))
    return (context, fc1_grad, fc2_grad)


def solution(mesh):
    in_specs = (
        P(("enc", "dec", "grp"), None, None, None),
        P(),
        P(),
        P("enc", None),
        P("enc"),
        P("enc", None),
        P(),
        P(),
        P(),
        P(("enc", "grp"), None, None),
        P("enc", "dec"),
        P(),
        P(("enc", "grp"), None),
        P(("enc", "grp")),
        P(("enc", "dec", "grp"), None, None, None),
    )
    out_specs = (
        P(("enc", "grp"), None, "dec"),
        P(("enc", "dec", "grp"), None),
        P(("enc", "dec", "grp"), None),
    )
    paired = mesh.shape["dec"] == 2 and mesh.shape["grp"] == 2 and mesh.shape["enc"] % 2 == 0
    if paired and mesh.shape["enc"] == 8:
        return jax.shard_map(
            on_column, mesh=mesh, in_specs=in_specs, out_specs=out_specs, check_vma=False
        )
    return jax.shard_map(
        on_device, mesh=mesh, in_specs=in_specs, out_specs=out_specs, check_vma=False
    )
```
